256 devices in a mesh: gene: 64 (over x, z, core), cell: 4 (over y).
Axes of the slice: x: 4, y: 4, z: 8, core: 2. Of those that a mesh axis runs over, the one named last changes fastest.
Arguments:
- pool_counts: bfloat16 [20480, 16384], P('gene', 'cell'), may hold values from 0 to 6.5
- cell_picks: int32 [7, 4096], P(None, 'cell'), may hold values from 0 to 16383, as said below
- loadings_init: float32 [64, 20480], P(None, 'gene'), may hold values from -0.0390625 to 0.0390625
Outputs:
- scaled_loadings: float32 [64, 20480], P(None, 'gene')
The draws below stay inside these ranges and needn't reach their ends.
Inputs may be any that keep to these rules, and one draw needn't show every extreme that they name: `cell_picks`: column b of every row names a pool cell in [(b // 1024) * 4096, (b // 1024 + 1) * 4096); no cell is named twice in one row.
All inputs are finite; a program needn't handle non-finite values.
Results may differ from the reference program's by a relative error of at most 0.018.
Values may be sent and summed in bfloat16 or wider, within the bound.
No kernel may reach another device: no remote copies, remote signals or barrier semaphores. Data moves between devices by JAX's collectives and lax.ppermute only.
A program may use at most 64 MiB of HBM per device.

```python
import math
import jax
import jax.numpy as jnp
from jax import lax

GENES = 20480
COMPS = 64
STEPS = 7
BATCH_DEV = 1024
POOL_DEV = 4096
BATCH = 4096
POOL = 16384


def draw_pool_counts(key, part):
    scale_key, noise_key = jax.random.split(jax.random.fold_in(key, 11))
    genes = jnp.arange(GENES, dtype=jnp.float32)
    rising = 1.0 + 2.0 * genes / max(GENES - 1, 1)
    lowest, highest = (math.log(0.1), math.log(10.0))
    gene_scale = jnp.exp(jax.random.uniform(scale_key, (GENES,), jnp.float32, lowest, highest)) * rising
    noise = jnp.minimum(jax.random.exponential(noise_key, (GENES, POOL), jnp.float32), 12.0)
    return jnp.log1p(gene_scale[:, None] * noise).astype(jnp.bfloat16)


def draw_cell_picks(key, part):
    base = jax.random.fold_in(key, 23)
    rows = []
    for step_index in range(STEPS):
        pieces = []
        for group_index in range(BATCH // BATCH_DEV):
            group_key = jax.random.fold_in(jax.random.fold_in(base, step_index), group_index)
            order = jax.random.permutation(group_key, POOL_DEV).astype(jnp.int32)
            pieces.append(order[:BATCH_DEV] + group_index * POOL_DEV)
        rows.append(jnp.concatenate(pieces))
    return jnp.stack(rows).astype(jnp.int32)


def steps_of(rng, extent, cuts, low, top_value):
    level = 1.0
    for position, shards_of in cuts:
        draws = jax.random.uniform(jax.random.fold_in(jax.random.fold_in(rng, 6), position), (shards_of,), jnp.float32, low / len(cuts), top_value / len(cuts))
        level = level * jnp.repeat(jnp.exp(draws), extent[position] // shards_of).reshape((-1,) + (1,) * (len(extent) - 1 - position))
    return level


def bell_draw(own_key, dims, scale, limit, cuts=(), kind=jnp.bfloat16):
    loudness = steps_of(own_key, dims, cuts, -0.22, 0.18) if cuts else 1.0
    drawn = jax.random.normal(own_key, dims, jnp.float32) * scale * loudness
    return jnp.minimum(jnp.maximum(drawn, -limit), limit).astype(kind)


def setup_inputs(seed: int = 0) -> dict:
    seeds = jax.random.split(jax.random.key(seed), 4)
    return {
        "pool_counts": draw_pool_counts(jax.random.fold_in(seeds[3], 71), 0),
        "cell_picks": draw_cell_picks(jax.random.fold_in(seeds[3], 71), 0),
        "loadings_init": bell_draw(seeds[2], (COMPS, GENES), GENES ** -0.5, 0.0390625, ((1, 64),), jnp.float32),
    }


step_rate = 1.0

def reference(pool_counts, cell_picks, loadings_init):
    loadings = loadings_init
    block_width = GENES // 8
    for step_index in range(STEPS):
        chosen = cell_picks[step_index]
        weights_low = loadings.astype(jnp.bfloat16)
        scores = jnp.zeros((COMPS, BATCH), jnp.float32)
        batch_means = []
        for block_index in range(8):
            lowest = block_index * block_width
            gathered = jnp.take(pool_counts[lowest:lowest + block_width], chosen, axis=1)
            means_part = lax.optimization_barrier(jnp.sum(gathered.astype(jnp.float32), axis=1)) / BATCH
            weight_part = weights_low[:, lowest:lowest + block_width]
            scores = scores + jnp.dot(weight_part.astype(jnp.float32), gathered.astype(jnp.float32), preferred_element_type=jnp.float32)
            shift = jnp.dot(weight_part.astype(jnp.float32), means_part, precision=lax.Precision.HIGHEST)
            scores = scores - shift[:, None]
            batch_means.append(means_part)
        scores_low = scores.astype(jnp.bfloat16)
        row_totals = lax.optimization_barrier(jnp.sum(scores_low.astype(jnp.float32), axis=1))
        updates = []
        for block_index in range(8):
            lowest = block_index * block_width
            gathered = jnp.take(pool_counts[lowest:lowest + block_width], chosen, axis=1)
            raw_update = lax.dot_general(scores_low.astype(jnp.float32), gathered.astype(jnp.float32), (((1,), (1,)), ((), ())), preferred_element_type=jnp.float32)
            updates.append((raw_update - row_totals[:, None] * batch_means[block_index][None, :]) / BATCH)
        update = jnp.concatenate(updates, axis=1)
        stepped = loadings + step_rate * update
        gram_matrix = jnp.dot(stepped, stepped.T, precision=lax.Precision.HIGHEST)
        factor = jnp.linalg.cholesky(gram_matrix)
        loadings = lax.linalg.triangular_solve(factor, stepped, left_side=True, lower=True)
    return loadings * math.sqrt(GENES)
```

```python
import math

import jax
import jax.numpy as jnp
from jax import lax
from jax.experimental import pallas as pl
from jax.experimental.pallas import tpu as pltpu
from jax.sharding import PartitionSpec as P

f32 = jnp.float32
bf16 = jnp.bfloat16
STEP_RATE = 1.0
HIGH = lax.Precision.HIGHEST
NT = (((1,), (1,)), ((), ()))
NN = (((1,), (0,)), ((), ()))


def vmem_call(kernel, outs, count, flops=0, name=None):
    spec = pl.BlockSpec(memory_space=pltpu.VMEM)
    return pl.pallas_call(
        kernel,
        out_shape=outs,
        in_specs=[spec] * count,
        out_specs=jax.tree.map(lambda _: spec, outs),
        cost_estimate=pl.CostEstimate(flops=flops, transcendentals=0, bytes_accessed=0),
        name=name,
    )


def split_pair(value):
    high = value.astype(bf16)
    low = (value - high.astype(f32)).astype(bf16)
    return jnp.concatenate([high, low], axis=0)


def pack_partial(stepped, tile, shift, out_ref):
    comps = stepped.shape[0]
    both = lax.dot_general(split_pair(stepped), tile, NT, preferred_element_type=f32)
    scores = both[:comps] + both[comps:]
    if shift is not None:
        scores = scores - shift
    gram = lax.dot_general(stepped, stepped, NT, precision=HIGH, preferred_element_type=f32)
    chunks = scores.shape[1] // 128
    for j in range(chunks):
        out_ref[pl.ds(j, comps, stride=chunks + 1), :] = scores[:, j * 128 : (j + 1) * 128]
    out_ref[pl.ds(chunks, comps, stride=chunks + 1), :] = jnp.concatenate(
        [gram, jnp.zeros((comps, 128 - comps), f32)], axis=1
    )


def first_kernel(loadings_ref, tile_ref, out_ref):
    pack_partial(loadings_ref[...], tile_ref[...], None, out_ref)


def stepped_from(parts, previous, inverse, genes, batch):
    comps = previous.shape[0]
    total = parts[0][...] + parts[1][...] + parts[2][...] + parts[3][...]
    mean = total[comps : comps + 1, :genes] * (1.0 / batch)
    next_mean = total[comps + 1 : comps + 2, :genes] * (1.0 / batch)
    rows = total[:comps, genes : genes + 1]
    update = (total[:comps, :genes] - rows * mean) * (1.0 / batch)
    stepped = previous + STEP_RATE * update
    if inverse is not None:
        stepped = lax.dot_general(inverse, stepped, NN, precision=HIGH, preferred_element_type=f32)
    return stepped, next_mean


def make_middle(batch, normalised):
    def kernel(a, b, c, d, previous_ref, *refs):
        inverse = refs[0][...] if normalised else None
        tile_ref, out_ref, stepped_ref = refs[-3:]
        genes = previous_ref.shape[1]
        stepped, mean = stepped_from((a, b, c, d), previous_ref[...], inverse, genes, batch)
        stepped_ref[...] = stepped
        shift = jnp.sum(stepped * mean, axis=1, keepdims=True)
        pack_partial(stepped, tile_ref[...], shift, out_ref)

    return kernel


def make_last(batch):
    def kernel(a, b, c, d, previous_ref, inverse_ref, gram_ref, stepped_ref):
        genes = previous_ref.shape[1]
        stepped, _ = stepped_from((a, b, c, d), previous_ref[...], inverse_ref[...], genes, batch)
        stepped_ref[...] = stepped
        gram = lax.dot_general(stepped, stepped, NT, precision=HIGH, preferred_element_type=f32)
        comps = stepped.shape[0]
        gram_ref[...] = jnp.concatenate([gram, jnp.zeros((comps, 128 - comps), f32)], axis=1)

    return kernel


def make_sum(count, rows):
    def kernel(in_ref, out_ref):
        for j in range(rows):
            total = jnp.sum(in_ref[pl.ds(j, count, stride=rows), :], axis=0, keepdims=True)
            out_ref[pl.ds(j, count, stride=rows), :] = jnp.broadcast_to(total, (count, 128))

    return kernel


def make_update(comps, rows):
    def kernel(in_ref, tile_ref, sums_ref, next_ref, out_ref):
        genes = tile_ref.shape[1]
        width = out_ref.shape[1]
        scores = jnp.concatenate(
            [in_ref[pl.ds(j, comps, stride=rows), :] for j in range(rows - 1)], axis=1
        )
        both = lax.dot_general(split_pair(scores), tile_ref[...], NN, preferred_element_type=f32)
        raw = both[:comps] + both[comps:]
        totals = jnp.sum(scores, axis=1, keepdims=True)
        out_ref[:comps, :] = jnp.concatenate(
            [raw, jnp.broadcast_to(totals, (comps, width - genes))], axis=1
        )
        pad = jnp.zeros((1, width - genes), f32)
        out_ref[comps : comps + 1, :] = jnp.concatenate([sums_ref[...], pad], axis=1)
        out_ref[comps + 1 : comps + 2, :] = jnp.concatenate([next_ref[...], pad], axis=1)
        out_ref[comps + 2 :, :] = jnp.zeros((out_ref.shape[0] - comps - 2, width), f32)

    return kernel


def inverse_factor(gram):
    size = gram.shape[0]
    rows = lax.broadcasted_iota(jnp.int32, (8, 2 * size), 0)
    lanes = lax.broadcasted_iota(jnp.int32, (8, 2 * size), 1)
    blocks = []
    for b in range(size // 8):
        eye = jnp.where(lanes == rows + (b * 8 + size), 1.0, 0.0).astype(f32)
        left = jnp.concatenate([gram[b * 8 : b * 8 + 8, :], jnp.zeros((8, size), f32)], axis=1)
        blocks.append(left + eye)
    scale = [jnp.zeros((8, 1), f32) for _ in blocks]
    for k in range(size):
        b, r = divmod(k, 8)
        row = blocks[b][r : r + 1, :]
        pivot = blocks[b][r : r + 1, k : k + 1]
        scaled = row / pivot
        scale[b] = jnp.where(rows[:, :1] == r, lax.rsqrt(pivot), scale[b])
        for i in range(b, size // 8):
            column = blocks[i][:, k : k + 1]
            if i == b:
                column = jnp.where(rows[:, :1] > r, column, 0.0)
            blocks[i] = blocks[i] - column * scaled
    return jnp.concatenate([m * s for m, s in zip(blocks, scale)], axis=0)[:, size:]


def make_factor(comps, rows):
    def kernel(in_ref, out_ref):
        gram = in_ref[pl.ds(rows - 1, comps, stride=rows), :][:, :comps]
        out_ref[...] = inverse_factor(gram)

    return kernel


def make_finish(scale):
    def kernel(in_ref, stepped_ref, out_ref):
        comps = stepped_ref.shape[0]
        inverse = inverse_factor(in_ref[:, :comps])
        out_ref[...] = scale * lax.dot_general(
            inverse, stepped_ref[...], NN, precision=HIGH, preferred_element_type=f32
        )

    return kernel


def shards(pool_counts, cell_picks, loadings_init):
    comps, genes = loadings_init.shape
    steps, cells = cell_picks.shape
    local_pool = pool_counts.shape[1]
    gene_devices = lax.axis_size("gene")
    cell_devices = lax.axis_size("cell")
    batch = cells * cell_devices
    rows = cells // 128 + 1
    width = genes + 128 - genes % 128
    group = lax.axis_index("cell")
    chosen = cell_picks - group * local_pool
    pool_by_cell = pool_counts.T

    def tile_of(step):
        return jnp.take(pool_by_cell, chosen[step], axis=0, mode="clip")

    def sums_of(tile):
        return jnp.sum(tile, axis=0, dtype=f32, keepdims=True)

    def exchange(value):
        pieces = value.reshape(gene_devices, 1, value.shape[0] // gene_devices * 128)
        arrived = lax.all_to_all(pieces, "gene", 0, 0, tiled=True)
        return arrived.reshape(value.shape)

    def reduced(value):
        count = value.shape[0] // gene_devices
        shape = jax.ShapeDtypeStruct(value.shape, f32)
        copies = vmem_call(make_sum(gene_devices, count), shape, 1, name="add_up")(exchange(value))
        return exchange(copies)

    packed = jax.ShapeDtypeStruct((comps * rows, 128), f32)
    square = jax.ShapeDtypeStruct((comps, comps), f32)
    local = jax.ShapeDtypeStruct((comps, genes), f32)
    shared = jax.ShapeDtypeStruct((comps + 8, width), f32)

    tile = tile_of(0)
    sums = sums_of(tile)
    stepped = loadings_init
    inverse = None
    partial = vmem_call(first_kernel, packed, 2, name="first")(loadings_init, tile)
    for step in range(steps):
        if step + 1 < steps:
            next_tile = tile_of(step + 1)
            next_sums = sums_of(next_tile)
        else:
            next_tile, next_sums = tile, sums
        everything = reduced(partial)
        mine = vmem_call(make_update(comps, rows), shared, 4, name="update")(
            everything, tile, sums, next_sums
        )
        parts = [mine] + [
            lax.ppermute(mine, "cell", [(i, (i + k) % cell_devices) for i in range(cell_devices)])
            for k in range(1, cell_devices)
        ]
        inputs = [*parts, stepped]
        if step > 0:
            inverse = vmem_call(make_factor(comps, rows), square, 1, flops=10**9, name="factor")(everything)
            inputs.append(inverse)
        if step + 1 < steps:
            inputs.append(next_tile)
            partial, stepped = vmem_call(
                make_middle(batch, step > 0), (packed, local), len(inputs), name="middle"
            )(*inputs)
            tile, sums = next_tile, next_sums
        else:
            gram, stepped = vmem_call(
                make_last(batch), (jax.ShapeDtypeStruct((comps, 128), f32), local), len(inputs), name="last"
            )(*inputs)
    gram = reduced(gram)
    scale = math.sqrt(genes * gene_devices)
    return vmem_call(make_finish(scale), local, 2, name="finish")(gram, stepped)


def solution(mesh):
    placed = (P("gene", "cell"), P(None, "cell"), P(None, "gene"))
    return jax.shard_map(
        shards, mesh=mesh, in_specs=placed, out_specs=P(None, "gene"), check_vma=False
    )
```

```python
import math

import jax
import jax.numpy as jnp
from jax import lax
from jax.experimental import pallas as pl
from jax.experimental.pallas import tpu as pltpu
from jax.sharding import PartitionSpec as P

f32 = jnp.float32
bf16 = jnp.bfloat16
STEP_RATE = 1.0
HIGH = lax.Precision.HIGHEST
NT = (((1,), (1,)), ((), ()))
NN = (((1,), (0,)), ((), ()))


def vmem_call(kernel, outs, count, flops=0, name=None, core=True):
    spec = pl.BlockSpec(memory_space=pltpu.VMEM)
    call = pl.pallas_call(
        kernel,
        out_shape=jax.tree.map(lambda s: pltpu.VMEM(s.shape, s.dtype), outs),
        in_specs=[pl.BlockSpec(memory_space=pltpu.SMEM)] * core + [spec] * count,
        out_specs=jax.tree.map(lambda _: spec, outs),
        cost_estimate=pl.CostEstimate(flops=flops, transcendentals=0, bytes_accessed=0),
        name=name,
    )

    def run(*args):
        held = [pltpu.with_memory_space_constraint(a, pltpu.VMEM) for a in args[core:]]
        return call(*args[:core], *held)

    return run


def split_pair(value):
    high = value.astype(bf16)
    low = (value - high.astype(f32)).astype(bf16)
    return jnp.concatenate([high, low], axis=0)


def gram_of(stepped):
    return lax.dot_general(stepped, stepped, NT, precision=HIGH, preferred_element_type=f32)


def by_core(first, mine, other):
    return jnp.concatenate([jnp.where(first, mine, other), jnp.where(first, other, mine)], axis=0)


def pack_partial(stepped, tile, shift, first, keep_ref, send_ref):
    comps = stepped.shape[0]
    half = comps // 2
    both = lax.dot_general(split_pair(stepped), tile, NT, preferred_element_type=f32)
    scores = both[:comps] + both[comps:]
    if shift is not None:
        scores = scores - shift
    gram = jnp.concatenate([gram_of(stepped), jnp.zeros((comps, 128 - comps), f32)], axis=1)
    rows = scores.shape[1] // 128 + 1
    for j in range(rows):
        chunk = scores[:, j * 128 : (j + 1) * 128] if j + 1 < rows else gram
        top, bottom = chunk[:half], chunk[half:]
        keep_ref[pl.ds(j, half, stride=rows), :] = jnp.where(first, top, bottom)
        send_ref[pl.ds(j, half, stride=rows), :] = jnp.where(first, bottom, top)


def first_kernel(core_ref, loadings_ref, tile_ref, keep_ref, send_ref):
    pack_partial(loadings_ref[...], tile_ref[...], None, core_ref[0] == 0, keep_ref, send_ref)


def stepped_from(parts, previous, inverse, batch):
    comps, genes = previous.shape
    total = sum(part[:comps, :genes].astype(f32) for part in parts)
    stepped = previous + STEP_RATE * (total * (1.0 / batch))
    if inverse is not None:
        stepped = lax.dot_general(inverse, stepped, NN, precision=HIGH, preferred_element_type=f32)
    return stepped


def make_middle(batch, normalised):
    def kernel(core_ref, a, b, c, d, previous_ref, *refs):
        inverse = refs[0][...] if normalised else None
        tile_ref, keep_ref, send_ref, stepped_ref, mean_ref = refs[-5:]
        comps, genes = previous_ref.shape
        parts = (a, b, c, d)
        stepped = stepped_from(parts, previous_ref[...], inverse, batch)
        stepped_ref[...] = stepped
        sums = sum(part[comps : comps + 2, :genes].astype(f32) for part in parts)
        mean = (sums[:1] + sums[1:]) * (1.0 / batch)
        mean_ref[...] = mean
        shift = jnp.sum(stepped * mean, axis=1, keepdims=True)
        pack_partial(stepped, tile_ref[...], shift, core_ref[0] == 0, keep_ref, send_ref)

    return kernel


def make_last(batch):
    def kernel(a, b, c, d, previous_ref, inverse_ref, gram_ref, stepped_ref):
        stepped = stepped_from((a, b, c, d), previous_ref[...], inverse_ref[...], batch)
        stepped_ref[...] = stepped
        gram = gram_of(stepped)
        half = gram.shape[0] // 2
        gram_ref[...] = jnp.concatenate([gram[:half], gram[half:]], axis=1)

    return kernel


def make_sum(count, rows):
    def kernel(in_ref, out_ref):
        for j in range(rows):
            total = jnp.sum(in_ref[pl.ds(j, count, stride=rows), :], axis=0, keepdims=True)
            out_ref[pl.ds(j, count, stride=rows), :] = jnp.broadcast_to(total, (count, 128))

    return kernel


def make_update(half, rows):
    def kernel(core_ref, mine_ref, other_ref, tile_ref, mean_ref, next_ref, out_ref):
        genes = tile_ref.shape[1]
        comps = 2 * half
        width = out_ref.shape[1]
        chunks = [
            by_core(
                core_ref[0] == 0,
                mine_ref[pl.ds(j, half, stride=rows), :],
                other_ref[pl.ds(j, half, stride=rows), :],
            )
            for j in range(rows - 1)
        ]
        scores = jnp.concatenate(chunks, axis=1)
        both = lax.dot_general(split_pair(scores), tile_ref[...], NN, preferred_element_type=f32)
        totals = jnp.sum(scores, axis=1, keepdims=True)
        raw = both[:comps] + both[comps:] - totals * mean_ref[...]
        rest = out_ref.shape[0] - comps - 2
        tall = jnp.concatenate(
            [raw.astype(bf16), split_pair(next_ref[...]), jnp.zeros((rest, genes), bf16)], axis=0
        )
        out_ref[...] = jnp.concatenate([tall, jnp.zeros((tall.shape[0], width - genes), bf16)], axis=1)

    return kernel


def inverse_factor(gram):
    size = gram.shape[0]
    shape = (8, 2 * size)
    rows = lax.broadcasted_iota(jnp.int32, shape, 0)
    lanes = lax.broadcasted_iota(jnp.int32, shape, 1)
    blocks = []
    for b in range(size // 8):
        eye = jnp.where(lanes == rows + (b * 8 + size), 1.0, 0.0).astype(f32)
        left = jnp.concatenate([gram[b * 8 : b * 8 + 8, :], jnp.zeros((8, size), f32)], axis=1)
        blocks.append(left + eye)
    results = list(blocks)
    for k in range(0, size, 2):
        b, r = divmod(k, 8)
        upper = blocks[b][r : r + 1, :]
        lower = blocks[b][r + 1 : r + 2, :]
        columns = [
            tuple(jnp.broadcast_to(blocks[i][:, k + h : k + h + 1], shape) for h in range(2))
            for i in range(b, size // 8)
        ]
        p = columns[0][0][r : r + 1, :]
        q = columns[0][0][r + 1 : r + 2, :]
        t = columns[0][1][r + 1 : r + 2, :]
        over = 1.0 / (p * t - q * q)
        first = (t * upper - q * lower) * over
        second = (p * lower - q * upper) * over
        inverse_p = 1.0 / p
        slope = q * inverse_p
        top = upper * lax.rsqrt(p)
        low = (lower - slope * upper) * lax.rsqrt(t - slope * q)
        results[b] = jnp.where(rows == r, top, jnp.where(rows == r + 1, low, results[b]))
        for i in range(b, size // 8):
            x, y = columns[i - b]
            change = x * first + y * second
            if i == b:
                change = jnp.where(rows > r + 1, change, 0.0)
            blocks[i] = blocks[i] - change
    return jnp.concatenate(results, axis=0)[:, size:]


def make_factor(half, rows):
    def kernel(core_ref, mine_ref, other_ref, out_ref):
        gram = by_core(
            core_ref[0] == 0,
            mine_ref[pl.ds(rows - 1, half, stride=rows), :],
            other_ref[pl.ds(rows - 1, half, stride=rows), :],
        )
        out_ref[...] = inverse_factor(gram[:, : 2 * half])

    return kernel


def make_finish(scale):
    def kernel(in_ref, stepped_ref, out_ref):
        comps = stepped_ref.shape[0]
        total = jnp.sum(in_ref[...], axis=0)
        gram = jnp.concatenate([total[:, :comps], total[:, comps:]], axis=0)
        out_ref[...] = scale * lax.dot_general(
            inverse_factor(gram), stepped_ref[...], NN, precision=HIGH, preferred_element_type=f32
        )

    return kernel


def shards(pool_counts, cell_picks, loadings_init):
    comps, genes = loadings_init.shape
    steps, cells = cell_picks.shape
    half = comps // 2
    local_pool = pool_counts.shape[1]
    cell_devices = lax.axis_size("cell")
    gene_devices = lax.axis_size("gene")
    chips = gene_devices // 2
    batch = cells * cell_devices
    rows = cells // 128 + 1
    width = genes + 128 - genes % 128
    core = (lax.axis_index("gene") % 2).astype(jnp.int32).reshape(1)
    chosen = cell_picks - lax.axis_index("cell") * local_pool
    pool_by_cell = pool_counts.T
    same_core = [[2 * chip + which for chip in range(chips)] for which in range(2)]

    def tile_of(step):
        return jnp.take(pool_by_cell, chosen[step], axis=0, mode="clip")

    def sums_of(tile):
        return jnp.sum(tile, axis=0, dtype=f32, keepdims=True)

    def swap_cores(value):
        return lax.ppermute(value, "gene", [(i, i ^ 1) for i in range(gene_devices)])

    def round_cells(value):
        return [value] + [
            lax.ppermute(value, "cell", [(i, (i + k) % cell_devices) for i in range(cell_devices)])
            for k in range(1, cell_devices)
        ]

    def exchange(value):
        pieces = value.reshape(chips, 1, value.size // chips)
        arrived = lax.all_to_all(pieces, "gene", 0, 0, tiled=True, axis_index_groups=same_core)
        return arrived.reshape(value.shape)

    packed = jax.ShapeDtypeStruct((half * rows, 128), f32)
    square = jax.ShapeDtypeStruct((comps, comps), f32)
    local = jax.ShapeDtypeStruct((comps, genes), f32)
    row = jax.ShapeDtypeStruct((1, genes), f32)
    shared = jax.ShapeDtypeStruct((comps + 8, width), bf16)

    tile = tile_of(0)
    mean = sum(round_cells(sums_of(tile))) * (1.0 / batch)
    stepped = loadings_init
    keep, send = vmem_call(first_kernel, (packed, packed), 2, name="first")(core, loadings_init, tile)
    for step in range(steps):
        more = step + 1 < steps
        next_tile = tile_of(step + 1) if more else tile
        next_sums = sums_of(next_tile) if more else mean
        chip_sum = keep + swap_cores(send)
        copies = vmem_call(make_sum(chips, rows), packed, 1, name="add_up", core=False)(exchange(chip_sum))
        mine = exchange(copies)
        other = swap_cores(mine)
        change = vmem_call(make_update(half, rows), shared, 5, name="update")(
            core, mine, other, tile, mean, next_sums
        )
        inputs = [*round_cells(change), stepped]
        if step > 0:
            inputs.append(
                vmem_call(make_factor(half, rows), square, 2, flops=10**9, name="factor")(core, mine, other)
            )
        if more:
            inputs.append(next_tile)
            keep, send, stepped, mean = vmem_call(
                make_middle(batch, step > 0), (packed, packed, local, row), len(inputs), name="middle"
            )(core, *inputs)
            tile = next_tile
        else:
            gram, stepped = vmem_call(
                make_last(batch),
                (jax.ShapeDtypeStruct((half, 2 * comps), f32), local),
                len(inputs),
                name="last",
                core=False,
            )(*inputs)
    gram = gram + swap_cores(gram)
    depth = 8
    planes = chips // depth
    gram = sum(
        [gram]
        + [
            lax.ppermute(gram, "gene", [(i, (i + k * 2 * depth) % gene_devices) for i in range(gene_devices)])
            for k in range(1, planes)
        ]
    )
    columns = [
        [(plane * depth + level) * 2 + which for level in range(depth)]
        for plane in range(planes)
        for which in range(2)
    ]
    grams = lax.all_to_all(
        jnp.broadcast_to(gram[None], (depth, *gram.shape)), "gene", 0, 0, tiled=True, axis_index_groups=columns
    )
    scale = math.sqrt(genes * gene_devices)
    return vmem_call(make_finish(scale), local, 2, name="finish", core=False)(grams, stepped)


def solution(mesh):
    placed = (P("gene", "cell"), P(None, "cell"), P(None, "gene"))
    return jax.shard_map(
        shards, mesh=mesh, in_specs=placed, out_specs=P(None, "gene"), check_vma=False
    )
```

```python
import math

import jax
import jax.numpy as jnp
from jax import lax
from jax.experimental import pallas as pl
from jax.experimental.pallas import tpu as pltpu
from jax.sharding import PartitionSpec as P

f32 = jnp.float32
bf16 = jnp.bfloat16
STEP_RATE = 1.0
HIGH = lax.Precision.HIGHEST
NT = (((1,), (1,)), ((), ()))
NN = (((1,), (0,)), ((), ()))


def vmem_call(kernel, outs, count, flops=0, name=None, core=True):
    spec = pl.BlockSpec(memory_space=pltpu.VMEM)
    call = pl.pallas_call(
        kernel,
        out_shape=jax.tree.map(lambda s: pltpu.VMEM(s.shape, s.dtype), outs),
        in_specs=[pl.BlockSpec(memory_space=pltpu.SMEM)] * core + [spec] * count,
        out_specs=jax.tree.map(lambda _: spec, outs),
        cost_estimate=pl.CostEstimate(flops=flops, transcendentals=0, bytes_accessed=0),
        name=name,
    )

    def run(*args):
        held = [pltpu.with_memory_space_constraint(a, pltpu.VMEM) for a in args[core:]]
        return call(*args[:core], *held)

    return run


def split_pair(value):
    high = value.astype(bf16)
    low = (value - high.astype(f32)).astype(bf16)
    return jnp.concatenate([high, low], axis=0)


def gram_of(stepped):
    return lax.dot_general(stepped, stepped, NT, precision=HIGH, preferred_element_type=f32)


def by_core(first, mine, other):
    return jnp.concatenate([jnp.where(first, mine, other), jnp.where(first, other, mine)], axis=0)


def pack_partial(stepped, tile, shift, first, keep_ref, send_ref):
    comps = stepped.shape[0]
    half = comps // 2
    both = lax.dot_general(split_pair(stepped), tile, NT, preferred_element_type=f32)
    scores = both[:comps] + both[comps:]
    if shift is not None:
        scores = scores - shift
    gram = jnp.concatenate([gram_of(stepped), jnp.zeros((comps, 128 - comps), f32)], axis=1)
    rows = scores.shape[1] // 128 + 1
    for j in range(rows):
        chunk = scores[:, j * 128 : (j + 1) * 128] if j + 1 < rows else gram
        top, bottom = chunk[:half], chunk[half:]
        keep_ref[pl.ds(j, half, stride=rows), :] = jnp.where(first, top, bottom)
        send_ref[pl.ds(j, half, stride=rows), :] = jnp.where(first, bottom, top)


def first_kernel(core_ref, loadings_ref, tile_ref, keep_ref, send_ref):
    pack_partial(loadings_ref[...], tile_ref[...], None, core_ref[0] == 0, keep_ref, send_ref)


def stepped_from(parts, previous, inverse, batch):
    comps, genes = previous.shape
    total = sum(part[:comps, :genes].astype(f32) for part in parts)
    stepped = previous + STEP_RATE * (total * (1.0 / batch))
    if inverse is not None:
        stepped = lax.dot_general(inverse, stepped, NN, precision=HIGH, preferred_element_type=f32)
    return stepped


def make_middle(batch, normalised):
    def kernel(core_ref, a, b, c, d, previous_ref, *refs):
        inverse = refs[0][...] if normalised else None
        tile_ref, keep_ref, send_ref, stepped_ref, mean_ref = refs[-5:]
        comps, genes = previous_ref.shape
        parts = (a, b, c, d)
        stepped = stepped_from(parts, previous_ref[...], inverse, batch)
        stepped_ref[...] = stepped
        sums = sum(part[comps : comps + 2, :genes].astype(f32) for part in parts)
        mean = (sums[:1] + sums[1:]) * (1.0 / batch)
        mean_ref[...] = mean
        shift = jnp.sum(stepped * mean, axis=1, keepdims=True)
        pack_partial(stepped, tile_ref[...], shift, core_ref[0] == 0, keep_ref, send_ref)

    return kernel


def make_last(batch):
    def kernel(a, b, c, d, previous_ref, inverse_ref, gram_ref, stepped_ref):
        stepped = stepped_from((a, b, c, d), previous_ref[...], inverse_ref[...], batch)
        stepped_ref[...] = stepped
        gram = gram_of(stepped)
        half = gram.shape[0] // 2
        gram_ref[...] = jnp.concatenate([gram[:half], gram[half:]], axis=1)

    return kernel


def make_sum(count, rows):
    def kernel(in_ref, out_ref):
        for j in range(rows):
            total = jnp.sum(in_ref[pl.ds(j, count, stride=rows), :], axis=0, keepdims=True)
            out_ref[pl.ds(j, count, stride=rows), :] = jnp.broadcast_to(total, (count, 128))

    return kernel


def make_update(half, rows):
    def kernel(core_ref, mine_ref, other_ref, tile_ref, mean_ref, next_ref, out_ref):
        genes = tile_ref.shape[1]
        comps = 2 * half
        width = out_ref.shape[1]
        chunks = [
            by_core(
                core_ref[0] == 0,
                mine_ref[pl.ds(j, half, stride=rows), :],
                other_ref[pl.ds(j, half, stride=rows), :],
            )
            for j in range(rows - 1)
        ]
        scores = jnp.concatenate(chunks, axis=1)
        both = lax.dot_general(split_pair(scores), tile_ref[...], NN, preferred_element_type=f32)
        totals = jnp.sum(scores, axis=1, keepdims=True)
        raw = both[:comps] + both[comps:] - totals * mean_ref[...]
        rest = out_ref.shape[0] - comps - 2
        tall = jnp.concatenate(
            [raw.astype(bf16), split_pair(next_ref[...]), jnp.zeros((rest, genes), bf16)], axis=0
        )
        out_ref[...] = jnp.concatenate([tall, jnp.zeros((tall.shape[0], width - genes), bf16)], axis=1)

    return kernel


def inverse_factor(gram):
    size = gram.shape[0]
    shape = (8, 2 * size)
    rows = lax.broadcasted_iota(jnp.int32, shape, 0)
    lanes = lax.broadcasted_iota(jnp.int32, shape, 1)
    blocks = []
    for b in range(size // 8):
        eye = jnp.where(lanes == rows + (b * 8 + size), 1.0, 0.0).astype(f32)
        left = jnp.concatenate([gram[b * 8 : b * 8 + 8, :], jnp.zeros((8, size), f32)], axis=1)
        blocks.append(left + eye)
    results = list(blocks)
    for k in range(0, size, 2):
        b, r = divmod(k, 8)
        upper = blocks[b][r : r + 1, :]
        lower = blocks[b][r + 1 : r + 2, :]
        columns = [
            tuple(jnp.broadcast_to(blocks[i][:, k + h : k + h + 1], shape) for h in range(2))
            for i in range(b, size // 8)
        ]
        p = columns[0][0][r : r + 1, :]
        q = columns[0][0][r + 1 : r + 2, :]
        t = columns[0][1][r + 1 : r + 2, :]
        over = 1.0 / (p * t - q * q)
        first = (t * upper - q * lower) * over
        second = (p * lower - q * upper) * over
        inverse_p = 1.0 / p
        slope = q * inverse_p
        top = upper * lax.rsqrt(p)
        low = (lower - slope * upper) * lax.rsqrt(t - slope * q)
        results[b] = jnp.where(rows == r, top, jnp.where(rows == r + 1, low, results[b]))
        for i in range(b, size // 8):
            x, y = columns[i - b]
            change = x * first + y * second
            if i == b:
                change = jnp.where(rows > r + 1, change, 0.0)
            blocks[i] = blocks[i] - change
    return jnp.concatenate(results, axis=0)[:, size:]


def make_factor(half, rows):
    def kernel(core_ref, mine_ref, other_ref, out_ref):
        gram = by_core(
            core_ref[0] == 0,
            mine_ref[pl.ds(rows - 1, half, stride=rows), :],
            other_ref[pl.ds(rows - 1, half, stride=rows), :],
        )
        out_ref[...] = inverse_factor(gram[:, : 2 * half])

    return kernel


def make_finish(scale):
    def kernel(in_ref, stepped_ref, out_ref):
        comps = stepped_ref.shape[0]
        total = jnp.sum(in_ref[...], axis=0)
        gram = jnp.concatenate([total[:, :comps], total[:, comps:]], axis=0)
        out_ref[...] = scale * lax.dot_general(
            inverse_factor(gram), stepped_ref[...], NN, precision=HIGH, preferred_element_type=f32
        )

    return kernel


def shards(pool_counts, cell_picks, loadings_init):
    comps, genes = loadings_init.shape
    steps, cells = cell_picks.shape
    half = comps // 2
    local_pool = pool_counts.shape[1]
    cell_devices = lax.axis_size("cell")
    gene_devices = lax.axis_size("gene")
    chips = gene_devices // 2
    batch = cells * cell_devices
    rows = cells // 128 + 1
    width = genes + 128 - genes % 128
    core = (lax.axis_index("gene") % 2).astype(jnp.int32).reshape(1)
    chosen = cell_picks - lax.axis_index("cell") * local_pool
    pool_by_cell = pool_counts.T
    same_core = [[2 * chip + which for chip in range(chips)] for which in range(2)]

    def tile_of(step):
        return jnp.take(pool_by_cell, chosen[step], axis=0, mode="clip")

    def sums_of(tile):
        return jnp.sum(tile, axis=0, dtype=f32, keepdims=True)

    def swap_cores(value):
        return lax.ppermute(value, "gene", [(i, i ^ 1) for i in range(gene_devices)])

    def round_cells(value):
        return [value] + [
            lax.ppermute(value, "cell", [(i, (i + k) % cell_devices) for i in range(cell_devices)])
            for k in range(1, cell_devices)
        ]

    def exchange(value):
        pieces = value.reshape(chips, 1, value.size // chips)
        arrived = lax.all_to_all(pieces, "gene", 0, 0, tiled=True, axis_index_groups=same_core)
        return arrived.reshape(value.shape)

    packed = jax.ShapeDtypeStruct((half * rows, 128), f32)
    square = jax.ShapeDtypeStruct((comps, comps), f32)
    local = jax.ShapeDtypeStruct((comps, genes), f32)
    row = jax.ShapeDtypeStruct((1, genes), f32)
    shared = jax.ShapeDtypeStruct((comps + 8, width), bf16)

    tile = tile_of(0)
    mean = sum(round_cells(sums_of(tile))) * (1.0 / batch)
    keep, send = vmem_call(first_kernel, (packed, packed), 2, name="first")(core, loadings_init, tile)

    def scores_of(keep, send):
        chip_sum = keep + swap_cores(send)
        copies = vmem_call(make_sum(chips, rows), packed, 1, name="add_up", core=False)(exchange(chip_sum))
        mine = exchange(copies)
        return mine, swap_cores(mine)

    def change_of(mine, other, tile, mean, next_sums):
        change = vmem_call(make_update(half, rows), shared, 5, name="update")(
            core, mine, other, tile, mean, next_sums
        )
        return round_cells(change)

    def factor_of(mine, other):
        return vmem_call(make_factor(half, rows), square, 2, flops=10**9, name="factor")(core, mine, other)

    def advance(parts, stepped, inverse, next_tile):
        inputs = [*parts, stepped, *inverse, next_tile]
        return vmem_call(
            make_middle(batch, bool(inverse)), (packed, packed, local, row), len(inputs), name="middle"
        )(core, *inputs)

    def one_step(step, state):
        keep, send, stepped, mean, tile = state
        next_tile = tile_of(step + 1)
        mine, other = scores_of(keep, send)
        parts = change_of(mine, other, tile, mean, sums_of(next_tile))
        inverse = (factor_of(mine, other),)
        return (*advance(parts, stepped, inverse, next_tile), next_tile)

    next_tile = tile_of(1)
    mine, other = scores_of(keep, send)
    parts = change_of(mine, other, tile, mean, sums_of(next_tile))
    state = (*advance(parts, loadings_init, (), next_tile), next_tile)
    keep, send, stepped, mean, tile = lax.fori_loop(1, steps - 1, one_step, state)
    mine, other = scores_of(keep, send)
    parts = change_of(mine, other, tile, mean, mean)
    inverse = factor_of(mine, other)
    gram, stepped = vmem_call(
        make_last(batch),
        (jax.ShapeDtypeStruct((half, 2 * comps), f32), local),
        len(parts) + 2,
        name="last",
        core=False,
    )(*parts, stepped, inverse)
    gram = gram + swap_cores(gram)
    depth = 8
    planes = chips // depth
    gram = sum(
        [gram]
        + [
            lax.ppermute(gram, "gene", [(i, (i + k * 2 * depth) % gene_devices) for i in range(gene_devices)])
            for k in range(1, planes)
        ]
    )
    columns = [
        [(plane * depth + level) * 2 + which for level in range(depth)]
        for plane in range(planes)
        for which in range(2)
    ]
    grams = lax.all_to_all(
        jnp.broadcast_to(gram[None], (depth, *gram.shape)), "gene", 0, 0, tiled=True, axis_index_groups=columns
    )
    scale = math.sqrt(genes * gene_devices)
    return vmem_call(make_finish(scale), local, 2, name="finish", core=False)(grams, stepped)


def solution(mesh):
    placed = (P("gene", "cell"), P(None, "cell"), P(None, "gene"))
    return jax.shard_map(
        shards, mesh=mesh, in_specs=placed, out_specs=P(None, "gene"), check_vma=False
    )
```

```python
import math

import jax
import jax.numpy as jnp
from jax import lax
from jax.experimental import pallas as pl
from jax.experimental.pallas import tpu as pltpu
from jax.sharding import PartitionSpec as P

f32 = jnp.float32
bf16 = jnp.bfloat16
STEP_RATE = 1.0
DEPTH = 8
HIGH = lax.Precision.HIGHEST
NT = (((1,), (1,)), ((), ()))
NN = (((1,), (0,)), ((), ()))


def vmem_call(kernel, outs, count, flops=0, name=None, place=True, scratch=()):
    spec = pl.BlockSpec(memory_space=pltpu.VMEM)
    call = pl.pallas_call(
        kernel,
        out_shape=jax.tree.map(lambda s: pltpu.VMEM(s.shape, s.dtype), outs),
        in_specs=[pl.BlockSpec(memory_space=pltpu.SMEM)] * place + [spec] * count,
        out_specs=jax.tree.map(lambda _: spec, outs),
        cost_estimate=pl.CostEstimate(flops=flops, transcendentals=0, bytes_accessed=0),
        scratch_shapes=scratch,
        name=name,
    )

    def run(*args):
        held = [pltpu.with_memory_space_constraint(a, pltpu.VMEM) for a in args[place:]]
        return call(*args[:place], *held)

    return run


def split_pair(value):
    high = value.astype(bf16)
    low = (value - high.astype(f32)).astype(bf16)
    return jnp.concatenate([high, low], axis=0)


def gram_of(stepped):
    return lax.dot_general(stepped, stepped, NT, precision=HIGH, preferred_element_type=f32)


def pack_partial(stepped, tile, shift, first, keep_ref, send_ref):
    comps = stepped.shape[0]
    half = comps // 2
    both = lax.dot_general(split_pair(stepped), tile, NT, preferred_element_type=f32)
    scores = both[:comps] + both[comps:]
    if shift is not None:
        scores = scores - shift
    gram = jnp.concatenate([gram_of(stepped), jnp.zeros((comps, 128 - comps), f32)], axis=1)
    tiles = scores.shape[1] // 128 + 1
    for j in range(tiles):
        chunk = scores[:, j * 128 : (j + 1) * 128] if j + 1 < tiles else gram
        mine = jnp.where(first, chunk[:half], chunk[half:])
        other = jnp.where(first, chunk[half:], chunk[:half])
        for group in range(half // 8):
            start = (group * tiles + j) * 8
            keep_ref[start : start + 8, :] = mine[group * 8 : group * 8 + 8]
            send_ref[start : start + 8, :] = other[group * 8 : group * 8 + 8]


def first_kernel(place_ref, loadings_ref, tile_ref, keep_ref, send_ref):
    pack_partial(loadings_ref[...], tile_ref[...], None, place_ref[0] == 0, keep_ref, send_ref)


def pair_kernel(place_ref, keep_ref, came_ref, *out_refs):
    planes = len(out_refs)
    size = out_refs[0].shape[0]
    for k, out_ref in enumerate(out_refs):
        start = pl.multiple_of(lax.rem(place_ref[1] + k, planes) * size, 8)
        out_ref[...] = keep_ref[pl.ds(start, size), :] + came_ref[pl.ds(start, size), :]


def plane_kernel(a, b, c, d, out_ref):
    total = a[...] + b[...] + c[...] + d[...]
    rows = total.shape[0] - 8
    gram = total[rows:, :64]
    high = gram.astype(bf16)
    rest = gram - high.astype(f32)
    middle = rest.astype(bf16)
    low = (rest - middle.astype(f32)).astype(bf16)
    parts = jnp.concatenate(
        [jnp.concatenate([high, middle], axis=1), jnp.concatenate([low, low], axis=1)], axis=0
    )
    for copy in range(out_ref.shape[0]):
        out_ref[copy, :rows, :] = total[:rows].astype(bf16)
        out_ref[copy, rows:, :] = parts


def column_kernel(in_ref, out_ref):
    total = jnp.sum(in_ref[...].astype(f32), axis=0)
    rows = out_ref.shape[0] - 8
    out_ref[:rows, :] = total[:rows]
    gram = total[rows : rows + 8, :64] + (total[rows : rows + 8, 64:] + total[rows + 8 :, :64])
    out_ref[rows:, :] = jnp.concatenate([gram, jnp.zeros((8, 64), f32)], axis=1)


def stepped_from(parts, previous, inverse, batch):
    comps, genes = previous.shape
    total = sum(part[:comps, :genes].astype(f32) for part in parts)
    stepped = previous + STEP_RATE * (total * (1.0 / batch))
    if inverse is not None:
        stepped = lax.dot_general(inverse, stepped, NN, precision=HIGH, preferred_element_type=f32)
    return stepped


def make_middle(batch, normalised):
    def kernel(place_ref, a, b, c, d, previous_ref, *refs):
        inverse = refs[0][...] if normalised else None
        tile_ref, keep_ref, send_ref, stepped_ref, mean_ref = refs[-5:]
        comps, genes = previous_ref.shape
        parts = (a, b, c, d)
        stepped = stepped_from(parts, previous_ref[...], inverse, batch)
        stepped_ref[...] = stepped
        sums = sum(part[comps : comps + 2, :genes].astype(f32) for part in parts)
        mean = (sums[:1] + sums[1:]) * (1.0 / batch)
        mean_ref[...] = mean
        shift = jnp.sum(stepped * mean, axis=1, keepdims=True)
        pack_partial(stepped, tile_ref[...], shift, place_ref[0] == 0, keep_ref, send_ref)

    return kernel


def make_last(batch):
    def kernel(a, b, c, d, previous_ref, inverse_ref, gram_ref, stepped_ref):
        stepped = stepped_from((a, b, c, d), previous_ref[...], inverse_ref[...], batch)
        stepped_ref[...] = stepped
        gram = gram_of(stepped)
        half = gram.shape[0] // 2
        gram_ref[...] = jnp.concatenate([gram[:half], gram[half:]], axis=1)

    return kernel


def update_kernel(place_ref, *refs):
    *piece_refs, tile_ref, mean_ref, next_ref, out_ref, gram_ref, work_ref = refs
    genes = tile_ref.shape[1]
    width = out_ref.shape[1]
    planes = len(piece_refs) // 2
    size = piece_refs[0].shape[0]
    tiles = size // 8
    for h in range(2):
        which = place_ref[0] if h == 0 else 1 - place_ref[0]
        for k in range(planes):
            group = which * planes + lax.rem(place_ref[1] + (planes - k), planes)
            start = pl.multiple_of(group * size, 8)
            work_ref[pl.ds(start, size), :] = piece_refs[h * planes + k][...]
    chunks = []
    for j in range(tiles):
        starts = [(group * tiles + j) * 8 for group in range(2 * planes)]
        chunks.append(jnp.concatenate([work_ref[start : start + 8, :] for start in starts], axis=0))
    scores = jnp.concatenate(chunks[:-1], axis=1)
    gram_ref[...] = chunks[-1]
    comps = scores.shape[0]
    both = lax.dot_general(split_pair(scores), tile_ref[...], NN, preferred_element_type=f32)
    totals = jnp.sum(scores, axis=1, keepdims=True)
    raw = both[:comps] + both[comps:] - totals * mean_ref[...]
    rest = out_ref.shape[0] - comps - 2
    tall = jnp.concatenate(
        [raw.astype(bf16), split_pair(next_ref[...]), jnp.zeros((rest, genes), bf16)], axis=0
    )
    out_ref[...] = jnp.concatenate([tall, jnp.zeros((tall.shape[0], width - genes), bf16)], axis=1)


def inverse_factor(gram):
    size = gram.shape[0]
    shape = (8, 2 * size)
    rows = lax.broadcasted_iota(jnp.int32, shape, 0)
    lanes = lax.broadcasted_iota(jnp.int32, shape, 1)
    blocks = []
    for b in range(size // 8):
        eye = jnp.where(lanes == rows + (b * 8 + size), 1.0, 0.0).astype(f32)
        left = jnp.concatenate([gram[b * 8 : b * 8 + 8, :], jnp.zeros((8, size), f32)], axis=1)
        blocks.append(left + eye)
    results = list(blocks)
    for k in range(0, size, 2):
        b, r = divmod(k, 8)
        upper = blocks[b][r : r + 1, :]
        lower = blocks[b][r + 1 : r + 2, :]
        columns = [
            tuple(jnp.broadcast_to(blocks[i][:, k + h : k + h + 1], shape) for h in range(2))
            for i in range(b, size // 8)
        ]
        p = columns[0][0][r : r + 1, :]
        q = columns[0][0][r + 1 : r + 2, :]
        t = columns[0][1][r + 1 : r + 2, :]
        over = 1.0 / (p * t - q * q)
        first = (t * upper - q * lower) * over
        second = (p * lower - q * upper) * over
        inverse_p = 1.0 / p
        slope = q * inverse_p
        top = upper * lax.rsqrt(p)
        low = (lower - slope * upper) * lax.rsqrt(t - slope * q)
        results[b] = jnp.where(rows == r, top, jnp.where(rows == r + 1, low, results[b]))
        for i in range(b, size // 8):
            x, y = columns[i - b]
            change = x * first + y * second
            if i == b:
                change = jnp.where(rows > r + 1, change, 0.0)
            blocks[i] = blocks[i] - change
    return jnp.concatenate(results, axis=0)[:, size:]


def factor_kernel(gram_ref, out_ref):
    out_ref[...] = inverse_factor(gram_ref[:, : gram_ref.shape[0]])


def make_finish(scale):
    def kernel(in_ref, stepped_ref, out_ref):
        comps = stepped_ref.shape[0]
        total = jnp.sum(in_ref[...], axis=0)
        gram = jnp.concatenate([total[:, :comps], total[:, comps:]], axis=0)
        out_ref[...] = scale * lax.dot_general(
            inverse_factor(gram), stepped_ref[...], NN, precision=HIGH, preferred_element_type=f32
        )

    return kernel


def shards(pool_counts, cell_picks, loadings_init):
    comps, genes = loadings_init.shape
    steps, cells = cell_picks.shape
    half = comps // 2
    local_pool = pool_counts.shape[1]
    cell_devices = lax.axis_size("cell")
    gene_devices = lax.axis_size("gene")
    batch = cells * cell_devices
    width = genes + 128 - genes % 128
    depth = DEPTH
    planes = gene_devices // (2 * depth)
    index = lax.axis_index("gene").astype(jnp.int32)
    place = jnp.stack([index % 2, index // (2 * depth)])
    chosen = cell_picks - lax.axis_index("cell") * local_pool
    pool_by_cell = pool_counts.T
    columns = [
        [(plane * depth + level) * 2 + which for level in range(depth)]
        for plane in range(planes)
        for which in range(2)
    ]

    def tile_of(step):
        return jnp.take(pool_by_cell, chosen[step], axis=0, mode="clip")

    def sums_of(tile):
        return jnp.sum(tile, axis=0, dtype=f32, keepdims=True)

    def swap_cores(value):
        return lax.ppermute(value, "gene", [(i, i ^ 1) for i in range(gene_devices)])

    def round_cells(value):
        return [value] + [
            lax.ppermute(value, "cell", [(i, (i + k) % cell_devices) for i in range(cell_devices)])
            for k in range(1, cell_devices)
        ]

    def to_plane(value, k):
        return lax.ppermute(value, "gene", [(i, (i + k * 2 * depth) % gene_devices) for i in range(gene_devices)])

    def down_columns(copies):
        return lax.all_to_all(copies, "gene", 0, 0, tiled=True, axis_index_groups=columns)

    tiles = cells // 128 + 1
    packed = jax.ShapeDtypeStruct((planes * tiles * 8, 128), f32)
    piece = jax.ShapeDtypeStruct((tiles * 8, 128), f32)
    copies_shape = jax.ShapeDtypeStruct((depth, (tiles + 1) * 8, 128), bf16)
    wide = jax.ShapeDtypeStruct((comps, 128), f32)
    square = jax.ShapeDtypeStruct((comps, comps), f32)
    local = jax.ShapeDtypeStruct((comps, genes), f32)
    row = jax.ShapeDtypeStruct((1, genes), f32)
    shared = jax.ShapeDtypeStruct((comps + 8, width), bf16)

    tile = tile_of(0)
    mean = sum(round_cells(sums_of(tile))) * (1.0 / batch)
    keep, send = vmem_call(first_kernel, (packed, packed), 2, name="first")(place, loadings_init, tile)

    def scores_of(keep, send):
        mine, *others = vmem_call(pair_kernel, (piece,) * planes, 2, name="pair")(place, keep, swap_cores(send))
        came = [to_plane(value, k) for k, value in enumerate(others, 1)]
        copies = vmem_call(plane_kernel, copies_shape, planes, name="plane", place=False)(mine, *came)
        total = vmem_call(column_kernel, piece, 1, name="column", place=False)(down_columns(copies))
        pieces = [total] + [to_plane(total, k) for k in range(1, planes)]
        return pieces + [swap_cores(value) for value in pieces]

    def change_of(pieces, tile, mean, next_sums):
        change, gram = vmem_call(
            update_kernel, (shared, wide), len(pieces) + 3, name="update",
            scratch=[pltpu.VMEM((2 * packed.shape[0], 128), f32)],
        )(place, *pieces, tile, mean, next_sums)
        return round_cells(change), gram

    def factor_of(gram):
        return vmem_call(factor_kernel, square, 1, flops=10**9, name="factor", place=False)(gram)

    def advance(parts, stepped, inverse, next_tile):
        inputs = [*parts, stepped, *inverse, next_tile]
        return vmem_call(
            make_middle(batch, bool(inverse)), (packed, packed, local, row), len(inputs), name="middle"
        )(place, *inputs)

    def one_step(step, state):
        keep, send, stepped, mean, tile = state
        next_tile = tile_of(step + 1)
        parts, gram = change_of(scores_of(keep, send), tile, mean, sums_of(next_tile))
        return (*advance(parts, stepped, (factor_of(gram),), next_tile), next_tile)

    next_tile = tile_of(1)
    parts, _ = change_of(scores_of(keep, send), tile, mean, sums_of(next_tile))
    state = (*advance(parts, loadings_init, (), next_tile), next_tile)
    keep, send, stepped, mean, tile = lax.fori_loop(1, steps - 1, one_step, state)
    parts, gram = change_of(scores_of(keep, send), tile, mean, mean)
    inverse = factor_of(gram)
    gram, stepped = vmem_call(
        make_last(batch),
        (jax.ShapeDtypeStruct((half, 2 * comps), f32), local),
        len(parts) + 2,
        name="last",
        place=False,
    )(*parts, stepped, inverse)
    gram = gram + swap_cores(gram)
    gram = sum([gram] + [to_plane(gram, k) for k in range(1, planes)])
    grams = down_columns(jnp.broadcast_to(gram[None], (depth, *gram.shape)))
    scale = math.sqrt(genes * gene_devices)
    return vmem_call(make_finish(scale), local, 2, name="finish", place=False)(grams, stepped)


def solution(mesh):
    placed = (P("gene", "cell"), P(None, "cell"), P(None, "gene"))
    return jax.shard_map(
        shards, mesh=mesh, in_specs=placed, out_specs=P(None, "gene"), check_vma=False
    )
```

```python
import math

import jax
import jax.numpy as jnp
from jax import lax
from jax.experimental import pallas as pl
from jax.experimental.pallas import tpu as pltpu
from jax.sharding import PartitionSpec as P

f32 = jnp.float32
bf16 = jnp.bfloat16
STEP_RATE = 1.0
HIGH = lax.Precision.HIGHEST
NT = (((1,), (1,)), ((), ()))
NN = (((1,), (0,)), ((), ()))


def vmem_call(kernel, outs, count, flops=0, name=None, core=True, pool=0, scratch=(), held=True):
    spec = pl.BlockSpec(memory_space=pltpu.VMEM)
    call = pl.pallas_call(
        kernel,
        out_shape=jax.tree.map(lambda s: pltpu.VMEM(s.shape, s.dtype), outs) if held else outs,
        in_specs=[pl.BlockSpec(memory_space=pltpu.SMEM)] * core
        + [spec] * count
        + [pl.BlockSpec(memory_space=pl.ANY)] * pool,
        out_specs=jax.tree.map(lambda _: spec, outs),
        cost_estimate=pl.CostEstimate(flops=flops, transcendentals=0, bytes_accessed=0),
        scratch_shapes=scratch,
        name=name,
    )

    def run(*args):
        last = core + count
        near = [pltpu.with_memory_space_constraint(a, pltpu.VMEM) for a in args[core:last]]
        return call(*args[:core], *near, *args[last:])

    return run


def split_pair(value):
    high = value.astype(bf16)
    low = (value - high.astype(f32)).astype(bf16)
    return jnp.concatenate([high, low], axis=0)


def gram_of(stepped):
    return lax.dot_general(stepped, stepped, NT, precision=HIGH, preferred_element_type=f32)


def by_core(first, mine, other):
    return jnp.concatenate([jnp.where(first, mine, other), jnp.where(first, other, mine)], axis=0)


def spread(scores, gram, first, keep_ref, send_ref):
    comps = scores.shape[0]
    half = comps // 2
    gram = jnp.concatenate([gram, jnp.zeros((comps, 128 - comps), f32)], axis=1)
    rows = scores.shape[1] // 128 + 1
    for j in range(rows):
        chunk = scores[:, j * 128 : (j + 1) * 128] if j + 1 < rows else gram
        top, bottom = chunk[:half], chunk[half:]
        keep_ref[pl.ds(j, half, stride=rows), :] = jnp.where(first, top, bottom)
        send_ref[pl.ds(j, half, stride=rows), :] = jnp.where(first, bottom, top)


def pack_partial(stepped, tile, shift, first, keep_ref, send_ref):
    comps = stepped.shape[0]
    both = lax.dot_general(split_pair(stepped), tile, NT, preferred_element_type=f32)
    spread(both[:comps] + both[comps:] - shift, gram_of(stepped), first, keep_ref, send_ref)


def first_kernel(core_ref, loadings_ref, picks_ref, pool_ref, keep_ref, send_ref, buffer_ref, sems):
    chunks, _, size = buffer_ref.shape
    copies = [
        pltpu.make_async_copy(pool_ref.at[:, pl.ds(i * size, size)], buffer_ref.at[i], sems.at[i])
        for i in range(chunks)
    ]
    for copy in copies:
        copy.start()
    loadings = loadings_ref[...]
    comps = loadings.shape[0]
    pair = split_pair(loadings)
    picks = picks_ref[...]
    places = lax.broadcasted_iota(jnp.int32, (size, picks.shape[1]), 0)
    chosen = jnp.zeros((2 * comps, picks.shape[1]), f32)
    for i, copy in enumerate(copies):
        copy.wait()
        both = lax.dot_general(pair, buffer_ref[i], NN, preferred_element_type=f32)
        every = split_pair(both[:comps] + both[comps:])
        one_hot = jnp.where(places == picks - i * size, 1.0, 0.0).astype(bf16)
        chosen = chosen + lax.dot_general(every, one_hot, NN, preferred_element_type=f32)
    spread(chosen[:comps] + chosen[comps:], gram_of(loadings), core_ref[0] == 0, keep_ref, send_ref)


def add_kernel(a, b, out_ref):
    out_ref[...] = a[...] + b[...]


def stepped_from(parts, previous, inverse, batch):
    comps, genes = previous.shape
    total = sum(part[:comps, :genes].astype(f32) for part in parts)
    stepped = previous + STEP_RATE * (total * (1.0 / batch))
    if inverse is not None:
        stepped = lax.dot_general(inverse, stepped, NN, precision=HIGH, preferred_element_type=f32)
    return stepped


def make_middle(batch, normalised):
    def kernel(core_ref, a, b, c, d, previous_ref, *refs):
        inverse = refs[0][...] if normalised else None
        tile_ref, keep_ref, send_ref, stepped_ref, mean_ref = refs[-5:]
        comps, genes = previous_ref.shape
        parts = (a, b, c, d)
        stepped = stepped_from(parts, previous_ref[...], inverse, batch)
        stepped_ref[...] = stepped
        sums = sum(part[comps : comps + 2, :genes].astype(f32) for part in parts)
        mean = (sums[:1] + sums[1:]) * (1.0 / batch)
        mean_ref[...] = mean
        shift = jnp.sum(stepped * mean, axis=1, keepdims=True)
        pack_partial(stepped, tile_ref[...], shift, core_ref[0] == 0, keep_ref, send_ref)

    return kernel


def make_last(batch):
    def kernel(a, b, c, d, previous_ref, inverse_ref, gram_ref, stepped_ref):
        stepped = stepped_from((a, b, c, d), previous_ref[...], inverse_ref[...], batch)
        stepped_ref[...] = stepped
        gram = gram_of(stepped)
        half = gram.shape[0] // 2
        gram_ref[...] = jnp.concatenate([gram[:half], gram[half:]], axis=1)

    return kernel


def make_sum(count, rows):
    def kernel(in_ref, out_ref):
        for j in range(rows):
            total = jnp.sum(in_ref[pl.ds(j, count, stride=rows), :], axis=0, keepdims=True)
            out_ref[pl.ds(j, count, stride=rows), :] = jnp.broadcast_to(total, (count, 128))

    return kernel


def make_update(half, rows):
    def kernel(core_ref, mine_ref, other_ref, tile_ref, mean_ref, next_ref, out_ref):
        genes = tile_ref.shape[1]
        comps = 2 * half
        width = out_ref.shape[1]
        chunks = [
            by_core(
                core_ref[0] == 0,
                mine_ref[pl.ds(j, half, stride=rows), :],
                other_ref[pl.ds(j, half, stride=rows), :],
            )
            for j in range(rows - 1)
        ]
        scores = jnp.concatenate(chunks, axis=1)
        both = lax.dot_general(split_pair(scores), tile_ref[...], NN, preferred_element_type=f32)
        totals = jnp.sum(scores, axis=1, keepdims=True)
        raw = both[:comps] + both[comps:] - totals * mean_ref[...]
        rest = out_ref.shape[0] - comps - 2
        tall = jnp.concatenate(
            [raw.astype(bf16), split_pair(next_ref[...]), jnp.zeros((rest, genes), bf16)], axis=0
        )
        out_ref[...] = jnp.concatenate([tall, jnp.zeros((tall.shape[0], width - genes), bf16)], axis=1)

    return kernel


def inverse_factor(gram):
    size = gram.shape[0]
    shape = (8, 2 * size)
    rows = lax.broadcasted_iota(jnp.int32, shape, 0)
    lanes = lax.broadcasted_iota(jnp.int32, shape, 1)
    blocks = []
    for b in range(size // 8):
        eye = jnp.where(lanes == rows + (b * 8 + size), 1.0, 0.0).astype(f32)
        left = jnp.concatenate([gram[b * 8 : b * 8 + 8, :], jnp.zeros((8, size), f32)], axis=1)
        blocks.append(left + eye)
    results = list(blocks)
    for k in range(0, size, 2):
        b, r = divmod(k, 8)
        upper = blocks[b][r : r + 1, :]
        lower = blocks[b][r + 1 : r + 2, :]
        columns = [
            tuple(jnp.broadcast_to(blocks[i][:, k + h : k + h + 1], shape) for h in range(2))
            for i in range(b, size // 8)
        ]
        p = columns[0][0][r : r + 1, :]
        q = columns[0][0][r + 1 : r + 2, :]
        t = columns[0][1][r + 1 : r + 2, :]
        over = 1.0 / (p * t - q * q)
        first = (t * upper - q * lower) * over
        second = (p * lower - q * upper) * over
        inverse_p = 1.0 / p
        slope = q * inverse_p
        top = upper * lax.rsqrt(p)
        low = (lower - slope * upper) * lax.rsqrt(t - slope * q)
        results[b] = jnp.where(rows == r, top, jnp.where(rows == r + 1, low, results[b]))
        for i in range(b, size // 8):
            x, y = columns[i - b]
            change = x * first + y * second
            if i == b:
                change = jnp.where(rows > r + 1, change, 0.0)
            blocks[i] = blocks[i] - change
    return jnp.concatenate(results, axis=0)[:, size:]


def make_factor(half, rows):
    def kernel(core_ref, mine_ref, other_ref, out_ref):
        gram = by_core(
            core_ref[0] == 0,
            mine_ref[pl.ds(rows - 1, half, stride=rows), :],
            other_ref[pl.ds(rows - 1, half, stride=rows), :],
        )
        out_ref[...] = inverse_factor(gram[:, : 2 * half])

    return kernel


def make_finish(scale):
    def kernel(in_ref, stepped_ref, out_ref):
        comps = stepped_ref.shape[0]
        total = jnp.sum(in_ref[...], axis=0)
        gram = jnp.concatenate([total[:, :comps], total[:, comps:]], axis=0)
        out_ref[...] = scale * lax.dot_general(
            inverse_factor(gram), stepped_ref[...], NN, precision=HIGH, preferred_element_type=f32
        )

    return kernel


def shards(pool_counts, cell_picks, loadings_init):
    comps, genes = loadings_init.shape
    steps, cells = cell_picks.shape
    half = comps // 2
    local_pool = pool_counts.shape[1]
    cell_devices = lax.axis_size("cell")
    gene_devices = lax.axis_size("gene")
    chips = gene_devices // 2
    batch = cells * cell_devices
    rows = cells // 128 + 1
    width = genes + 128 - genes % 128
    core = (lax.axis_index("gene") % 2).astype(jnp.int32).reshape(1)
    chosen = cell_picks - lax.axis_index("cell") * local_pool
    pool_by_cell = pool_counts.T
    same_core = [[2 * chip + which for chip in range(chips)] for which in range(2)]

    def tile_of(step):
        return jnp.take(pool_by_cell, chosen[step], axis=0, mode="clip")

    def sums_of(tile):
        return jnp.sum(tile, axis=0, dtype=f32, keepdims=True)

    def swap_cores(value):
        return lax.ppermute(value, "gene", [(i, i ^ 1) for i in range(gene_devices)])

    def round_cells(value):
        return [value] + [
            lax.ppermute(value, "cell", [(i, (i + k) % cell_devices) for i in range(cell_devices)])
            for k in (2, 1, 3)
        ]

    def exchange(value):
        pieces = value.reshape(chips, 1, value.size // chips)
        arrived = lax.all_to_all(pieces, "gene", 0, 0, tiled=True, axis_index_groups=same_core)
        return arrived.reshape(value.shape)

    packed = jax.ShapeDtypeStruct((half * rows, 128), f32)
    square = jax.ShapeDtypeStruct((comps, comps), f32)
    local = jax.ShapeDtypeStruct((comps, genes), f32)
    row = jax.ShapeDtypeStruct((1, genes), f32)
    shared = jax.ShapeDtypeStruct((comps + 8, width), bf16)

    tile = tile_of(0)
    mean = sum(round_cells(sums_of(tile))) * (1.0 / batch)
    chunk = local_pool // 8
    keep, send = vmem_call(
        first_kernel,
        (packed, packed),
        2,
        name="first",
        pool=1,
        scratch=[pltpu.VMEM((8, genes, chunk), bf16), pltpu.SemaphoreType.DMA((8,))],
    )(core, loadings_init, chosen[:1], pool_counts)

    def scores_of(keep, send):
        chip_sum = vmem_call(add_kernel, packed, 2, name="pair", core=False)(keep, swap_cores(send))
        copies = vmem_call(make_sum(chips, rows), packed, 1, name="add_up", core=False)(exchange(chip_sum))
        mine = exchange(copies)
        return mine, swap_cores(mine)

    def change_of(mine, other, tile, mean, next_sums):
        change = vmem_call(make_update(half, rows), shared, 5, name="update")(
            core, mine, other, tile, mean, next_sums
        )
        return round_cells(change)

    def factor_of(mine, other):
        return vmem_call(make_factor(half, rows), square, 2, flops=10**9, name="factor")(core, mine, other)

    def advance(parts, stepped, inverse, next_tile):
        inputs = [*parts, stepped, *inverse, next_tile]
        return vmem_call(
            make_middle(batch, bool(inverse)), (packed, packed, local, row), len(inputs), name="middle"
        )(core, *inputs)

    def one_step(step, state):
        keep, send, stepped, mean, tile = state
        next_tile = tile_of(step + 1)
        mine, other = scores_of(keep, send)
        parts = change_of(mine, other, tile, mean, sums_of(next_tile))
        inverse = (factor_of(mine, other),)
        return (*advance(parts, stepped, inverse, next_tile), next_tile)

    next_tile = tile_of(1)
    mine, other = scores_of(keep, send)
    parts = change_of(mine, other, tile, mean, sums_of(next_tile))
    state = (*advance(parts, loadings_init, (), next_tile), next_tile)
    keep, send, stepped, mean, tile = lax.fori_loop(1, steps - 1, one_step, state)
    mine, other = scores_of(keep, send)
    parts = change_of(mine, other, tile, mean, mean)
    inverse = factor_of(mine, other)
    gram, stepped = vmem_call(
        make_last(batch),
        (jax.ShapeDtypeStruct((half, 2 * comps), f32), local),
        len(parts) + 2,
        name="last",
        core=False,
    )(*parts, stepped, inverse)
    gram = gram + swap_cores(gram)
    depth = 8
    planes = chips // depth
    gram = sum(
        [gram]
        + [
            lax.ppermute(gram, "gene", [(i, (i + k * 2 * depth) % gene_devices) for i in range(gene_devices)])
            for k in range(1, planes)
        ]
    )
    columns = [
        [(plane * depth + level) * 2 + which for level in range(depth)]
        for plane in range(planes)
        for which in range(2)
    ]
    grams = lax.all_to_all(
        jnp.broadcast_to(gram[None], (depth, *gram.shape)), "gene", 0, 0, tiled=True, axis_index_groups=columns
    )
    scale = math.sqrt(genes * gene_devices)
    return vmem_call(make_finish(scale), local, 2, name="finish", core=False, held=False)(grams, stepped)


def solution(mesh):
    placed = (P("gene", "cell"), P(None, "cell"), P(None, "gene"))
    return jax.shard_map(
        shards, mesh=mesh, in_specs=placed, out_specs=P(None, "gene"), check_vma=False
    )
```

```python
import math

import jax
import jax.numpy as jnp
from jax import lax
from jax.experimental import pallas as pl
from jax.experimental.pallas import tpu as pltpu
from jax.sharding import PartitionSpec as P

f32 = jnp.float32
bf16 = jnp.bfloat16
STEP_RATE = 1.0
HIGH = lax.Precision.HIGHEST
NT = (((1,), (1,)), ((), ()))
NN = (((1,), (0,)), ((), ()))


def vmem_call(kernel, outs, count, flops=0, name=None, core=True, pool=0, scratch=(), held=True):
    spec = pl.BlockSpec(memory_space=pltpu.VMEM)
    call = pl.pallas_call(
        kernel,
        out_shape=jax.tree.map(lambda s: pltpu.VMEM(s.shape, s.dtype), outs) if held else outs,
        in_specs=[pl.BlockSpec(memory_space=pltpu.SMEM)] * core
        + [spec] * count
        + [pl.BlockSpec(memory_space=pl.ANY)] * pool,
        out_specs=jax.tree.map(lambda _: spec, outs),
        cost_estimate=pl.CostEstimate(flops=flops, transcendentals=0, bytes_accessed=0),
        scratch_shapes=scratch,
        name=name,
    )

    def run(*args):
        last = core + count
        near = [pltpu.with_memory_space_constraint(a, pltpu.VMEM) for a in args[core:last]]
        return call(*args[:core], *near, *args[last:])

    return run


def split_pair(value):
    high = value.astype(bf16)
    low = (value - high.astype(f32)).astype(bf16)
    return jnp.concatenate([high, low], axis=0)


def gram_of(stepped):
    return lax.dot_general(stepped, stepped, NT, precision=HIGH, preferred_element_type=f32)


def by_core(first, mine, other):
    return jnp.concatenate([jnp.where(first, mine, other), jnp.where(first, other, mine)], axis=0)


def spread(scores, gram, first, keep_ref, send_ref):
    comps = scores.shape[0]
    half = comps // 2
    gram = jnp.concatenate([gram, jnp.zeros((comps, 128 - comps), f32)], axis=1)
    rows = scores.shape[1] // 128 + 1
    for j in range(rows):
        chunk = scores[:, j * 128 : (j + 1) * 128] if j + 1 < rows else gram
        top, bottom = chunk[:half], chunk[half:]
        keep_ref[pl.ds(j, half, stride=rows), :] = jnp.where(first, top, bottom)
        send_ref[pl.ds(j, half, stride=rows), :] = jnp.where(first, bottom, top)


def pack_partial(stepped, tile, shift, first, keep_ref, send_ref):
    comps = stepped.shape[0]
    both = lax.dot_general(split_pair(stepped), tile, NT, preferred_element_type=f32)
    spread(both[:comps] + both[comps:] - shift, gram_of(stepped), first, keep_ref, send_ref)


def first_kernel(core_ref, loadings_ref, picks_ref, pool_ref, keep_ref, send_ref, buffer_ref, sems):
    chunks, _, size = buffer_ref.shape
    copies = [
        pltpu.make_async_copy(pool_ref.at[:, pl.ds(i * size, size)], buffer_ref.at[i], sems.at[i])
        for i in range(chunks)
    ]
    for copy in copies:
        copy.start()
    loadings = loadings_ref[...]
    comps = loadings.shape[0]
    pair = split_pair(loadings)
    picks = picks_ref[...]
    places = lax.broadcasted_iota(jnp.int32, (size, picks.shape[1]), 0)
    chosen = jnp.zeros((2 * comps, picks.shape[1]), f32)
    for i, copy in enumerate(copies):
        copy.wait()
        both = lax.dot_general(pair, buffer_ref[i], NN, preferred_element_type=f32)
        every = split_pair(both[:comps] + both[comps:])
        one_hot = jnp.where(places == picks - i * size, 1.0, 0.0).astype(bf16)
        chosen = chosen + lax.dot_general(every, one_hot, NN, preferred_element_type=f32)
    spread(chosen[:comps] + chosen[comps:], gram_of(loadings), core_ref[0] == 0, keep_ref, send_ref)


def add_kernel(a, b, out_ref):
    out_ref[...] = a[...] + b[...]


def stepped_from(parts, previous, inverse, batch, left=0.0):
    comps, genes = previous.shape
    total = sum(part[:comps, :genes].astype(f32) for part in parts) + left
    stepped = previous + STEP_RATE * (total * (1.0 / batch))
    if inverse is not None:
        stepped = lax.dot_general(inverse, stepped, NN, precision=HIGH, preferred_element_type=f32)
    return stepped


def pair_rows(part, start, genes):
    return part[start : start + 1, :genes].astype(f32) + part[start + 1 : start + 2, :genes].astype(f32)


def between_groups(parts, comps, genes, batch):
    sums = [pair_rows(part, comps + 2, genes) for part in parts]
    mean = sum(sums) * (1.0 / batch)
    total = jnp.zeros((comps, genes), f32)
    for part, own in zip(parts, sums):
        totals = part[:comps, genes : genes + 1].astype(f32) + part[:comps, genes + 1 : genes + 2].astype(f32)
        total = total + totals * (own * (len(parts) / batch) - mean)
    return total


def make_middle(batch, normalised):
    def kernel(core_ref, a, b, c, d, previous_ref, *refs):
        inverse = refs[0][...] if normalised else None
        tile_ref, keep_ref, send_ref, stepped_ref, mean_ref = refs[-5:]
        comps, genes = previous_ref.shape
        parts = (a, b, c, d)
        left = 0.0 if normalised else between_groups(parts, comps, genes, batch)
        stepped = stepped_from(parts, previous_ref[...], inverse, batch, left)
        stepped_ref[...] = stepped
        mean = sum(pair_rows(part, comps, genes) for part in parts) * (1.0 / batch)
        mean_ref[...] = mean
        shift = jnp.sum(stepped * mean, axis=1, keepdims=True)
        pack_partial(stepped, tile_ref[...], shift, core_ref[0] == 0, keep_ref, send_ref)

    return kernel


def make_last(batch):
    def kernel(a, b, c, d, previous_ref, inverse_ref, gram_ref, stepped_ref):
        stepped = stepped_from((a, b, c, d), previous_ref[...], inverse_ref[...], batch)
        stepped_ref[...] = stepped
        gram = gram_of(stepped)
        half = gram.shape[0] // 2
        gram_ref[...] = jnp.concatenate([gram[:half], gram[half:]], axis=1)

    return kernel


def make_sum(count, rows):
    def kernel(in_ref, out_ref):
        for j in range(rows):
            total = jnp.sum(in_ref[pl.ds(j, count, stride=rows), :], axis=0, keepdims=True)
            out_ref[pl.ds(j, count, stride=rows), :] = jnp.broadcast_to(total, (count, 128))

    return kernel


def make_update(half, rows, cells=None):
    def kernel(core_ref, mine_ref, other_ref, tile_ref, mean_ref, next_ref, out_ref):
        genes = tile_ref.shape[1]
        comps = 2 * half
        width = out_ref.shape[1]
        chunks = [
            by_core(
                core_ref[0] == 0,
                mine_ref[pl.ds(j, half, stride=rows), :],
                other_ref[pl.ds(j, half, stride=rows), :],
            )
            for j in range(rows - 1)
        ]
        scores = jnp.concatenate(chunks, axis=1)
        both = lax.dot_general(split_pair(scores), tile_ref[...], NN, preferred_element_type=f32)
        totals = jnp.sum(scores, axis=1, keepdims=True)
        mean = mean_ref[...] * (1.0 / cells) if cells else mean_ref[...]
        raw = both[:comps] + both[comps:] - totals * mean
        rest = out_ref.shape[0] - comps - 4
        tall = jnp.concatenate(
            [
                raw.astype(bf16),
                split_pair(next_ref[...]),
                split_pair(mean_ref[...]),
                jnp.zeros((rest, genes), bf16),
            ],
            axis=0,
        )
        high = totals.astype(bf16)
        low = (totals - high.astype(f32)).astype(bf16)
        side = jnp.concatenate([high, low, jnp.zeros((comps, width - genes - 2), bf16)], axis=1)
        side = jnp.concatenate([side, jnp.zeros((tall.shape[0] - comps, width - genes), bf16)], axis=0)
        out_ref[...] = jnp.concatenate([tall, side], axis=1)

    return kernel


def inverse_factor(gram):
    size = gram.shape[0]
    shape = (8, 2 * size)
    rows = lax.broadcasted_iota(jnp.int32, shape, 0)
    lanes = lax.broadcasted_iota(jnp.int32, shape, 1)
    blocks = []
    for b in range(size // 8):
        eye = jnp.where(lanes == rows + (b * 8 + size), 1.0, 0.0).astype(f32)
        left = jnp.concatenate([gram[b * 8 : b * 8 + 8, :], jnp.zeros((8, size), f32)], axis=1)
        blocks.append(left + eye)
    results = list(blocks)
    for k in range(0, size, 2):
        b, r = divmod(k, 8)
        upper = blocks[b][r : r + 1, :]
        lower = blocks[b][r + 1 : r + 2, :]
        columns = [
            tuple(jnp.broadcast_to(blocks[i][:, k + h : k + h + 1], shape) for h in range(2))
            for i in range(b, size // 8)
        ]
        p = columns[0][0][r : r + 1, :]
        q = columns[0][0][r + 1 : r + 2, :]
        t = columns[0][1][r + 1 : r + 2, :]
        over = 1.0 / (p * t - q * q)
        first = (t * upper - q * lower) * over
        second = (p * lower - q * upper) * over
        inverse_p = 1.0 / p
        slope = q * inverse_p
        top = upper * lax.rsqrt(p)
        low = (lower - slope * upper) * lax.rsqrt(t - slope * q)
        results[b] = jnp.where(rows == r, top, jnp.where(rows == r + 1, low, results[b]))
        for i in range(b, size // 8):
            x, y = columns[i - b]
            change = x * first + y * second
            if i == b:
                change = jnp.where(rows > r + 1, change, 0.0)
            blocks[i] = blocks[i] - change
    return jnp.concatenate(results, axis=0)[:, size:]


def make_factor(half, rows):
    def kernel(core_ref, mine_ref, other_ref, out_ref):
        gram = by_core(
            core_ref[0] == 0,
            mine_ref[pl.ds(rows - 1, half, stride=rows), :],
            other_ref[pl.ds(rows - 1, half, stride=rows), :],
        )
        out_ref[...] = inverse_factor(gram[:, : 2 * half])

    return kernel


def make_finish(scale):
    def kernel(in_ref, stepped_ref, out_ref):
        comps = stepped_ref.shape[0]
        total = jnp.sum(in_ref[...], axis=0)
        gram = jnp.concatenate([total[:, :comps], total[:, comps:]], axis=0)
        out_ref[...] = scale * lax.dot_general(
            inverse_factor(gram), stepped_ref[...], NN, precision=HIGH, preferred_element_type=f32
        )

    return kernel


def shards(pool_counts, cell_picks, loadings_init):
    comps, genes = loadings_init.shape
    steps, cells = cell_picks.shape
    half = comps // 2
    local_pool = pool_counts.shape[1]
    cell_devices = lax.axis_size("cell")
    gene_devices = lax.axis_size("gene")
    chips = gene_devices // 2
    batch = cells * cell_devices
    rows = cells // 128 + 1
    width = genes + 128 - genes % 128
    core = (lax.axis_index("gene") % 2).astype(jnp.int32).reshape(1)
    chosen = cell_picks - lax.axis_index("cell") * local_pool
    pool_by_cell = pool_counts.T
    same_core = [[2 * chip + which for chip in range(chips)] for which in range(2)]

    def tile_of(picks):
        return jnp.take(pool_by_cell, picks, axis=0, mode="clip")

    def sums_of(tile):
        return jnp.sum(tile, axis=0, dtype=f32, keepdims=True)

    def swap_cores(value):
        return lax.ppermute(value, "gene", [(i, i ^ 1) for i in range(gene_devices)])

    def round_cells(value):
        return [value] + [
            lax.ppermute(value, "cell", [(i, (i + k) % cell_devices) for i in range(cell_devices)])
            for k in range(1, cell_devices)
        ]

    def exchange(value):
        pieces = value.reshape(chips, 1, value.size // chips)
        arrived = lax.all_to_all(pieces, "gene", 0, 0, tiled=True, axis_index_groups=same_core)
        return arrived.reshape(value.shape)

    packed = jax.ShapeDtypeStruct((half * rows, 128), f32)
    square = jax.ShapeDtypeStruct((comps, comps), f32)
    local = jax.ShapeDtypeStruct((comps, genes), f32)
    row = jax.ShapeDtypeStruct((1, genes), f32)
    shared = jax.ShapeDtypeStruct((comps + 8, width), bf16)

    tile = tile_of(chosen[0])
    chunk = local_pool // 8
    keep, send = vmem_call(
        first_kernel,
        (packed, packed),
        2,
        name="first",
        pool=1,
        scratch=[pltpu.VMEM((8, genes, chunk), bf16), pltpu.SemaphoreType.DMA((8,))],
    )(core, loadings_init, chosen[:1], pool_counts)

    def scores_of(keep, send):
        chip_sum = vmem_call(add_kernel, packed, 2, name="pair", core=False)(keep, swap_cores(send))
        copies = vmem_call(make_sum(chips, rows), packed, 1, name="add_up", core=False)(exchange(chip_sum))
        mine = exchange(copies)
        return mine, swap_cores(mine)

    def change_of(mine, other, tile, mean, next_sums, own=None):
        change = vmem_call(make_update(half, rows, own), shared, 5, name="update")(
            core, mine, other, tile, mean, next_sums
        )
        return round_cells(change)

    def factor_of(mine, other):
        return vmem_call(make_factor(half, rows), square, 2, flops=10**9, name="factor")(core, mine, other)

    def advance(parts, stepped, inverse, next_tile):
        inputs = [*parts, stepped, *inverse, next_tile]
        return vmem_call(
            make_middle(batch, bool(inverse)), (packed, packed, local, row), len(inputs), name="middle"
        )(core, *inputs)

    def one_step(state):
        step, keep, send, stepped, mean, tile = state
        following = step + 1
        picks = lax.dynamic_index_in_dim(chosen, following, keepdims=False)
        following, picks, send = lax.optimization_barrier((following, picks, send))
        next_tile = tile_of(picks)
        mine, other = scores_of(keep, send)
        parts = change_of(mine, other, tile, mean, sums_of(next_tile))
        inverse = (factor_of(mine, other),)
        return (following, *advance(parts, stepped, inverse, next_tile), next_tile)

    next_tile = tile_of(chosen[1])
    mine, other = scores_of(keep, send)
    parts = change_of(mine, other, tile, sums_of(tile), sums_of(next_tile), cells)
    state = (*advance(parts, loadings_init, (), next_tile), next_tile)
    _, keep, send, stepped, mean, tile = lax.while_loop(
        lambda state: state[0] < steps - 1, one_step, (jnp.int32(1), *state)
    )
    mine, other = scores_of(keep, send)
    parts = change_of(mine, other, tile, mean, mean)
    inverse = factor_of(mine, other)
    gram, stepped = vmem_call(
        make_last(batch),
        (jax.ShapeDtypeStruct((half, 2 * comps), f32), local),
        len(parts) + 2,
        name="last",
        core=False,
    )(*parts, stepped, inverse)
    gram = gram + swap_cores(gram)
    depth = 8
    planes = chips // depth
    gram = sum(
        [gram]
        + [
            lax.ppermute(gram, "gene", [(i, (i + k * 2 * depth) % gene_devices) for i in range(gene_devices)])
            for k in range(1, planes)
        ]
    )
    columns = [
        [(plane * depth + level) * 2 + which for level in range(depth)]
        for plane in range(planes)
        for which in range(2)
    ]
    grams = lax.all_to_all(
        jnp.broadcast_to(gram[None], (depth, *gram.shape)), "gene", 0, 0, tiled=True, axis_index_groups=columns
    )
    scale = math.sqrt(genes * gene_devices)
    return vmem_call(make_finish(scale), local, 2, name="finish", core=False, held=False)(grams, stepped)


def solution(mesh):
    placed = (P("gene", "cell"), P(None, "cell"), P(None, "gene"))
    return jax.shard_map(
        shards, mesh=mesh, in_specs=placed, out_specs=P(None, "gene"), check_vma=False
    )
```

```python
import math

import jax
import jax.numpy as jnp
from jax import lax
from jax.experimental import pallas as pl
from jax.experimental.pallas import tpu as pltpu
from jax.sharding import PartitionSpec as P

f32 = jnp.float32
bf16 = jnp.bfloat16
STEP_RATE = 1.0
HIGH = lax.Precision.HIGHEST
NT = (((1,), (1,)), ((), ()))
NN = (((1,), (0,)), ((), ()))


def vmem_call(kernel, outs, count, flops=0, name=None, core=True, pool=0, scratch=(), held=True):
    spec = pl.BlockSpec(memory_space=pltpu.VMEM)
    call = pl.pallas_call(
        kernel,
        out_shape=jax.tree.map(lambda s: pltpu.VMEM(s.shape, s.dtype), outs) if held else outs,
        in_specs=[pl.BlockSpec(memory_space=pltpu.SMEM)] * core
        + [spec] * count
        + [pl.BlockSpec(memory_space=pl.ANY)] * pool,
        out_specs=jax.tree.map(lambda _: spec, outs),
        cost_estimate=pl.CostEstimate(flops=flops, transcendentals=0, bytes_accessed=0),
        scratch_shapes=scratch,
        name=name,
    )

    def run(*args):
        last = core + count
        near = [pltpu.with_memory_space_constraint(a, pltpu.VMEM) for a in args[core:last]]
        return call(*args[:core], *near, *args[last:])

    return run


def split_pair(value):
    high = value.astype(bf16)
    low = (value - high.astype(f32)).astype(bf16)
    return jnp.concatenate([high, low], axis=0)


def gram_of(stepped):
    return lax.dot_general(stepped, stepped, NT, precision=HIGH, preferred_element_type=f32)


def by_core(first, mine, other):
    return jnp.concatenate([jnp.where(first, mine, other), jnp.where(first, other, mine)], axis=0)


def spread(scores, gram, first, keep_ref, send_ref):
    comps = scores.shape[0]
    half = comps // 2
    gram = jnp.concatenate([gram, jnp.zeros((comps, 128 - comps), f32)], axis=1)
    rows = scores.shape[1] // 128 + 1
    for j in range(rows):
        chunk = scores[:, j * 128 : (j + 1) * 128] if j + 1 < rows else gram
        top, bottom = chunk[:half], chunk[half:]
        keep_ref[pl.ds(j, half, stride=rows), :] = jnp.where(first, top, bottom)
        send_ref[pl.ds(j, half, stride=rows), :] = jnp.where(first, bottom, top)


def pack_partial(stepped, tile, shift, first, keep_ref, send_ref):
    comps = stepped.shape[0]
    both = lax.dot_general(split_pair(stepped), tile, NT, preferred_element_type=f32)
    spread(both[:comps] + both[comps:] - shift, gram_of(stepped), first, keep_ref, send_ref)


def first_kernel(place_ref, loadings_ref, picks_ref, pool_ref, keep_ref, send_ref, start_ref, names_ref, buffer_ref, sems):
    chunks, _, size = buffer_ref.shape
    near = [
        pltpu.make_async_copy(loadings_ref, start_ref, sems.at[chunks]),
        pltpu.make_async_copy(picks_ref, names_ref, sems.at[chunks + 1]),
    ]
    copies = [
        pltpu.make_async_copy(pool_ref.at[:, pl.ds(i * size, size)], buffer_ref.at[i], sems.at[i])
        for i in range(chunks)
    ]
    for copy in near + copies:
        copy.start()
    for copy in near:
        copy.wait()
    loadings = start_ref[...]
    comps = loadings.shape[0]
    pair = split_pair(loadings)
    picks = names_ref[0:1, :] - place_ref[1]
    places = lax.broadcasted_iota(jnp.int32, (size, picks.shape[1]), 0)
    chosen = jnp.zeros((2 * comps, picks.shape[1]), f32)
    for i, copy in enumerate(copies):
        copy.wait()
        both = lax.dot_general(pair, buffer_ref[i], NN, preferred_element_type=f32)
        every = split_pair(both[:comps] + both[comps:])
        one_hot = jnp.where(places == picks - i * size, 1.0, 0.0).astype(bf16)
        chosen = chosen + lax.dot_general(every, one_hot, NN, preferred_element_type=f32)
    spread(chosen[:comps] + chosen[comps:], gram_of(loadings), place_ref[0] == 0, keep_ref, send_ref)


def add_kernel(a, b, out_ref):
    out_ref[...] = a[...] + b[...]


def stepped_from(parts, previous, inverse, batch, left=0.0):
    comps, genes = previous.shape
    total = sum(part[:comps, :genes].astype(f32) for part in parts) + left
    stepped = previous + STEP_RATE * (total * (1.0 / batch))
    if inverse is not None:
        stepped = lax.dot_general(inverse, stepped, NN, precision=HIGH, preferred_element_type=f32)
    return stepped


def pair_rows(part, start, genes):
    return part[start : start + 1, :genes].astype(f32) + part[start + 1 : start + 2, :genes].astype(f32)


def between_groups(parts, comps, genes, batch):
    sums = [pair_rows(part, comps + 2, genes) for part in parts]
    mean = sum(sums) * (1.0 / batch)
    total = jnp.zeros((comps, genes), f32)
    for part, own in zip(parts, sums):
        totals = part[:comps, genes : genes + 1].astype(f32) + part[:comps, genes + 1 : genes + 2].astype(f32)
        total = total + totals * (own * (len(parts) / batch) - mean)
    return total


def make_middle(batch, normalised):
    def kernel(core_ref, a, b, c, d, previous_ref, *refs):
        inverse = refs[0][...] if normalised else None
        tile_ref, keep_ref, send_ref, stepped_ref, mean_ref = refs[-5:]
        comps, genes = previous_ref.shape
        parts = (a, b, c, d)
        left = 0.0 if normalised else between_groups(parts, comps, genes, batch)
        stepped = stepped_from(parts, previous_ref[...], inverse, batch, left)
        stepped_ref[...] = stepped
        mean = sum(pair_rows(part, comps, genes) for part in parts) * (1.0 / batch)
        mean_ref[...] = mean
        shift = jnp.sum(stepped * mean, axis=1, keepdims=True)
        pack_partial(stepped, tile_ref[...], shift, core_ref[0] == 0, keep_ref, send_ref)

    return kernel


def make_last(batch):
    def kernel(core_ref, a, b, c, d, previous_ref, inverse_ref, keep_ref, send_ref, stepped_ref):
        stepped = stepped_from((a, b, c, d), previous_ref[...], inverse_ref[...], batch)
        stepped_ref[...] = stepped
        gram = gram_of(stepped)
        quarter = gram.shape[0] // 4
        top = jnp.concatenate([gram[:quarter], gram[quarter : 2 * quarter]], axis=1)
        bottom = jnp.concatenate([gram[2 * quarter : 3 * quarter], gram[3 * quarter :]], axis=1)
        first = core_ref[0] == 0
        keep_ref[...] = jnp.where(first, top, bottom)
        send_ref[...] = jnp.where(first, bottom, top)

    return kernel


def make_sum(count, rows):
    def kernel(in_ref, out_ref):
        for j in range(rows):
            total = jnp.sum(in_ref[pl.ds(j, count, stride=rows), :], axis=0, keepdims=True)
            out_ref[pl.ds(j, count, stride=rows), :] = jnp.broadcast_to(total, (count, 128))

    return kernel


def make_update(half, rows, cells=None):
    def kernel(core_ref, mine_ref, other_ref, tile_ref, mean_ref, next_ref, out_ref):
        genes = tile_ref.shape[1]
        comps = 2 * half
        width = out_ref.shape[1]
        chunks = [
            by_core(
                core_ref[0] == 0,
                mine_ref[pl.ds(j, half, stride=rows), :],
                other_ref[pl.ds(j, half, stride=rows), :],
            )
            for j in range(rows - 1)
        ]
        scores = jnp.concatenate(chunks, axis=1)
        both = lax.dot_general(split_pair(scores), tile_ref[...], NN, preferred_element_type=f32)
        totals = jnp.sum(scores, axis=1, keepdims=True)
        mean = mean_ref[...] * (1.0 / cells) if cells else mean_ref[...]
        raw = both[:comps] + both[comps:] - totals * mean
        rest = out_ref.shape[0] - comps - 4
        tall = jnp.concatenate(
            [
                raw.astype(bf16),
                split_pair(next_ref[...]),
                split_pair(mean_ref[...]),
                jnp.zeros((rest, genes), bf16),
            ],
            axis=0,
        )
        high = totals.astype(bf16)
        low = (totals - high.astype(f32)).astype(bf16)
        side = jnp.concatenate([high, low, jnp.zeros((comps, width - genes - 2), bf16)], axis=1)
        side = jnp.concatenate([side, jnp.zeros((tall.shape[0] - comps, width - genes), bf16)], axis=0)
        out_ref[...] = jnp.concatenate([tall, side], axis=1)

    return kernel


def inverse_factor(gram):
    size = gram.shape[0]
    shape = (8, 2 * size)
    rows = lax.broadcasted_iota(jnp.int32, shape, 0)
    lanes = lax.broadcasted_iota(jnp.int32, shape, 1)
    blocks = []
    for b in range(size // 8):
        eye = jnp.where(lanes == rows + (b * 8 + size), 1.0, 0.0).astype(f32)
        left = jnp.concatenate([gram[b * 8 : b * 8 + 8, :], jnp.zeros((8, size), f32)], axis=1)
        blocks.append(left + eye)
    results = list(blocks)
    for k in range(0, size, 2):
        b, r = divmod(k, 8)
        upper = blocks[b][r : r + 1, :]
        lower = blocks[b][r + 1 : r + 2, :]
        columns = [
            tuple(jnp.broadcast_to(blocks[i][:, k + h : k + h + 1], shape) for h in range(2))
            for i in range(b, size // 8)
        ]
        p = columns[0][0][r : r + 1, :]
        q = columns[0][0][r + 1 : r + 2, :]
        t = columns[0][1][r + 1 : r + 2, :]
        over = 1.0 / (p * t - q * q)
        first = (t * upper - q * lower) * over
        second = (p * lower - q * upper) * over
        inverse_p = 1.0 / p
        slope = q * inverse_p
        top = upper * lax.rsqrt(p)
        low = (lower - slope * upper) * lax.rsqrt(t - slope * q)
        results[b] = jnp.where(rows == r, top, jnp.where(rows == r + 1, low, results[b]))
        for i in range(b, size // 8):
            x, y = columns[i - b]
            change = x * first + y * second
            if i == b:
                change = jnp.where(rows > r + 1, change, 0.0)
            blocks[i] = blocks[i] - change
    return jnp.concatenate(results, axis=0)[:, size:]


def make_factor(half, rows):
    def kernel(core_ref, mine_ref, other_ref, out_ref):
        gram = by_core(
            core_ref[0] == 0,
            mine_ref[pl.ds(rows - 1, half, stride=rows), :],
            other_ref[pl.ds(rows - 1, half, stride=rows), :],
        )
        out_ref[...] = inverse_factor(gram[:, : 2 * half])

    return kernel


def copies_kernel(a, b, out_ref):
    out_ref[...] = jnp.broadcast_to((a[...] + b[...])[None], out_ref.shape)


def total_kernel(in_ref, out_ref):
    out_ref[...] = jnp.sum(in_ref[...], axis=0)


def make_finish(scale):
    def kernel(core_ref, mine_ref, other_ref, stepped_ref, out_ref):
        comps = stepped_ref.shape[0]
        total = by_core(core_ref[0] == 0, mine_ref[...], other_ref[...])
        quarter = comps // 4
        gram = jnp.concatenate(
            [total[h : h + quarter, w : w + comps] for h in (0, quarter) for w in (0, comps)], axis=0
        )
        out_ref[...] = scale * lax.dot_general(
            inverse_factor(gram), stepped_ref[...], NN, precision=HIGH, preferred_element_type=f32
        )

    return kernel


def shards(pool_counts, cell_picks, loadings_init):
    comps, genes = loadings_init.shape
    steps, cells = cell_picks.shape
    half = comps // 2
    local_pool = pool_counts.shape[1]
    cell_devices = lax.axis_size("cell")
    gene_devices = lax.axis_size("gene")
    chips = gene_devices // 2
    batch = cells * cell_devices
    rows = cells // 128 + 1
    width = genes + 128 - genes % 128
    first_cell = lax.axis_index("cell").astype(jnp.int32) * local_pool
    core = jnp.stack([lax.axis_index("gene").astype(jnp.int32) % 2, first_cell])
    chosen = cell_picks - first_cell
    pool_by_cell = pool_counts.T
    same_core = [[2 * chip + which for chip in range(chips)] for which in range(2)]

    def tile_of(picks):
        return jnp.take(pool_by_cell, picks, axis=0, mode="clip")

    def sums_of(tile):
        return jnp.sum(tile, axis=0, dtype=f32, keepdims=True)

    def swap_cores(value):
        return lax.ppermute(value, "gene", [(i, i ^ 1) for i in range(gene_devices)])

    def round_cells(value):
        return [value] + [
            lax.ppermute(value, "cell", [(i, (i + k) % cell_devices) for i in range(cell_devices)])
            for k in range(1, cell_devices)
        ]

    def exchange(value):
        pieces = value.reshape(chips, 1, value.size // chips)
        arrived = lax.all_to_all(pieces, "gene", 0, 0, tiled=True, axis_index_groups=same_core)
        return arrived.reshape(value.shape)

    packed = jax.ShapeDtypeStruct((half * rows, 128), f32)
    square = jax.ShapeDtypeStruct((comps, comps), f32)
    local = jax.ShapeDtypeStruct((comps, genes), f32)
    row = jax.ShapeDtypeStruct((1, genes), f32)
    shared = jax.ShapeDtypeStruct((comps + 8, width), bf16)

    chunk = local_pool // 8
    keep, send = vmem_call(
        first_kernel,
        (packed, packed),
        0,
        name="first",
        pool=3,
        scratch=[
            pltpu.VMEM((comps, genes), f32),
            pltpu.VMEM((steps, cells), jnp.int32),
            pltpu.VMEM((8, genes, chunk), bf16),
            pltpu.SemaphoreType.DMA((10,)),
        ],
    )(core, loadings_init, cell_picks, pool_counts)

    def scores_of(keep, send, later):
        chip_sum = vmem_call(add_kernel, packed, 2, name="pair", core=False)(keep, swap_cores(send))
        came, later = lax.optimization_barrier((exchange(chip_sum), later))
        copies = vmem_call(make_sum(chips, rows), packed, 1, name="add_up", core=False)(came)
        mine = exchange(copies)
        return mine, swap_cores(mine), later

    def change_of(mine, other, tile, mean, next_sums, own=None):
        change = vmem_call(make_update(half, rows, own), shared, 5, name="update")(
            core, mine, other, tile, mean, next_sums
        )
        return round_cells(change)

    def factor_of(mine, other):
        return vmem_call(make_factor(half, rows), square, 2, flops=10**9, name="factor")(core, mine, other)

    def advance(parts, stepped, inverse, next_tile):
        inputs = [*parts, stepped, *inverse, next_tile]
        return vmem_call(
            make_middle(batch, bool(inverse)), (packed, packed, local, row), len(inputs), name="middle"
        )(core, *inputs)

    def one_step(state):
        step, keep, send, stepped, mean, tile = state
        following = step + 1
        picks = lax.dynamic_index_in_dim(chosen, following, keepdims=False)
        following, picks, send = lax.optimization_barrier((following, picks, send))
        mine, other, picks = scores_of(keep, send, picks)
        next_tile = tile_of(picks)
        parts = change_of(mine, other, tile, mean, sums_of(next_tile))
        inverse = (factor_of(mine, other),)
        return (following, *advance(parts, stepped, inverse, next_tile), next_tile)

    mine, other, picks = scores_of(keep, send, chosen[:2])
    tile, next_tile = jnp.split(tile_of(picks.reshape(-1)), 2)
    parts = change_of(mine, other, tile, sums_of(tile), sums_of(next_tile), cells)
    state = (*advance(parts, loadings_init, (), next_tile), next_tile)
    _, keep, send, stepped, mean, tile = lax.while_loop(
        lambda state: state[0] < steps - 1, one_step, (jnp.int32(1), *state)
    )
    mine, other, _ = scores_of(keep, send, ())
    parts = change_of(mine, other, tile, mean, mean)
    inverse = factor_of(mine, other)
    few = jax.ShapeDtypeStruct((comps // 4, 2 * comps), f32)
    many = jax.ShapeDtypeStruct((chips, comps // 4, 2 * comps), f32)
    keep, send, stepped = vmem_call(make_last(batch), (few, few, local), len(parts) + 2, name="last")(
        core, *parts, stepped, inverse
    )
    copies = vmem_call(copies_kernel, many, 2, name="copies", core=False)(keep, swap_cores(send))
    came = lax.all_to_all(copies, "gene", 0, 0, tiled=True, axis_index_groups=same_core)
    mine = vmem_call(total_kernel, few, 1, name="total", core=False)(came)
    scale = math.sqrt(genes * gene_devices)
    return vmem_call(make_finish(scale), local, 3, name="finish", held=False)(
        core, mine, swap_cores(mine), stepped
    )


def solution(mesh):
    placed = (P("gene", "cell"), P(None, "cell"), P(None, "gene"))
    return jax.shard_map(
        shards, mesh=mesh, in_specs=placed, out_specs=P(None, "gene"), check_vma=False
    )
```

```python
import math

import jax
import jax.numpy as jnp
from jax import lax
from jax.experimental import pallas as pl
from jax.experimental.pallas import tpu as pltpu
from jax.sharding import PartitionSpec as P

f32 = jnp.float32
bf16 = jnp.bfloat16
STEP_RATE = 1.0
HIGH = lax.Precision.HIGHEST
NT = (((1,), (1,)), ((), ()))
NN = (((1,), (0,)), ((), ()))


def vmem_call(kernel, outs, count, flops=0, name=None, core=True, pool=0, scratch=(), held=True):
    spec = pl.BlockSpec(memory_space=pltpu.VMEM)
    call = pl.pallas_call(
        kernel,
        out_shape=jax.tree.map(lambda s: pltpu.VMEM(s.shape, s.dtype), outs) if held else outs,
        in_specs=[pl.BlockSpec(memory_space=pltpu.SMEM)] * core
        + [spec] * count
        + [pl.BlockSpec(memory_space=pl.ANY)] * pool,
        out_specs=jax.tree.map(lambda _: spec, outs),
        cost_estimate=pl.CostEstimate(flops=flops, transcendentals=0, bytes_accessed=0),
        scratch_shapes=scratch,
        name=name,
    )

    def run(*args):
        last = core + count
        near = [pltpu.with_memory_space_constraint(a, pltpu.VMEM) for a in args[core:last]]
        return call(*args[:core], *near, *args[last:])

    return run


def split_pair(value):
    high = value.astype(bf16)
    low = (value - high.astype(f32)).astype(bf16)
    return jnp.concatenate([high, low], axis=0)


def gram_of(stepped):
    return lax.dot_general(stepped, stepped, NT, precision=HIGH, preferred_element_type=f32)


def by_core(first, mine, other):
    return jnp.concatenate([jnp.where(first, mine, other), jnp.where(first, other, mine)], axis=0)


def spread(scores, gram, first, keep_ref, send_ref):
    comps = scores.shape[0]
    half = comps // 2
    gram = jnp.concatenate([gram, jnp.zeros((comps, 128 - comps), f32)], axis=1)
    rows = scores.shape[1] // 128 + 1
    for j in range(rows):
        chunk = scores[:, j * 128 : (j + 1) * 128] if j + 1 < rows else gram
        top, bottom = chunk[:half], chunk[half:]
        keep_ref[pl.ds(j, half, stride=rows), :] = jnp.where(first, top, bottom)
        send_ref[pl.ds(j, half, stride=rows), :] = jnp.where(first, bottom, top)


def pack_partial(stepped, tile, shift, first, keep_ref, send_ref):
    comps = stepped.shape[0]
    both = lax.dot_general(split_pair(stepped), tile, NT, preferred_element_type=f32)
    spread(both[:comps] + both[comps:] - shift, gram_of(stepped), first, keep_ref, send_ref)


def first_kernel(core_ref, cell_ref, loadings_ref, picks_ref, pool_ref, keep_ref, send_ref, start_ref, names_ref, buffer_ref, sems):
    chunks, _, size = buffer_ref.shape
    near = [
        pltpu.make_async_copy(loadings_ref, start_ref, sems.at[chunks]),
        pltpu.make_async_copy(picks_ref, names_ref, sems.at[chunks + 1]),
    ]
    copies = [
        pltpu.make_async_copy(pool_ref.at[:, pl.ds(i * size, size)], buffer_ref.at[i], sems.at[i])
        for i in range(chunks)
    ]
    for copy in near + copies:
        copy.start()
    for copy in near:
        copy.wait()
    loadings = start_ref[...]
    comps = loadings.shape[0]
    pair = split_pair(loadings)
    picks = names_ref[0:1, :] - cell_ref[0]
    places = lax.broadcasted_iota(jnp.int32, (size, picks.shape[1]), 0)
    chosen = jnp.zeros((2 * comps, picks.shape[1]), f32)
    for i, copy in enumerate(copies):
        copy.wait()
        both = lax.dot_general(pair, buffer_ref[i], NN, preferred_element_type=f32)
        every = split_pair(both[:comps] + both[comps:])
        one_hot = jnp.where(places == picks - i * size, 1.0, 0.0).astype(bf16)
        chosen = chosen + lax.dot_general(every, one_hot, NN, preferred_element_type=f32)
    spread(chosen[:comps] + chosen[comps:], gram_of(loadings), core_ref[0] == 0, keep_ref, send_ref)


def add_kernel(a, b, out_ref):
    out_ref[...] = a[...] + b[...]


def stepped_from(parts, previous, inverse, batch, left=0.0):
    comps, genes = previous.shape
    total = sum(part[:comps, :genes].astype(f32) for part in parts) + left
    stepped = previous + STEP_RATE * (total * (1.0 / batch))
    if inverse is not None:
        stepped = lax.dot_general(inverse, stepped, NN, precision=HIGH, preferred_element_type=f32)
    return stepped


def pair_rows(part, start, genes):
    return part[start : start + 1, :genes].astype(f32) + part[start + 1 : start + 2, :genes].astype(f32)


def between_groups(parts, comps, genes, batch):
    sums = [pair_rows(part, comps + 2, genes) for part in parts]
    mean = sum(sums) * (1.0 / batch)
    total = jnp.zeros((comps, genes), f32)
    for part, own in zip(parts, sums):
        totals = part[:comps, genes : genes + 1].astype(f32) + part[:comps, genes + 1 : genes + 2].astype(f32)
        total = total + totals * (own * (len(parts) / batch) - mean)
    return total


def make_middle(batch, normalised):
    def kernel(core_ref, a, b, c, d, previous_ref, *refs):
        inverse = refs[0][...] if normalised else None
        tile_ref, keep_ref, send_ref, stepped_ref, mean_ref = refs[-5:]
        comps, genes = previous_ref.shape
        parts = (a, b, c, d)
        left = 0.0 if normalised else between_groups(parts, comps, genes, batch)
        stepped = stepped_from(parts, previous_ref[...], inverse, batch, left)
        stepped_ref[...] = stepped
        mean = sum(pair_rows(part, comps, genes) for part in parts) * (1.0 / batch)
        mean_ref[...] = mean
        shift = jnp.sum(stepped * mean, axis=1, keepdims=True)
        pack_partial(stepped, tile_ref[...], shift, core_ref[0] == 0, keep_ref, send_ref)

    return kernel


def make_last(batch):
    def kernel(core_ref, a, b, c, d, previous_ref, inverse_ref, keep_ref, send_ref, stepped_ref):
        stepped = stepped_from((a, b, c, d), previous_ref[...], inverse_ref[...], batch)
        stepped_ref[...] = stepped
        gram = gram_of(stepped)
        quarter = gram.shape[0] // 4
        top = jnp.concatenate([gram[:quarter], gram[quarter : 2 * quarter]], axis=1)
        bottom = jnp.concatenate([gram[2 * quarter : 3 * quarter], gram[3 * quarter :]], axis=1)
        first = core_ref[0] == 0
        keep_ref[...] = jnp.where(first, top, bottom)
        send_ref[...] = jnp.where(first, bottom, top)

    return kernel


def make_sum(count, rows):
    def kernel(in_ref, out_ref):
        for j in range(rows):
            total = jnp.sum(in_ref[pl.ds(j, count, stride=rows), :], axis=0, keepdims=True)
            out_ref[pl.ds(j, count, stride=rows), :] = jnp.broadcast_to(total, (count, 128))

    return kernel


def make_update(half, rows, cells=None):
    def kernel(core_ref, mine_ref, other_ref, tile_ref, mean_ref, next_ref, out_ref):
        genes = tile_ref.shape[1]
        comps = 2 * half
        width = out_ref.shape[1]
        chunks = [
            by_core(
                core_ref[0] == 0,
                mine_ref[pl.ds(j, half, stride=rows), :],
                other_ref[pl.ds(j, half, stride=rows), :],
            )
            for j in range(rows - 1)
        ]
        scores = jnp.concatenate(chunks, axis=1)
        both = lax.dot_general(split_pair(scores), tile_ref[...], NN, preferred_element_type=f32)
        totals = jnp.sum(scores, axis=1, keepdims=True)
        mean = mean_ref[...] * (1.0 / cells) if cells else mean_ref[...]
        raw = both[:comps] + both[comps:] - totals * mean
        rest = out_ref.shape[0] - comps - 4
        tall = jnp.concatenate(
            [
                raw.astype(bf16),
                split_pair(next_ref[...]),
                split_pair(mean_ref[...]),
                jnp.zeros((rest, genes), bf16),
            ],
            axis=0,
        )
        high = totals.astype(bf16)
        low = (totals - high.astype(f32)).astype(bf16)
        side = jnp.concatenate([high, low, jnp.zeros((comps, width - genes - 2), bf16)], axis=1)
        side = jnp.concatenate([side, jnp.zeros((tall.shape[0] - comps, width - genes), bf16)], axis=0)
        out_ref[...] = jnp.concatenate([tall, side], axis=1)

    return kernel


def inverse_factor(gram):
    size = gram.shape[0]
    shape = (8, 2 * size)
    rows = lax.broadcasted_iota(jnp.int32, shape, 0)
    lanes = lax.broadcasted_iota(jnp.int32, shape, 1)
    blocks = []
    for b in range(size // 8):
        eye = jnp.where(lanes == rows + (b * 8 + size), 1.0, 0.0).astype(f32)
        left = jnp.concatenate([gram[b * 8 : b * 8 + 8, :], jnp.zeros((8, size), f32)], axis=1)
        blocks.append(left + eye)
    results = list(blocks)
    for k in range(0, size, 2):
        b, r = divmod(k, 8)
        upper = blocks[b][r : r + 1, :]
        lower = blocks[b][r + 1 : r + 2, :]
        columns = [
            tuple(jnp.broadcast_to(blocks[i][:, k + h : k + h + 1], shape) for h in range(2))
            for i in range(b, size // 8)
        ]
        p = columns[0][0][r : r + 1, :]
        q = columns[0][0][r + 1 : r + 2, :]
        t = columns[0][1][r + 1 : r + 2, :]
        over = 1.0 / (p * t - q * q)
        first = (t * upper - q * lower) * over
        second = (p * lower - q * upper) * over
        inverse_p = 1.0 / p
        slope = q * inverse_p
        top = upper * lax.rsqrt(p)
        low = (lower - slope * upper) * lax.rsqrt(t - slope * q)
        results[b] = jnp.where(rows == r, top, jnp.where(rows == r + 1, low, results[b]))
        for i in range(b, size // 8):
            x, y = columns[i - b]
            change = x * first + y * second
            if i == b:
                change = jnp.where(rows > r + 1, change, 0.0)
            blocks[i] = blocks[i] - change
    return jnp.concatenate(results, axis=0)[:, size:]


def make_factor(half, rows):
    def kernel(core_ref, mine_ref, other_ref, out_ref):
        gram = by_core(
            core_ref[0] == 0,
            mine_ref[pl.ds(rows - 1, half, stride=rows), :],
            other_ref[pl.ds(rows - 1, half, stride=rows), :],
        )
        out_ref[...] = inverse_factor(gram[:, : 2 * half])

    return kernel


def copies_kernel(a, b, out_ref):
    out_ref[...] = jnp.broadcast_to((a[...] + b[...])[None], out_ref.shape)


def total_kernel(in_ref, out_ref):
    out_ref[...] = jnp.sum(in_ref[...], axis=0)


def make_finish(scale):
    def kernel(core_ref, mine_ref, other_ref, stepped_ref, out_ref):
        comps = stepped_ref.shape[0]
        total = by_core(core_ref[0] == 0, mine_ref[...], other_ref[...])
        quarter = comps // 4
        gram = jnp.concatenate(
            [total[h : h + quarter, w : w + comps] for h in (0, quarter) for w in (0, comps)], axis=0
        )
        out_ref[...] = scale * lax.dot_general(
            inverse_factor(gram), stepped_ref[...], NN, precision=HIGH, preferred_element_type=f32
        )

    return kernel


def shards(pool_counts, cell_picks, loadings_init):
    comps, genes = loadings_init.shape
    steps, cells = cell_picks.shape
    half = comps // 2
    local_pool = pool_counts.shape[1]
    cell_devices = lax.axis_size("cell")
    gene_devices = lax.axis_size("gene")
    chips = gene_devices // 2
    batch = cells * cell_devices
    rows = cells // 128 + 1
    width = genes + 128 - genes % 128
    first_cell = lax.axis_index("cell").astype(jnp.int32) * local_pool
    core = (lax.axis_index("gene") % 2).astype(jnp.int32).reshape(1)
    chosen = cell_picks - first_cell
    pool_by_cell = pool_counts.T
    same_core = [[2 * chip + which for chip in range(chips)] for which in range(2)]

    def tile_of(picks):
        return jnp.take(pool_by_cell, picks, axis=0, mode="clip")

    def sums_of(tile):
        return jnp.sum(tile, axis=0, dtype=f32, keepdims=True)

    def swap_cores(value):
        return lax.ppermute(value, "gene", [(i, i ^ 1) for i in range(gene_devices)])

    def round_cells(value):
        return [value] + [
            lax.ppermute(value, "cell", [(i, (i + k) % cell_devices) for i in range(cell_devices)])
            for k in range(1, cell_devices)
        ]

    def exchange(value):
        pieces = value.reshape(chips, 1, value.size // chips)
        arrived = lax.all_to_all(pieces, "gene", 0, 0, tiled=True, axis_index_groups=same_core)
        return arrived.reshape(value.shape)

    packed = jax.ShapeDtypeStruct((half * rows, 128), f32)
    square = jax.ShapeDtypeStruct((comps, comps), f32)
    local = jax.ShapeDtypeStruct((comps, genes), f32)
    row = jax.ShapeDtypeStruct((1, genes), f32)
    shared = jax.ShapeDtypeStruct((comps + 8, width), bf16)

    chunk = local_pool // 8
    keep, send = vmem_call(
        first_kernel,
        (packed, packed),
        0,
        name="first",
        core=2,
        pool=3,
        scratch=[
            pltpu.VMEM((comps, genes), f32),
            pltpu.VMEM((steps, cells), jnp.int32),
            pltpu.VMEM((8, genes, chunk), bf16),
            pltpu.SemaphoreType.DMA((10,)),
        ],
    )(core, first_cell.reshape(1), loadings_init, cell_picks, pool_counts)

    def scores_of(keep, send, later):
        chip_sum = vmem_call(add_kernel, packed, 2, name="pair", core=False)(keep, swap_cores(send))
        came, later = lax.optimization_barrier((exchange(chip_sum), later))
        copies = vmem_call(make_sum(chips, rows), packed, 1, name="add_up", core=False)(came)
        mine = exchange(copies)
        return mine, swap_cores(mine), later

    def change_of(mine, other, tile, mean, next_sums, own=None):
        change = vmem_call(make_update(half, rows, own), shared, 5, name="update")(
            core, mine, other, tile, mean, next_sums
        )
        return round_cells(change)

    def factor_of(mine, other):
        return vmem_call(make_factor(half, rows), square, 2, flops=10**9, name="factor")(core, mine, other)

    def advance(parts, stepped, inverse, next_tile):
        inputs = [*parts, stepped, *inverse, next_tile]
        return vmem_call(
            make_middle(batch, bool(inverse)), (packed, packed, local, row), len(inputs), name="middle"
        )(core, *inputs)

    def one_step(state):
        step, keep, send, stepped, mean, tile = state
        following = step + 1
        picks = lax.dynamic_index_in_dim(chosen, following, keepdims=False)
        following, picks, send = lax.optimization_barrier((following, picks, send))
        mine, other, picks = scores_of(keep, send, picks)
        next_tile = tile_of(picks)
        parts = change_of(mine, other, tile, mean, sums_of(next_tile))
        inverse = (factor_of(mine, other),)
        return (following, *advance(parts, stepped, inverse, next_tile), next_tile)

    mine, other, picks = scores_of(keep, send, chosen[:2])
    tile, next_tile = jnp.split(tile_of(picks.reshape(-1)), 2)
    parts = change_of(mine, other, tile, sums_of(tile), sums_of(next_tile), cells)
    state = (*advance(parts, loadings_init, (), next_tile), next_tile)
    _, keep, send, stepped, mean, tile = lax.while_loop(
        lambda state: state[0] < steps - 1, one_step, (jnp.int32(1), *state)
    )
    mine, other, _ = scores_of(keep, send, ())
    parts = change_of(mine, other, tile, mean, mean)
    inverse = factor_of(mine, other)
    few = jax.ShapeDtypeStruct((comps // 4, 2 * comps), f32)
    many = jax.ShapeDtypeStruct((chips, comps // 4, 2 * comps), f32)
    keep, send, stepped = vmem_call(make_last(batch), (few, few, local), len(parts) + 2, name="last")(
        core, *parts, stepped, inverse
    )
    copies = vmem_call(copies_kernel, many, 2, name="copies", core=False)(keep, swap_cores(send))
    came = lax.all_to_all(copies, "gene", 0, 0, tiled=True, axis_index_groups=same_core)
    mine = vmem_call(total_kernel, few, 1, name="total", core=False)(came)
    scale = math.sqrt(genes * gene_devices)
    return vmem_call(make_finish(scale), local, 3, name="finish", held=False)(
        core, mine, swap_cores(mine), stepped
    )


def solution(mesh):
    placed = (P("gene", "cell"), P(None, "cell"), P(None, "gene"))
    return jax.shard_map(
        shards, mesh=mesh, in_specs=placed, out_specs=P(None, "gene"), check_vma=False
    )
```

```python
import math

import jax
import jax.numpy as jnp
from jax import lax
from jax.experimental import pallas as pl
from jax.experimental.pallas import tpu as pltpu
from jax.sharding import PartitionSpec as P

f32 = jnp.float32
bf16 = jnp.bfloat16
STEP_RATE = 1.0
HIGH = lax.Precision.HIGHEST
NT = (((1,), (1,)), ((), ()))
NN = (((1,), (0,)), ((), ()))


def vmem_call(kernel, outs, count, flops=0, name=None, core=True, pool=0, scratch=(), held=True):
    spec = pl.BlockSpec(memory_space=pltpu.VMEM)
    call = pl.pallas_call(
        kernel,
        out_shape=jax.tree.map(lambda s: pltpu.VMEM(s.shape, s.dtype), outs) if held else outs,
        in_specs=[pl.BlockSpec(memory_space=pltpu.SMEM)] * core
        + [spec] * count
        + [pl.BlockSpec(memory_space=pl.ANY)] * pool,
        out_specs=jax.tree.map(lambda _: spec, outs),
        cost_estimate=pl.CostEstimate(flops=flops, transcendentals=0, bytes_accessed=0),
        scratch_shapes=scratch,
        name=name,
    )

    def run(*args):
        last = core + count
        near = [pltpu.with_memory_space_constraint(a, pltpu.VMEM) for a in args[core:last]]
        return call(*args[:core], *near, *args[last:])

    return run


def split_pair(value):
    high = value.astype(bf16)
    low = (value - high.astype(f32)).astype(bf16)
    return jnp.concatenate([high, low], axis=0)


def gram_of(stepped):
    return lax.dot_general(stepped, stepped, NT, precision=HIGH, preferred_element_type=f32)


def by_core(first, mine, other):
    return jnp.concatenate([jnp.where(first, mine, other), jnp.where(first, other, mine)], axis=0)


def spread(scores, gram, first, keep_ref, send_ref):
    comps = scores.shape[0]
    half = comps // 2
    gram = jnp.concatenate([gram, jnp.zeros((comps, 128 - comps), f32)], axis=1)
    rows = scores.shape[1] // 128 + 1
    for j in range(rows):
        chunk = scores[:, j * 128 : (j + 1) * 128] if j + 1 < rows else gram
        top, bottom = chunk[:half], chunk[half:]
        keep_ref[pl.ds(j, half, stride=rows), :] = jnp.where(first, top, bottom)
        send_ref[pl.ds(j, half, stride=rows), :] = jnp.where(first, bottom, top)


def pack_partial(stepped, tile, shift, first, keep_ref, send_ref):
    comps = stepped.shape[0]
    both = lax.dot_general(split_pair(stepped), tile, NT, preferred_element_type=f32)
    spread(both[:comps] + both[comps:] - shift, gram_of(stepped), first, keep_ref, send_ref)


def first_kernel(core_ref, cell_ref, loadings_ref, picks_ref, pool_ref, keep_ref, send_ref, start_ref, names_ref, buffer_ref, sems):
    chunks, _, size = buffer_ref.shape
    near = [
        pltpu.make_async_copy(loadings_ref, start_ref, sems.at[chunks]),
        pltpu.make_async_copy(picks_ref, names_ref, sems.at[chunks + 1]),
    ]
    copies = [
        pltpu.make_async_copy(pool_ref.at[:, pl.ds(i * size, size)], buffer_ref.at[i], sems.at[i])
        for i in range(chunks)
    ]
    for copy in near + copies:
        copy.start()
    for copy in near:
        copy.wait()
    loadings = start_ref[...]
    comps = loadings.shape[0]
    pair = split_pair(loadings)
    picks = names_ref[0:1, :] - cell_ref[0]
    places = lax.broadcasted_iota(jnp.int32, (size, picks.shape[1]), 0)
    chosen = jnp.zeros((2 * comps, picks.shape[1]), f32)
    for i, copy in enumerate(copies):
        copy.wait()
        both = lax.dot_general(pair, buffer_ref[i], NN, preferred_element_type=f32)
        every = split_pair(both[:comps] + both[comps:])
        one_hot = jnp.where(places == picks - i * size, 1.0, 0.0).astype(bf16)
        chosen = chosen + lax.dot_general(every, one_hot, NN, preferred_element_type=f32)
    spread(chosen[:comps] + chosen[comps:], gram_of(loadings), core_ref[0] == 0, keep_ref, send_ref)


def add_kernel(a, b, out_ref):
    out_ref[...] = a[...] + b[...]


def stepped_from(parts, previous, inverse, batch, left=0.0):
    comps, genes = previous.shape
    total = sum(part[:comps, :genes].astype(f32) for part in parts) + left
    stepped = previous + STEP_RATE * (total * (1.0 / batch))
    if inverse is not None:
        stepped = lax.dot_general(inverse, stepped, NN, precision=HIGH, preferred_element_type=f32)
    return stepped


def pair_rows(part, start, genes):
    return part[start : start + 1, :genes].astype(f32) + part[start + 1 : start + 2, :genes].astype(f32)


def between_groups(parts, comps, genes, batch):
    sums = [pair_rows(part, comps + 2, genes) for part in parts]
    mean = sum(sums) * (1.0 / batch)
    total = jnp.zeros((comps, genes), f32)
    for part, own in zip(parts, sums):
        totals = part[:comps, genes : genes + 1].astype(f32) + part[:comps, genes + 1 : genes + 2].astype(f32)
        total = total + totals * (own * (len(parts) / batch) - mean)
    return total


def make_middle(batch, normalised):
    def kernel(core_ref, a, b, c, d, previous_ref, *refs):
        inverse = refs[0][...] if normalised else None
        if normalised:
            tile_ref, keep_ref, send_ref, stepped_ref, mean_ref = refs[1:]
        else:
            tiles_ref, keep_ref, send_ref, stepped_ref, mean_ref, tile_ref = refs
            tile_ref[...] = tiles_ref[tile_ref.shape[0] :, :]
        comps, genes = previous_ref.shape
        parts = (a, b, c, d)
        left = 0.0 if normalised else between_groups(parts, comps, genes, batch)
        stepped = stepped_from(parts, previous_ref[...], inverse, batch, left)
        stepped_ref[...] = stepped
        mean = sum(pair_rows(part, comps, genes) for part in parts) * (1.0 / batch)
        mean_ref[...] = mean
        shift = jnp.sum(stepped * mean, axis=1, keepdims=True)
        pack_partial(stepped, tile_ref[...], shift, core_ref[0] == 0, keep_ref, send_ref)

    return kernel


def lay_out(block):
    return jnp.concatenate([block[h : h + 8] for h in range(0, 32, 8)], axis=1)


def gather_up(rows):
    return jnp.concatenate([rows[:, w : w + 32] for w in range(0, 128, 32)], axis=0)


def make_last(batch):
    def kernel(core_ref, a, b, c, d, previous_ref, inverse_ref, keep_ref, send_ref, stepped_ref):
        stepped = stepped_from((a, b, c, d), previous_ref[...], inverse_ref[...], batch)
        stepped_ref[...] = stepped
        gram = gram_of(stepped)
        half = gram.shape[0] // 2
        rows = lax.broadcasted_iota(jnp.int32, (half, half), 0)
        columns = lax.broadcasted_iota(jnp.int32, (half, half), 1)
        upper, lower = gram[:half, :half], gram[half:, half:]
        corner = lay_out(gram[half:, :half])
        triangles = lay_out(jnp.where(rows >= columns, upper, lower))
        diagonal = jnp.sum(jnp.where(rows == columns, lower, 0.0), axis=0, keepdims=True)
        diagonal = jnp.concatenate([diagonal, jnp.zeros((1, 128 - half), f32)], axis=1)
        first = core_ref[0] == 0
        nothing = jnp.zeros((1, 128), f32)
        keep_ref[:8, :] = jnp.where(first, corner, triangles)
        keep_ref[8:9, :] = jnp.where(first, nothing, diagonal)
        send_ref[:8, :] = jnp.where(first, triangles, corner)
        send_ref[8:9, :] = jnp.where(first, diagonal, nothing)

    return kernel


def make_sum(count, rows):
    def kernel(in_ref, out_ref):
        for j in range(rows):
            total = jnp.sum(in_ref[pl.ds(j, count, stride=rows), :], axis=0, keepdims=True)
            out_ref[pl.ds(j, count, stride=rows), :] = jnp.broadcast_to(total, (count, 128))

    return kernel


def make_update(half, rows, cells=None):
    def kernel(core_ref, mine_ref, other_ref, tile_ref, mean_ref, next_ref, out_ref):
        genes = tile_ref.shape[1]
        comps = 2 * half
        width = out_ref.shape[1]
        chunks = [
            by_core(
                core_ref[0] == 0,
                mine_ref[pl.ds(j, half, stride=rows), :],
                other_ref[pl.ds(j, half, stride=rows), :],
            )
            for j in range(rows - 1)
        ]
        scores = jnp.concatenate(chunks, axis=1)
        tile = tile_ref[: scores.shape[1], :]
        both = lax.dot_general(split_pair(scores), tile, NN, preferred_element_type=f32)
        totals = jnp.sum(scores, axis=1, keepdims=True)
        mean = mean_ref[...] * (1.0 / cells) if cells else mean_ref[...]
        raw = both[:comps] + both[comps:] - totals * mean
        rest = out_ref.shape[0] - comps - 4
        tall = jnp.concatenate(
            [
                raw.astype(bf16),
                split_pair(next_ref[...]),
                split_pair(mean_ref[...]),
                jnp.zeros((rest, genes), bf16),
            ],
            axis=0,
        )
        high = totals.astype(bf16)
        low = (totals - high.astype(f32)).astype(bf16)
        side = jnp.concatenate([high, low, jnp.zeros((comps, width - genes - 2), bf16)], axis=1)
        side = jnp.concatenate([side, jnp.zeros((tall.shape[0] - comps, width - genes), bf16)], axis=0)
        out_ref[...] = jnp.concatenate([tall, side], axis=1)

    return kernel


def inverse_factor(gram):
    size = gram.shape[0]
    shape = (8, 2 * size)
    rows = lax.broadcasted_iota(jnp.int32, shape, 0)
    lanes = lax.broadcasted_iota(jnp.int32, shape, 1)
    blocks = []
    for b in range(size // 8):
        eye = jnp.where(lanes == rows + (b * 8 + size), 1.0, 0.0).astype(f32)
        left = jnp.concatenate([gram[b * 8 : b * 8 + 8, :], jnp.zeros((8, size), f32)], axis=1)
        blocks.append(left + eye)
    results = list(blocks)
    for k in range(0, size, 2):
        b, r = divmod(k, 8)
        upper = blocks[b][r : r + 1, :]
        lower = blocks[b][r + 1 : r + 2, :]
        columns = [
            tuple(jnp.broadcast_to(blocks[i][:, k + h : k + h + 1], shape) for h in range(2))
            for i in range(b, size // 8)
        ]
        p = columns[0][0][r : r + 1, :]
        q = columns[0][0][r + 1 : r + 2, :]
        t = columns[0][1][r + 1 : r + 2, :]
        over = 1.0 / (p * t - q * q)
        first = (t * upper - q * lower) * over
        second = (p * lower - q * upper) * over
        inverse_p = 1.0 / p
        slope = q * inverse_p
        top = upper * lax.rsqrt(p)
        low = (lower - slope * upper) * lax.rsqrt(t - slope * q)
        results[b] = jnp.where(rows == r, top, jnp.where(rows == r + 1, low, results[b]))
        for i in range(b, size // 8):
            x, y = columns[i - b]
            change = x * first + y * second
            if i == b:
                change = jnp.where(rows > r + 1, change, 0.0)
            blocks[i] = blocks[i] - change
    return jnp.concatenate(results, axis=0)[:, size:]


def make_factor(half, rows):
    def kernel(core_ref, mine_ref, other_ref, out_ref):
        gram = by_core(
            core_ref[0] == 0,
            mine_ref[pl.ds(rows - 1, half, stride=rows), :],
            other_ref[pl.ds(rows - 1, half, stride=rows), :],
        )
        out_ref[...] = inverse_factor(gram[:, : 2 * half])

    return kernel


def copies_kernel(a, b, out_ref):
    rows = a.shape[0]
    count = out_ref.shape[0] // rows
    total = a[...] + b[...]
    for j in range(rows):
        out_ref[pl.ds(j, count, stride=rows), :] = jnp.broadcast_to(total[j : j + 1], (count, 128))


def total_kernel(in_ref, out_ref):
    rows = out_ref.shape[0]
    count = in_ref.shape[0] // rows
    for j in range(rows):
        out_ref[j : j + 1, :] = jnp.sum(in_ref[pl.ds(j, count, stride=rows), :], axis=0, keepdims=True)


def make_finish(scale):
    def kernel(core_ref, mine_ref, other_ref, stepped_ref, out_ref):
        first = core_ref[0] == 0
        corner = gather_up(jnp.where(first, mine_ref[:8, :], other_ref[:8, :]))
        triangles = gather_up(jnp.where(first, other_ref[:8, :], mine_ref[:8, :]))
        half = corner.shape[0]
        diagonal = jnp.where(first, other_ref[8:9, :half], mine_ref[8:9, :half])
        rows = lax.broadcasted_iota(jnp.int32, (half, half), 0)
        columns = lax.broadcasted_iota(jnp.int32, (half, half), 1)
        eye = jnp.where(rows == columns, 1.0, 0.0).astype(f32)

        def turned(block):
            return lax.dot_general(block, eye, (((0,), (0,)), ((), ())), precision=HIGH, preferred_element_type=f32)

        across = turned(triangles)
        upper = jnp.where(rows >= columns, triangles, across)
        lower = jnp.where(rows < columns, triangles, across)
        lower = jnp.where(rows == columns, jnp.broadcast_to(diagonal, (half, half)), lower)
        gram = jnp.concatenate(
            [
                jnp.concatenate([upper, turned(corner)], axis=1),
                jnp.concatenate([corner, lower], axis=1),
            ],
            axis=0,
        )
        out_ref[...] = scale * lax.dot_general(
            inverse_factor(gram), stepped_ref[...], NN, precision=HIGH, preferred_element_type=f32
        )

    return kernel


def shards(pool_counts, cell_picks, loadings_init):
    comps, genes = loadings_init.shape
    steps, cells = cell_picks.shape
    half = comps // 2
    local_pool = pool_counts.shape[1]
    cell_devices = lax.axis_size("cell")
    gene_devices = lax.axis_size("gene")
    chips = gene_devices // 2
    batch = cells * cell_devices
    rows = cells // 128 + 1
    width = genes + 128 - genes % 128
    first_cell = lax.axis_index("cell").astype(jnp.int32) * local_pool
    core = (lax.axis_index("gene") % 2).astype(jnp.int32).reshape(1)
    chosen = cell_picks - first_cell
    pool_by_cell = pool_counts.T
    same_core = [[2 * chip + which for chip in range(chips)] for which in range(2)]

    def tile_of(picks):
        return jnp.take(pool_by_cell, picks, axis=0, mode="clip")

    def sums_of(tile):
        return jnp.sum(tile, axis=0, dtype=f32, keepdims=True)

    def swap_cores(value):
        return lax.ppermute(value, "gene", [(i, i ^ 1) for i in range(gene_devices)])

    def round_cells(value):
        return [value] + [
            lax.ppermute(value, "cell", [(i, (i + k) % cell_devices) for i in range(cell_devices)])
            for k in range(1, cell_devices)
        ]

    def exchange(value):
        pieces = value.reshape(chips, 1, value.size // chips)
        arrived = lax.all_to_all(pieces, "gene", 0, 0, tiled=True, axis_index_groups=same_core)
        return arrived.reshape(value.shape)

    packed = jax.ShapeDtypeStruct((half * rows, 128), f32)
    square = jax.ShapeDtypeStruct((comps, comps), f32)
    local = jax.ShapeDtypeStruct((comps, genes), f32)
    row = jax.ShapeDtypeStruct((1, genes), f32)
    shared = jax.ShapeDtypeStruct((comps + 8, width), bf16)

    chunk = local_pool // 8
    keep, send = vmem_call(
        first_kernel,
        (packed, packed),
        0,
        name="first",
        core=2,
        pool=3,
        scratch=[
            pltpu.VMEM((comps, genes), f32),
            pltpu.VMEM((steps, cells), jnp.int32),
            pltpu.VMEM((8, genes, chunk), bf16),
            pltpu.SemaphoreType.DMA((10,)),
        ],
    )(core, first_cell.reshape(1), loadings_init, cell_picks, pool_counts)

    def scores_of(keep, send, later):
        chip_sum = vmem_call(add_kernel, packed, 2, name="pair", core=False)(keep, swap_cores(send))
        came, later = lax.optimization_barrier((exchange(chip_sum), later))
        copies = vmem_call(make_sum(chips, rows), packed, 1, name="add_up", core=False)(came)
        mine = exchange(copies)
        return mine, swap_cores(mine), later

    def change_of(mine, other, tile, mean, next_sums, own=None):
        change = vmem_call(make_update(half, rows, own), shared, 5, name="update")(
            core, mine, other, tile, mean, next_sums
        )
        return round_cells(change)

    def factor_of(mine, other):
        return vmem_call(make_factor(half, rows), square, 2, flops=10**9, name="factor")(core, mine, other)

    def advance(parts, stepped, inverse, next_tile):
        inputs = [*parts, stepped, inverse, next_tile]
        return vmem_call(make_middle(batch, True), (packed, packed, local, row), len(inputs), name="middle")(
            core, *inputs
        )

    def one_step(state):
        step, keep, send, stepped, mean, tile = state
        following = step + 1
        picks = lax.dynamic_index_in_dim(chosen, following, keepdims=False)
        following, picks, send = lax.optimization_barrier((following, picks, send))
        mine, other, picks = scores_of(keep, send, picks)
        next_tile = tile_of(picks)
        parts = change_of(mine, other, tile, mean, sums_of(next_tile))
        inverse = factor_of(mine, other)
        return (following, *advance(parts, stepped, inverse, next_tile), next_tile)

    mine, other, picks = scores_of(keep, send, chosen[:2])
    tiles = tile_of(picks.reshape(-1))
    both_sums = jnp.sum(tiles.reshape(2, cells, genes), axis=1, dtype=f32)
    parts = change_of(mine, other, tiles, both_sums[:1], both_sums[1:], cells)
    state = vmem_call(
        make_middle(batch, False),
        (packed, packed, local, row, jax.ShapeDtypeStruct((cells, genes), bf16)),
        len(parts) + 2,
        name="middle",
    )(core, *parts, loadings_init, tiles)
    _, keep, send, stepped, mean, tile = lax.while_loop(
        lambda state: state[0] < steps - 1, one_step, (jnp.int32(1), *state)
    )
    mine, other, _ = scores_of(keep, send, ())
    parts = change_of(mine, other, tile, mean, mean)
    inverse = factor_of(mine, other)
    few = jax.ShapeDtypeStruct((9, 128), f32)
    many = jax.ShapeDtypeStruct((9 * chips, 128), f32)
    keep, send, stepped = vmem_call(make_last(batch), (few, few, local), len(parts) + 2, name="last")(
        core, *parts, stepped, inverse
    )
    copies = vmem_call(copies_kernel, many, 2, name="copies", core=False)(keep, swap_cores(send))
    mine = vmem_call(total_kernel, few, 1, name="total", core=False)(exchange(copies))
    scale = math.sqrt(genes * gene_devices)
    return vmem_call(make_finish(scale), local, 3, name="finish", held=False)(
        core, mine, swap_cores(mine), stepped
    )


def solution(mesh):
    placed = (P("gene", "cell"), P(None, "cell"), P(None, "gene"))
    return jax.shard_map(
        shards, mesh=mesh, in_specs=placed, out_specs=P(None, "gene"), check_vma=False
    )
```

```python
import math

import jax
import jax.numpy as jnp
from jax import lax
from jax.experimental import pallas as pl
from jax.experimental.pallas import tpu as pltpu
from jax.sharding import PartitionSpec as P

f32 = jnp.float32
bf16 = jnp.bfloat16
STEP_RATE = 1.0
HIGH = lax.Precision.HIGHEST
NT = (((1,), (1,)), ((), ()))
NN = (((1,), (0,)), ((), ()))


def vmem_call(kernel, outs, count, flops=0, name=None, core=True, pool=0, scratch=(), held=True):
    spec = pl.BlockSpec(memory_space=pltpu.VMEM)
    call = pl.pallas_call(
        kernel,
        out_shape=jax.tree.map(lambda s: pltpu.VMEM(s.shape, s.dtype), outs) if held else outs,
        in_specs=[pl.BlockSpec(memory_space=pltpu.SMEM)] * core
        + [spec] * count
        + [pl.BlockSpec(memory_space=pl.ANY)] * pool,
        out_specs=jax.tree.map(lambda _: spec, outs),
        cost_estimate=pl.CostEstimate(flops=flops, transcendentals=0, bytes_accessed=0),
        scratch_shapes=scratch,
        name=name,
    )

    def run(*args):
        last = core + count
        near = [pltpu.with_memory_space_constraint(a, pltpu.VMEM) for a in args[core:last]]
        return call(*args[:core], *near, *args[last:])

    return run


def split_pair(value):
    high = value.astype(bf16)
    low = (value - high.astype(f32)).astype(bf16)
    return jnp.concatenate([high, low], axis=0)


def gram_of(stepped):
    return lax.dot_general(stepped, stepped, NT, precision=HIGH, preferred_element_type=f32)


def by_core(first, mine, other):
    return jnp.concatenate([jnp.where(first, mine, other), jnp.where(first, other, mine)], axis=0)


def spread(scores, gram, first, keep_ref, send_ref):
    comps = scores.shape[0]
    half = comps // 2
    gram = jnp.concatenate([gram, jnp.zeros((comps, 128 - comps), f32)], axis=1)
    rows = scores.shape[1] // 128 + 1
    for j in range(rows):
        chunk = scores[:, j * 128 : (j + 1) * 128] if j + 1 < rows else gram
        top, bottom = chunk[:half], chunk[half:]
        keep_ref[pl.ds(j, half, stride=rows), :] = jnp.where(first, top, bottom)
        send_ref[pl.ds(j, half, stride=rows), :] = jnp.where(first, bottom, top)


def pack_partial(stepped, tile, shift, first, keep_ref, send_ref):
    comps = stepped.shape[0]
    both = lax.dot_general(split_pair(stepped), tile, NT, preferred_element_type=f32)
    spread(both[:comps] + both[comps:] - shift, gram_of(stepped), first, keep_ref, send_ref)


def first_kernel(core_ref, cell_ref, loadings_ref, picks_ref, pool_ref, keep_ref, send_ref, start_ref, names_ref, buffer_ref, sems):
    chunks, _, size = buffer_ref.shape
    near = [
        pltpu.make_async_copy(loadings_ref, start_ref, sems.at[chunks]),
        pltpu.make_async_copy(picks_ref, names_ref, sems.at[chunks + 1]),
    ]
    copies = [
        pltpu.make_async_copy(pool_ref.at[:, pl.ds(i * size, size)], buffer_ref.at[i], sems.at[i])
        for i in range(chunks)
    ]
    for copy in near + copies:
        copy.start()
    for copy in near:
        copy.wait()
    loadings = start_ref[...]
    comps = loadings.shape[0]
    pair = split_pair(loadings)
    picks = names_ref[0:1, :] - cell_ref[0]
    places = lax.broadcasted_iota(jnp.int32, (size, picks.shape[1]), 0)
    chosen = jnp.zeros((2 * comps, picks.shape[1]), f32)
    for i, copy in enumerate(copies):
        copy.wait()
        both = lax.dot_general(pair, buffer_ref[i], NN, preferred_element_type=f32)
        every = split_pair(both[:comps] + both[comps:])
        one_hot = jnp.where(places == picks - i * size, 1.0, 0.0).astype(bf16)
        chosen = chosen + lax.dot_general(every, one_hot, NN, preferred_element_type=f32)
    spread(chosen[:comps] + chosen[comps:], gram_of(loadings), core_ref[0] == 0, keep_ref, send_ref)


def add_kernel(a, b, out_ref):
    out_ref[...] = a[...] + b[...]


def stepped_from(parts, previous, inverse, batch, left=0.0):
    comps, genes = previous.shape
    total = sum(part[:comps, :genes].astype(f32) for part in parts) + left
    stepped = previous + STEP_RATE * (total * (1.0 / batch))
    if inverse is not None:
        stepped = lax.dot_general(inverse, stepped, NN, precision=HIGH, preferred_element_type=f32)
    return stepped


def pair_rows(part, start, genes):
    return part[start : start + 1, :genes].astype(f32) + part[start + 1 : start + 2, :genes].astype(f32)


def between_groups(parts, comps, genes, batch):
    sums = [pair_rows(part, comps + 2, genes) for part in parts]
    mean = sum(sums) * (1.0 / batch)
    total = jnp.zeros((comps, genes), f32)
    for part, own in zip(parts, sums):
        totals = part[:comps, genes : genes + 1].astype(f32) + part[:comps, genes + 1 : genes + 2].astype(f32)
        total = total + totals * (own * (len(parts) / batch) - mean)
    return total


def make_middle(batch, normalised):
    def kernel(core_ref, a, b, c, d, previous_ref, *refs):
        inverse = refs[0][...] if normalised else None
        tile_ref, keep_ref, send_ref, stepped_ref, mean_ref = refs[-5:]
        comps, genes = previous_ref.shape
        parts = (a, b, c, d)
        left = 0.0 if normalised else between_groups(parts, comps, genes, batch)
        stepped = stepped_from(parts, previous_ref[...], inverse, batch, left)
        stepped_ref[...] = stepped
        mean = sum(pair_rows(part, comps, genes) for part in parts) * (1.0 / batch)
        mean_ref[...] = mean
        shift = jnp.sum(stepped * mean, axis=1, keepdims=True)
        pack_partial(stepped, tile_ref[...], shift, core_ref[0] == 0, keep_ref, send_ref)

    return kernel


def lay_out(block):
    return jnp.concatenate([block[h : h + 8] for h in range(0, 32, 8)], axis=1)


def gather_up(rows):
    return jnp.concatenate([rows[:, w : w + 32] for w in range(0, 128, 32)], axis=0)


def make_last(batch):
    def kernel(core_ref, a, b, c, d, previous_ref, inverse_ref, keep_ref, send_ref, stepped_ref):
        stepped = stepped_from((a, b, c, d), previous_ref[...], inverse_ref[...], batch)
        stepped_ref[...] = stepped
        gram = gram_of(stepped)
        half = gram.shape[0] // 2
        rows = lax.broadcasted_iota(jnp.int32, (half, half), 0)
        columns = lax.broadcasted_iota(jnp.int32, (half, half), 1)
        upper, lower = gram[:half, :half], gram[half:, half:]
        corner = lay_out(gram[half:, :half])
        triangles = lay_out(jnp.where(rows >= columns, upper, lower))
        diagonal = jnp.sum(jnp.where(rows == columns, lower, 0.0), axis=0, keepdims=True)
        diagonal = jnp.concatenate([diagonal, jnp.zeros((1, 128 - half), f32)], axis=1)
        first = core_ref[0] == 0
        nothing = jnp.zeros((1, 128), f32)
        keep_ref[:8, :] = jnp.where(first, corner, triangles)
        keep_ref[8:9, :] = jnp.where(first, nothing, diagonal)
        send_ref[:8, :] = jnp.where(first, triangles, corner)
        send_ref[8:9, :] = jnp.where(first, diagonal, nothing)

    return kernel


def make_sum(count, rows):
    def kernel(in_ref, out_ref):
        for j in range(rows):
            total = jnp.sum(in_ref[pl.ds(j, count, stride=rows), :], axis=0, keepdims=True)
            out_ref[pl.ds(j, count, stride=rows), :] = jnp.broadcast_to(total, (count, 128))

    return kernel


def make_update(half, rows, cells=None):
    def kernel(core_ref, mine_ref, other_ref, tile_ref, mean_ref, next_ref, out_ref):
        genes = tile_ref.shape[1]
        comps = 2 * half
        width = out_ref.shape[1]
        chunks = [
            by_core(
                core_ref[0] == 0,
                mine_ref[pl.ds(j, half, stride=rows), :],
                other_ref[pl.ds(j, half, stride=rows), :],
            )
            for j in range(rows - 1)
        ]
        scores = jnp.concatenate(chunks, axis=1)
        both = lax.dot_general(split_pair(scores), tile_ref[...], NN, preferred_element_type=f32)
        totals = jnp.sum(scores, axis=1, keepdims=True)
        mean = mean_ref[...] * (1.0 / cells) if cells else mean_ref[...]
        raw = both[:comps] + both[comps:] - totals * mean
        rest = out_ref.shape[0] - comps - 4
        tall = jnp.concatenate(
            [
                raw.astype(bf16),
                split_pair(next_ref[...]),
                split_pair(mean_ref[...]),
                jnp.zeros((rest, genes), bf16),
            ],
            axis=0,
        )
        high = totals.astype(bf16)
        low = (totals - high.astype(f32)).astype(bf16)
        side = jnp.concatenate([high, low, jnp.zeros((comps, width - genes - 2), bf16)], axis=1)
        side = jnp.concatenate([side, jnp.zeros((tall.shape[0] - comps, width - genes), bf16)], axis=0)
        out_ref[...] = jnp.concatenate([tall, side], axis=1)

    return kernel


def inverse_factor(gram):
    size = gram.shape[0]
    shape = (8, 2 * size)
    rows = lax.broadcasted_iota(jnp.int32, shape, 0)
    lanes = lax.broadcasted_iota(jnp.int32, shape, 1)
    blocks = []
    for b in range(size // 8):
        eye = jnp.where(lanes == rows + (b * 8 + size), 1.0, 0.0).astype(f32)
        left = jnp.concatenate([gram[b * 8 : b * 8 + 8, :], jnp.zeros((8, size), f32)], axis=1)
        blocks.append(left + eye)
    results = list(blocks)
    for k in range(0, size, 2):
        b, r = divmod(k, 8)
        upper = blocks[b][r : r + 1, :]
        lower = blocks[b][r + 1 : r + 2, :]
        columns = [
            tuple(jnp.broadcast_to(blocks[i][:, k + h : k + h + 1], shape) for h in range(2))
            for i in range(b, size // 8)
        ]
        p = columns[0][0][r : r + 1, :]
        q = columns[0][0][r + 1 : r + 2, :]
        t = columns[0][1][r + 1 : r + 2, :]
        over = 1.0 / (p * t - q * q)
        first = (t * upper - q * lower) * over
        second = (p * lower - q * upper) * over
        inverse_p = 1.0 / p
        slope = q * inverse_p
        top = upper * lax.rsqrt(p)
        low = (lower - slope * upper) * lax.rsqrt(t - slope * q)
        results[b] = jnp.where(rows == r, top, jnp.where(rows == r + 1, low, results[b]))
        for i in range(b, size // 8):
            x, y = columns[i - b]
            change = x * first + y * second
            if i == b:
                change = jnp.where(rows > r + 1, change, 0.0)
            blocks[i] = blocks[i] - change
    return jnp.concatenate(results, axis=0)[:, size:]


def make_factor(half, rows):
    def kernel(core_ref, mine_ref, other_ref, out_ref):
        gram = by_core(
            core_ref[0] == 0,
            mine_ref[pl.ds(rows - 1, half, stride=rows), :],
            other_ref[pl.ds(rows - 1, half, stride=rows), :],
        )
        out_ref[...] = inverse_factor(gram[:, : 2 * half])

    return kernel


def copies_kernel(a, b, out_ref):
    rows = a.shape[0]
    count = out_ref.shape[0] // rows
    total = a[...] + b[...]
    for j in range(rows):
        out_ref[pl.ds(j, count, stride=rows), :] = jnp.broadcast_to(total[j : j + 1], (count, 128))


def total_kernel(in_ref, out_ref):
    rows = out_ref.shape[0]
    count = in_ref.shape[0] // rows
    for j in range(rows):
        out_ref[j : j + 1, :] = jnp.sum(in_ref[pl.ds(j, count, stride=rows), :], axis=0, keepdims=True)


def make_finish(scale):
    def kernel(core_ref, mine_ref, other_ref, stepped_ref, out_ref):
        first = core_ref[0] == 0
        corner = gather_up(jnp.where(first, mine_ref[:8, :], other_ref[:8, :]))
        triangles = gather_up(jnp.where(first, other_ref[:8, :], mine_ref[:8, :]))
        half = corner.shape[0]
        diagonal = jnp.where(first, other_ref[8:9, :half], mine_ref[8:9, :half])
        rows = lax.broadcasted_iota(jnp.int32, (half, half), 0)
        columns = lax.broadcasted_iota(jnp.int32, (half, half), 1)
        eye = jnp.where(rows == columns, 1.0, 0.0).astype(f32)

        def turned(block):
            return lax.dot_general(block, eye, (((0,), (0,)), ((), ())), precision=HIGH, preferred_element_type=f32)

        across = turned(triangles)
        upper = jnp.where(rows >= columns, triangles, across)
        lower = jnp.where(rows < columns, triangles, across)
        lower = jnp.where(rows == columns, jnp.broadcast_to(diagonal, (half, half)), lower)
        gram = jnp.concatenate(
            [
                jnp.concatenate([upper, turned(corner)], axis=1),
                jnp.concatenate([corner, lower], axis=1),
            ],
            axis=0,
        )
        out_ref[...] = scale * lax.dot_general(
            inverse_factor(gram), stepped_ref[...], NN, precision=HIGH, preferred_element_type=f32
        )

    return kernel


def shards(pool_counts, cell_picks, loadings_init):
    comps, genes = loadings_init.shape
    steps, cells = cell_picks.shape
    half = comps // 2
    local_pool = pool_counts.shape[1]
    cell_devices = lax.axis_size("cell")
    gene_devices = lax.axis_size("gene")
    chips = gene_devices // 2
    batch = cells * cell_devices
    rows = cells // 128 + 1
    width = genes + 128 - genes % 128
    first_cell = lax.axis_index("cell").astype(jnp.int32) * local_pool
    core = (lax.axis_index("gene") % 2).astype(jnp.int32).reshape(1)
    chosen = cell_picks - first_cell
    pool_by_cell = pool_counts.T
    same_core = [[2 * chip + which for chip in range(chips)] for which in range(2)]

    def tile_of(picks):
        return jnp.take(pool_by_cell, picks, axis=0, mode="clip")

    def sums_of(tile):
        return jnp.sum(tile, axis=0, dtype=f32, keepdims=True)

    def swap_cores(value):
        return lax.ppermute(value, "gene", [(i, i ^ 1) for i in range(gene_devices)])

    def round_cells(value):
        return [value] + [
            lax.ppermute(value, "cell", [(i, (i + k) % cell_devices) for i in range(cell_devices)])
            for k in range(1, cell_devices)
        ]

    def exchange(value):
        pieces = value.reshape(chips, 1, value.size // chips)
        arrived = lax.all_to_all(pieces, "gene", 0, 0, tiled=True, axis_index_groups=same_core)
        return arrived.reshape(value.shape)

    packed = jax.ShapeDtypeStruct((half * rows, 128), f32)
    square = jax.ShapeDtypeStruct((comps, comps), f32)
    local = jax.ShapeDtypeStruct((comps, genes), f32)
    row = jax.ShapeDtypeStruct((1, genes), f32)
    shared = jax.ShapeDtypeStruct((comps + 8, width), bf16)

    chunk = local_pool // 8
    keep, send = vmem_call(
        first_kernel,
        (packed, packed),
        0,
        name="first",
        core=2,
        pool=3,
        scratch=[
            pltpu.VMEM((comps, genes), f32),
            pltpu.VMEM((steps, cells), jnp.int32),
            pltpu.VMEM((8, genes, chunk), bf16),
            pltpu.SemaphoreType.DMA((10,)),
        ],
    )(core, first_cell.reshape(1), loadings_init, cell_picks, pool_counts)

    def scores_of(keep, send, later):
        chip_sum = vmem_call(add_kernel, packed, 2, name="pair", core=False)(keep, swap_cores(send))
        came, later = lax.optimization_barrier((exchange(chip_sum), later))
        copies = vmem_call(make_sum(chips, rows), packed, 1, name="add_up", core=False)(came)
        mine = exchange(copies)
        return mine, swap_cores(mine), later

    def change_of(mine, other, tile, mean, next_sums, own=None):
        change = vmem_call(make_update(half, rows, own), shared, 5, name="update")(
            core, mine, other, tile, mean, next_sums
        )
        return round_cells(change)

    def factor_of(mine, other):
        return vmem_call(make_factor(half, rows), square, 2, flops=10**9, name="factor")(core, mine, other)

    def advance(parts, stepped, inverse, next_tile):
        inputs = [*parts, stepped, *inverse, next_tile]
        return vmem_call(
            make_middle(batch, bool(inverse)), (packed, packed, local, row), len(inputs), name="middle"
        )(core, *inputs)

    def one_step(state):
        step, keep, send, stepped, mean, tile = state
        following = step + 1
        picks = lax.dynamic_index_in_dim(chosen, following, keepdims=False)
        following, picks, send = lax.optimization_barrier((following, picks, send))
        mine, other, picks = scores_of(keep, send, picks)
        next_tile = tile_of(picks)
        parts = change_of(mine, other, tile, mean, sums_of(next_tile))
        inverse = (factor_of(mine, other),)
        return (following, *advance(parts, stepped, inverse, next_tile), next_tile)

    mine, other, picks = scores_of(keep, send, chosen[:2])
    tile, next_tile = jnp.split(tile_of(picks.reshape(-1)), 2)
    parts = change_of(mine, other, tile, sums_of(tile), sums_of(next_tile), cells)
    state = (*advance(parts, loadings_init, (), next_tile), next_tile)
    _, keep, send, stepped, mean, tile = lax.while_loop(
        lambda state: state[0] < steps - 1, one_step, (jnp.int32(1), *state)
    )
    mine, other, _ = scores_of(keep, send, ())
    parts = change_of(mine, other, tile, mean, mean)
    inverse = factor_of(mine, other)
    few = jax.ShapeDtypeStruct((9, 128), f32)
    many = jax.ShapeDtypeStruct((9 * chips, 128), f32)
    keep, send, stepped = vmem_call(make_last(batch), (few, few, local), len(parts) + 2, name="last")(
        core, *parts, stepped, inverse
    )
    copies = vmem_call(copies_kernel, many, 2, name="copies", core=False)(keep, swap_cores(send))
    mine = vmem_call(total_kernel, few, 1, name="total", core=False)(exchange(copies))
    scale = math.sqrt(genes * gene_devices)
    return vmem_call(make_finish(scale), local, 3, name="finish", held=False)(
        core, mine, swap_cores(mine), stepped
    )


def solution(mesh):
    placed = (P("gene", "cell"), P(None, "cell"), P(None, "gene"))
    return jax.shard_map(
        shards, mesh=mesh, in_specs=placed, out_specs=P(None, "gene"), check_vma=False
    )
```

```python
import math

import jax
import jax.numpy as jnp
from jax import lax
from jax.experimental import pallas as pl
from jax.experimental.pallas import tpu as pltpu
from jax.sharding import PartitionSpec as P

f32 = jnp.float32
bf16 = jnp.bfloat16
STEP_RATE = 1.0
HIGH = lax.Precision.HIGHEST
NT = (((1,), (1,)), ((), ()))
NN = (((1,), (0,)), ((), ()))


def vmem_call(kernel, outs, count, flops=0, name=None, core=True, pool=0, scratch=(), held=True):
    spec = pl.BlockSpec(memory_space=pltpu.VMEM)
    call = pl.pallas_call(
        kernel,
        out_shape=jax.tree.map(lambda s: pltpu.VMEM(s.shape, s.dtype), outs) if held else outs,
        in_specs=[pl.BlockSpec(memory_space=pltpu.SMEM)] * core
        + [spec] * count
        + [pl.BlockSpec(memory_space=pl.ANY)] * pool,
        out_specs=jax.tree.map(lambda _: spec, outs),
        cost_estimate=pl.CostEstimate(flops=flops, transcendentals=0, bytes_accessed=0),
        scratch_shapes=scratch,
        name=name,
    )

    def run(*args):
        last = core + count
        near = [pltpu.with_memory_space_constraint(a, pltpu.VMEM) for a in args[core:last]]
        return call(*args[:core], *near, *args[last:])

    return run


def split_pair(value):
    high = value.astype(bf16)
    low = (value - high.astype(f32)).astype(bf16)
    return jnp.concatenate([high, low], axis=0)


def gram_of(stepped):
    return lax.dot_general(stepped, stepped, NT, precision=HIGH, preferred_element_type=f32)


def by_core(first, mine, other):
    return jnp.concatenate([jnp.where(first, mine, other), jnp.where(first, other, mine)], axis=0)


def spread(scores, gram, first, keep_ref, send_ref):
    comps = scores.shape[0]
    half = comps // 2
    gram = jnp.concatenate([gram, jnp.zeros((comps, 128 - comps), f32)], axis=1)
    rows = scores.shape[1] // 128 + 1
    for j in range(rows):
        chunk = scores[:, j * 128 : (j + 1) * 128] if j + 1 < rows else gram
        top, bottom = chunk[:half], chunk[half:]
        keep_ref[pl.ds(j, half, stride=rows), :] = jnp.where(first, top, bottom)
        send_ref[pl.ds(j, half, stride=rows), :] = jnp.where(first, bottom, top)


def pack_partial(stepped, tile, shift, first, keep_ref, send_ref):
    comps = stepped.shape[0]
    both = lax.dot_general(split_pair(stepped), tile, NT, preferred_element_type=f32)
    spread(both[:comps] + both[comps:] - shift, gram_of(stepped), first, keep_ref, send_ref)


def first_kernel(core_ref, cell_ref, loadings_ref, picks_ref, pool_ref, keep_ref, send_ref, start_ref, names_ref, buffer_ref, sems):
    chunks, _, size = buffer_ref.shape
    near = [
        pltpu.make_async_copy(loadings_ref, start_ref, sems.at[chunks]),
        pltpu.make_async_copy(picks_ref, names_ref, sems.at[chunks + 1]),
    ]
    copies = [
        pltpu.make_async_copy(pool_ref.at[:, pl.ds(i * size, size)], buffer_ref.at[i], sems.at[i])
        for i in range(chunks)
    ]
    for copy in near + copies:
        copy.start()
    for copy in near:
        copy.wait()
    loadings = start_ref[...]
    comps = loadings.shape[0]
    pair = split_pair(loadings)
    picks = names_ref[0:1, :] - cell_ref[0]
    places = lax.broadcasted_iota(jnp.int32, (size, picks.shape[1]), 0)
    chosen = jnp.zeros((2 * comps, picks.shape[1]), f32)
    for i, copy in enumerate(copies):
        copy.wait()
        both = lax.dot_general(pair, buffer_ref[i], NN, preferred_element_type=f32)
        every = split_pair(both[:comps] + both[comps:])
        one_hot = jnp.where(places == picks - i * size, 1.0, 0.0).astype(bf16)
        chosen = chosen + lax.dot_general(every, one_hot, NN, preferred_element_type=f32)
    spread(chosen[:comps] + chosen[comps:], gram_of(loadings), core_ref[0] == 0, keep_ref, send_ref)


def add_kernel(a, b, out_ref):
    out_ref[...] = a[...] + b[...]


def stepped_from(parts, previous, inverse, batch, left=0.0):
    comps, genes = previous.shape
    total = sum(part[:comps, :genes].astype(f32) for part in parts) + left
    stepped = previous + STEP_RATE * (total * (1.0 / batch))
    if inverse is not None:
        stepped = lax.dot_general(inverse, stepped, NN, precision=HIGH, preferred_element_type=f32)
    return stepped


def pair_rows(part, start, genes):
    return part[start : start + 1, :genes].astype(f32) + part[start + 1 : start + 2, :genes].astype(f32)


def between_groups(parts, comps, genes, batch):
    sums = [pair_rows(part, comps + 2, genes) for part in parts]
    mean = sum(sums) * (1.0 / batch)
    total = jnp.zeros((comps, genes), f32)
    for part, own in zip(parts, sums):
        totals = part[:comps, genes : genes + 1].astype(f32) + part[:comps, genes + 1 : genes + 2].astype(f32)
        total = total + totals * (own * (len(parts) / batch) - mean)
    return total


def make_middle(batch, normalised):
    def kernel(core_ref, a, b, c, d, previous_ref, *refs):
        inverse = refs[0][...] if normalised else None
        tile_ref, keep_ref, send_ref, stepped_ref, mean_ref = refs[-5:]
        comps, genes = previous_ref.shape
        parts = (a, b, c, d)
        left = 0.0 if normalised else between_groups(parts, comps, genes, batch)
        stepped = stepped_from(parts, previous_ref[...], inverse, batch, left)
        stepped_ref[...] = stepped
        mean = sum(pair_rows(part, comps, genes) for part in parts) * (1.0 / batch)
        mean_ref[...] = mean
        shift = jnp.sum(stepped * mean, axis=1, keepdims=True)
        pack_partial(stepped, tile_ref[...], shift, core_ref[0] == 0, keep_ref, send_ref)

    return kernel


def lay_out(block):
    return jnp.concatenate([block[h : h + 8] for h in range(0, 32, 8)], axis=1)


def gather_up(rows):
    return jnp.concatenate([rows[:, w : w + 32] for w in range(0, 128, 32)], axis=0)


def make_last(batch):
    def kernel(core_ref, a, b, c, d, previous_ref, inverse_ref, keep_ref, send_ref, stepped_ref):
        stepped = stepped_from((a, b, c, d), previous_ref[...], inverse_ref[...], batch)
        stepped_ref[...] = stepped
        gram = gram_of(stepped)
        half = gram.shape[0] // 2
        rows = lax.broadcasted_iota(jnp.int32, (half, half), 0)
        columns = lax.broadcasted_iota(jnp.int32, (half, half), 1)
        upper, lower = gram[:half, :half], gram[half:, half:]
        corner = lay_out(gram[half:, :half])
        triangles = lay_out(jnp.where(rows >= columns, upper, lower))
        diagonal = jnp.sum(jnp.where(rows == columns, lower, 0.0), axis=0, keepdims=True)
        diagonal = jnp.concatenate([diagonal, jnp.zeros((1, 128 - half), f32)], axis=1)
        first = core_ref[0] == 0
        nothing = jnp.zeros((1, 128), f32)
        keep_ref[:8, :] = jnp.where(first, corner, triangles)
        keep_ref[8:9, :] = jnp.where(first, nothing, diagonal)
        send_ref[:8, :] = jnp.where(first, triangles, corner)
        send_ref[8:9, :] = jnp.where(first, diagonal, nothing)

    return kernel


def make_sum(count, rows):
    def kernel(in_ref, out_ref):
        for j in range(rows):
            total = jnp.sum(in_ref[pl.ds(j, count, stride=rows), :], axis=0, keepdims=True)
            out_ref[pl.ds(j, count, stride=rows), :] = jnp.broadcast_to(total, (count, 128))

    return kernel


def make_update(half, rows, cells=None):
    def kernel(core_ref, mine_ref, other_ref, tile_ref, mean_ref, next_ref, out_ref):
        genes = tile_ref.shape[1]
        comps = 2 * half
        width = out_ref.shape[1]
        chunks = [
            by_core(
                core_ref[0] == 0,
                mine_ref[pl.ds(j, half, stride=rows), :],
                other_ref[pl.ds(j, half, stride=rows), :],
            )
            for j in range(rows - 1)
        ]
        scores = jnp.concatenate(chunks, axis=1)
        both = lax.dot_general(split_pair(scores), tile_ref[...], NN, preferred_element_type=f32)
        totals = jnp.sum(scores, axis=1, keepdims=True)
        mean = mean_ref[...] * (1.0 / cells) if cells else mean_ref[...]
        raw = both[:comps] + both[comps:] - totals * mean
        rest = out_ref.shape[0] - comps - 4
        tall = jnp.concatenate(
            [
                raw.astype(bf16),
                split_pair(next_ref[...]),
                split_pair(mean_ref[...]),
                jnp.zeros((rest, genes), bf16),
            ],
            axis=0,
        )
        high = totals.astype(bf16)
        low = (totals - high.astype(f32)).astype(bf16)
        side = jnp.concatenate([high, low, jnp.zeros((comps, width - genes - 2), bf16)], axis=1)
        side = jnp.concatenate([side, jnp.zeros((tall.shape[0] - comps, width - genes), bf16)], axis=0)
        out_ref[...] = jnp.concatenate([tall, side], axis=1)

    return kernel


def inverse_factor(gram):
    size = gram.shape[0]
    shape = (8, 2 * size)
    rows = lax.broadcasted_iota(jnp.int32, shape, 0)
    lanes = lax.broadcasted_iota(jnp.int32, shape, 1)
    blocks = []
    for b in range(size // 8):
        eye = jnp.where(lanes == rows + (b * 8 + size), 1.0, 0.0).astype(f32)
        left = jnp.concatenate([gram[b * 8 : b * 8 + 8, :], jnp.zeros((8, size), f32)], axis=1)
        blocks.append(left + eye)
    results = list(blocks)
    for k in range(0, size, 2):
        b, r = divmod(k, 8)
        upper = blocks[b][r : r + 1, :]
        lower = blocks[b][r + 1 : r + 2, :]
        columns = [
            tuple(jnp.broadcast_to(blocks[i][:, k + h : k + h + 1], shape) for h in range(2))
            for i in range(b, size // 8)
        ]
        p = columns[0][0][r : r + 1, :]
        q = columns[0][0][r + 1 : r + 2, :]
        t = columns[0][1][r + 1 : r + 2, :]
        over = 1.0 / (p * t - q * q)
        first = (t * upper - q * lower) * over
        second = (p * lower - q * upper) * over
        inverse_p = 1.0 / p
        slope = q * inverse_p
        top = upper * lax.rsqrt(p)
        low = (lower - slope * upper) * lax.rsqrt(t - slope * q)
        results[b] = jnp.where(rows == r, top, jnp.where(rows == r + 1, low, results[b]))
        for i in range(b, size // 8):
            x, y = columns[i - b]
            change = x * first + y * second
            if i == b:
                change = jnp.where(rows > r + 1, change, 0.0)
            blocks[i] = blocks[i] - change
    return jnp.concatenate(results, axis=0)[:, size:]


def make_factor(half, rows):
    def kernel(core_ref, mine_ref, other_ref, out_ref):
        gram = by_core(
            core_ref[0] == 0,
            mine_ref[pl.ds(rows - 1, half, stride=rows), :],
            other_ref[pl.ds(rows - 1, half, stride=rows), :],
        )
        out_ref[...] = inverse_factor(gram[:, : 2 * half])

    return kernel


def copies_kernel(a, b, out_ref):
    rows = a.shape[0]
    count = out_ref.shape[0] // rows
    total = a[...] + b[...]
    for j in range(rows):
        out_ref[pl.ds(j, count, stride=rows), :] = jnp.broadcast_to(total[j : j + 1], (count, 128))


def total_kernel(in_ref, out_ref):
    rows = out_ref.shape[0]
    count = in_ref.shape[0] // rows
    for j in range(rows):
        out_ref[j : j + 1, :] = jnp.sum(in_ref[pl.ds(j, count, stride=rows), :], axis=0, keepdims=True)


def make_finish(scale):
    def kernel(core_ref, mine_ref, other_ref, stepped_ref, out_ref):
        first = core_ref[0] == 0
        corner = gather_up(jnp.where(first, mine_ref[:8, :], other_ref[:8, :]))
        triangles = gather_up(jnp.where(first, other_ref[:8, :], mine_ref[:8, :]))
        half = corner.shape[0]
        diagonal = jnp.where(first, other_ref[8:9, :half], mine_ref[8:9, :half])
        rows = lax.broadcasted_iota(jnp.int32, (half, half), 0)
        columns = lax.broadcasted_iota(jnp.int32, (half, half), 1)
        eye = jnp.where(rows == columns, 1.0, 0.0).astype(f32)

        def turned(block):
            return lax.dot_general(block, eye, (((0,), (0,)), ((), ())), precision=HIGH, preferred_element_type=f32)

        across = turned(triangles)
        upper = jnp.where(rows >= columns, triangles, across)
        lower = jnp.where(rows < columns, triangles, across)
        lower = jnp.where(rows == columns, jnp.broadcast_to(diagonal, (half, half)), lower)
        gram = jnp.concatenate(
            [
                jnp.concatenate([upper, turned(corner)], axis=1),
                jnp.concatenate([corner, lower], axis=1),
            ],
            axis=0,
        )
        out_ref[...] = scale * lax.dot_general(
            inverse_factor(gram), stepped_ref[...], NN, precision=HIGH, preferred_element_type=f32
        )

    return kernel


def shards(pool_counts, cell_picks, loadings_init):
    comps, genes = loadings_init.shape
    steps, cells = cell_picks.shape
    half = comps // 2
    local_pool = pool_counts.shape[1]
    cell_devices = lax.axis_size("cell")
    gene_devices = lax.axis_size("gene")
    chips = gene_devices // 2
    batch = cells * cell_devices
    rows = cells // 128 + 1
    width = genes + 128 - genes % 128
    first_cell = lax.axis_index("cell").astype(jnp.int32) * local_pool
    core = (lax.axis_index("gene") % 2).astype(jnp.int32).reshape(1)
    chosen = cell_picks - first_cell
    pool_by_cell = pool_counts.T
    same_core = [[2 * chip + which for chip in range(chips)] for which in range(2)]

    def tile_of(picks):
        return jnp.take(pool_by_cell, picks, axis=0, mode="clip")

    def sums_of(tile):
        return jnp.sum(tile, axis=0, dtype=f32, keepdims=True)

    def swap_cores(value):
        return lax.ppermute(value, "gene", [(i, i ^ 1) for i in range(gene_devices)])

    def round_cells(value):
        return [value] + [
            lax.ppermute(value, "cell", [(i, (i + k) % cell_devices) for i in range(cell_devices)])
            for k in (1, 3, 2)
        ]

    def exchange(value):
        pieces = value.reshape(chips, 1, value.size // chips)
        arrived = lax.all_to_all(pieces, "gene", 0, 0, tiled=True, axis_index_groups=same_core)
        return arrived.reshape(value.shape)

    packed = jax.ShapeDtypeStruct((half * rows, 128), f32)
    square = jax.ShapeDtypeStruct((comps, comps), f32)
    local = jax.ShapeDtypeStruct((comps, genes), f32)
    row = jax.ShapeDtypeStruct((1, genes), f32)
    shared = jax.ShapeDtypeStruct((comps + 8, width), bf16)

    chunk = local_pool // 8
    keep, send = vmem_call(
        first_kernel,
        (packed, packed),
        0,
        name="first",
        core=2,
        pool=3,
        scratch=[
            pltpu.VMEM((comps, genes), f32),
            pltpu.VMEM((steps, cells), jnp.int32),
            pltpu.VMEM((8, genes, chunk), bf16),
            pltpu.SemaphoreType.DMA((10,)),
        ],
    )(core, first_cell.reshape(1), loadings_init, cell_picks, pool_counts)

    def scores_of(keep, send, later):
        chip_sum = vmem_call(add_kernel, packed, 2, name="pair", core=False)(keep, swap_cores(send))
        came, later = lax.optimization_barrier((exchange(chip_sum), later))
        copies = vmem_call(make_sum(chips, rows), packed, 1, name="add_up", core=False)(came)
        mine = exchange(copies)
        return mine, swap_cores(mine), later

    def change_of(mine, other, tile, mean, next_sums, own=None):
        change = vmem_call(make_update(half, rows, own), shared, 5, name="update")(
            core, mine, other, tile, mean, next_sums
        )
        return round_cells(change)

    def factor_of(mine, other):
        return vmem_call(make_factor(half, rows), square, 2, flops=10**9, name="factor")(core, mine, other)

    def advance(parts, stepped, inverse, next_tile):
        inputs = [*parts, stepped, *inverse, next_tile]
        return vmem_call(
            make_middle(batch, bool(inverse)), (packed, packed, local, row), len(inputs), name="middle"
        )(core, *inputs)

    def one_step(state):
        step, keep, send, stepped, mean, tile = state
        following = step + 1
        picks = lax.dynamic_index_in_dim(chosen, following, keepdims=False)
        following, picks, send = lax.optimization_barrier((following, picks, send))
        mine, other, picks = scores_of(keep, send, picks)
        next_tile = tile_of(picks)
        parts = change_of(mine, other, tile, mean, sums_of(next_tile))
        inverse = (factor_of(mine, other),)
        return (following, *advance(parts, stepped, inverse, next_tile), next_tile)

    mine, other, picks = scores_of(keep, send, chosen[:2])
    tile, next_tile = jnp.split(tile_of(picks.reshape(-1)), 2)
    parts = change_of(mine, other, tile, sums_of(tile), sums_of(next_tile), cells)
    state = (*advance(parts, loadings_init, (), next_tile), next_tile)
    _, keep, send, stepped, mean, tile = lax.while_loop(
        lambda state: state[0] < steps - 1, one_step, (jnp.int32(1), *state)
    )
    mine, other, _ = scores_of(keep, send, ())
    parts = change_of(mine, other, tile, mean, mean)
    inverse = factor_of(mine, other)
    few = jax.ShapeDtypeStruct((9, 128), f32)
    many = jax.ShapeDtypeStruct((9 * chips, 128), f32)
    keep, send, stepped = vmem_call(make_last(batch), (few, few, local), len(parts) + 2, name="last")(
        core, *parts, stepped, inverse
    )
    copies = vmem_call(copies_kernel, many, 2, name="copies", core=False)(keep, swap_cores(send))
    mine = vmem_call(total_kernel, few, 1, name="total", core=False)(exchange(copies))
    scale = math.sqrt(genes * gene_devices)
    return vmem_call(make_finish(scale), local, 3, name="finish", held=False)(
        core, mine, swap_cores(mine), stepped
    )


def solution(mesh):
    placed = (P("gene", "cell"), P(None, "cell"), P(None, "gene"))
    return jax.shard_map(
        shards, mesh=mesh, in_specs=placed, out_specs=P(None, "gene"), check_vma=False
    )
```

```python
import math

import jax
import jax.numpy as jnp
from jax import lax
from jax.experimental import pallas as pl
from jax.experimental.pallas import tpu as pltpu
from jax.sharding import PartitionSpec as P

f32 = jnp.float32
bf16 = jnp.bfloat16
STEP_RATE = 1.0
HIGH = lax.Precision.HIGHEST
NT = (((1,), (1,)), ((), ()))
NN = (((1,), (0,)), ((), ()))


def vmem_call(kernel, outs, count, flops=0, name=None, core=True, pool=0, scratch=(), held=True):
    spec = pl.BlockSpec(memory_space=pltpu.VMEM)
    call = pl.pallas_call(
        kernel,
        out_shape=jax.tree.map(lambda s: pltpu.VMEM(s.shape, s.dtype), outs) if held else outs,
        in_specs=[pl.BlockSpec(memory_space=pltpu.SMEM)] * core
        + [spec] * count
        + [pl.BlockSpec(memory_space=pl.ANY)] * pool,
        out_specs=jax.tree.map(lambda _: spec, outs),
        cost_estimate=pl.CostEstimate(flops=flops, transcendentals=0, bytes_accessed=0),
        scratch_shapes=scratch,
        name=name,
    )

    def run(*args):
        last = core + count
        near = [pltpu.with_memory_space_constraint(a, pltpu.VMEM) for a in args[core:last]]
        return call(*args[:core], *near, *args[last:])

    return run


def split_pair(value):
    high = value.astype(bf16)
    low = (value - high.astype(f32)).astype(bf16)
    return jnp.concatenate([high, low], axis=0)


def gram_of(stepped):
    return lax.dot_general(stepped, stepped, NT, precision=HIGH, preferred_element_type=f32)


def by_core(first, mine, other):
    return jnp.concatenate([jnp.where(first, mine, other), jnp.where(first, other, mine)], axis=0)


def spread(scores, gram, first, keep_ref, send_ref):
    comps = scores.shape[0]
    half = comps // 2
    gram = jnp.concatenate([gram, jnp.zeros((comps, 128 - comps), f32)], axis=1)
    rows = scores.shape[1] // 128 + 1
    for j in range(rows):
        chunk = scores[:, j * 128 : (j + 1) * 128] if j + 1 < rows else gram
        top, bottom = chunk[:half], chunk[half:]
        keep_ref[pl.ds(j, half, stride=rows), :] = jnp.where(first, top, bottom)
        send_ref[pl.ds(j, half, stride=rows), :] = jnp.where(first, bottom, top)


def pack_partial(stepped, tile, shift, first, keep_ref, send_ref):
    comps = stepped.shape[0]
    both = lax.dot_general(split_pair(stepped), tile, NT, preferred_element_type=f32)
    spread(both[:comps] + both[comps:] - shift, gram_of(stepped), first, keep_ref, send_ref)


def first_kernel(core_ref, cell_ref, loadings_ref, picks_ref, pool_ref, keep_ref, send_ref, start_ref, names_ref, buffer_ref, sems):
    chunks, _, size = buffer_ref.shape
    near = [
        pltpu.make_async_copy(loadings_ref, start_ref, sems.at[chunks]),
        pltpu.make_async_copy(picks_ref, names_ref, sems.at[chunks + 1]),
    ]
    copies = [
        pltpu.make_async_copy(pool_ref.at[:, pl.ds(i * size, size)], buffer_ref.at[i], sems.at[i])
        for i in range(chunks)
    ]
    for copy in near + copies:
        copy.start()
    for copy in near:
        copy.wait()
    loadings = start_ref[...]
    comps = loadings.shape[0]
    pair = split_pair(loadings)
    picks = names_ref[0:1, :] - cell_ref[0]
    places = lax.broadcasted_iota(jnp.int32, (size, picks.shape[1]), 0)
    chosen = jnp.zeros((2 * comps, picks.shape[1]), f32)
    for i, copy in enumerate(copies):
        copy.wait()
        both = lax.dot_general(pair, buffer_ref[i], NN, preferred_element_type=f32)
        every = split_pair(both[:comps] + both[comps:])
        one_hot = jnp.where(places == picks - i * size, 1.0, 0.0).astype(bf16)
        chosen = chosen + lax.dot_general(every, one_hot, NN, preferred_element_type=f32)
    spread(chosen[:comps] + chosen[comps:], gram_of(loadings), core_ref[0] == 0, keep_ref, send_ref)


def add_kernel(a, b, out_ref):
    out_ref[...] = a[...] + b[...]


def stepped_from(parts, previous, inverse, batch, left=0.0):
    comps, genes = previous.shape
    total = sum(part[:comps, :genes] for part in parts) + left
    stepped = previous + STEP_RATE * (total * (1.0 / batch))
    if inverse is not None:
        stepped = lax.dot_general(inverse, stepped, NN, precision=HIGH, preferred_element_type=f32)
    return stepped


def row_of(part, start, genes):
    return part[start : start + 1, :genes]


def between_groups(parts, comps, genes, batch):
    sums = [row_of(part, comps + 1, genes) for part in parts]
    mean = sum(sums) * (1.0 / batch)
    total = jnp.zeros((comps, genes), f32)
    for part, own in zip(parts, sums):
        total = total + part[:comps, genes : genes + 1] * (own * (len(parts) / batch) - mean)
    return total


def make_middle(batch, normalised):
    def kernel(core_ref, a, b, c, d, previous_ref, *refs):
        inverse = refs[0][...] if normalised else None
        tile_ref, keep_ref, send_ref, stepped_ref, mean_ref = refs[-5:]
        comps, genes = previous_ref.shape
        parts = (a, b, c, d)
        left = 0.0 if normalised else between_groups(parts, comps, genes, batch)
        stepped = stepped_from(parts, previous_ref[...], inverse, batch, left)
        stepped_ref[...] = stepped
        mean = sum(row_of(part, comps, genes) for part in parts) * (1.0 / batch)
        mean_ref[...] = mean
        shift = jnp.sum(stepped * mean, axis=1, keepdims=True)
        pack_partial(stepped, tile_ref[...], shift, core_ref[0] == 0, keep_ref, send_ref)

    return kernel


def lay_out(block):
    return jnp.concatenate([block[h : h + 8] for h in range(0, 32, 8)], axis=1)


def gather_up(rows):
    return jnp.concatenate([rows[:, w : w + 32] for w in range(0, 128, 32)], axis=0)


def make_last(batch):
    def kernel(core_ref, a, b, c, d, previous_ref, inverse_ref, keep_ref, send_ref, stepped_ref):
        stepped = stepped_from((a, b, c, d), previous_ref[...], inverse_ref[...], batch)
        stepped_ref[...] = stepped
        gram = gram_of(stepped)
        half = gram.shape[0] // 2
        rows = lax.broadcasted_iota(jnp.int32, (half, half), 0)
        columns = lax.broadcasted_iota(jnp.int32, (half, half), 1)
        upper, lower = gram[:half, :half], gram[half:, half:]
        corner = lay_out(gram[half:, :half])
        triangles = lay_out(jnp.where(rows >= columns, upper, lower))
        diagonal = jnp.sum(jnp.where(rows == columns, lower, 0.0), axis=0, keepdims=True)
        diagonal = jnp.concatenate([diagonal, jnp.zeros((1, 128 - half), f32)], axis=1)
        first = core_ref[0] == 0
        nothing = jnp.zeros((1, 128), f32)
        keep_ref[:8, :] = jnp.where(first, corner, triangles)
        keep_ref[8:9, :] = jnp.where(first, nothing, diagonal)
        send_ref[:8, :] = jnp.where(first, triangles, corner)
        send_ref[8:9, :] = jnp.where(first, diagonal, nothing)

    return kernel


def make_sum(count, rows):
    def kernel(in_ref, out_ref):
        for j in range(rows):
            total = jnp.sum(in_ref[pl.ds(j, count, stride=rows), :], axis=0, keepdims=True)
            out_ref[pl.ds(j, count, stride=rows), :] = jnp.broadcast_to(total, (count, 128))

    return kernel


def make_update(half, rows, cells=None):
    def kernel(core_ref, mine_ref, other_ref, tile_ref, mean_ref, next_ref, out_ref):
        genes = tile_ref.shape[1]
        comps = 2 * half
        width = out_ref.shape[1]
        chunks = [
            by_core(
                core_ref[0] == 0,
                mine_ref[pl.ds(j, half, stride=rows), :],
                other_ref[pl.ds(j, half, stride=rows), :],
            )
            for j in range(rows - 1)
        ]
        scores = jnp.concatenate(chunks, axis=1)
        both = lax.dot_general(split_pair(scores), tile_ref[...], NN, preferred_element_type=f32)
        totals = jnp.sum(scores, axis=1, keepdims=True)
        mean = mean_ref[...] * (1.0 / cells) if cells else mean_ref[...]
        raw = both[:comps] + both[comps:] - totals * mean
        rest = out_ref.shape[0] - comps - 2
        out_ref[:comps, :] = jnp.concatenate(
            [raw, jnp.broadcast_to(totals, (comps, width - genes))], axis=1
        )
        side = jnp.zeros((1, width - genes), f32)
        out_ref[comps : comps + 1, :] = jnp.concatenate([next_ref[...], side], axis=1)
        out_ref[comps + 1 : comps + 2, :] = jnp.concatenate([mean_ref[...], side], axis=1)
        out_ref[comps + 2 :, :] = jnp.zeros((rest, width), f32)

    return kernel


def inverse_factor(gram):
    size = gram.shape[0]
    shape = (8, 2 * size)
    rows = lax.broadcasted_iota(jnp.int32, shape, 0)
    lanes = lax.broadcasted_iota(jnp.int32, shape, 1)
    blocks = []
    for b in range(size // 8):
        eye = jnp.where(lanes == rows + (b * 8 + size), 1.0, 0.0).astype(f32)
        left = jnp.concatenate([gram[b * 8 : b * 8 + 8, :], jnp.zeros((8, size), f32)], axis=1)
        blocks.append(left + eye)
    results = list(blocks)
    for k in range(0, size, 2):
        b, r = divmod(k, 8)
        upper = blocks[b][r : r + 1, :]
        lower = blocks[b][r + 1 : r + 2, :]
        columns = [
            tuple(jnp.broadcast_to(blocks[i][:, k + h : k + h + 1], shape) for h in range(2))
            for i in range(b, size // 8)
        ]
        p = columns[0][0][r : r + 1, :]
        q = columns[0][0][r + 1 : r + 2, :]
        t = columns[0][1][r + 1 : r + 2, :]
        over = 1.0 / (p * t - q * q)
        first = (t * upper - q * lower) * over
        second = (p * lower - q * upper) * over
        inverse_p = 1.0 / p
        slope = q * inverse_p
        top = upper * lax.rsqrt(p)
        low = (lower - slope * upper) * lax.rsqrt(t - slope * q)
        results[b] = jnp.where(rows == r, top, jnp.where(rows == r + 1, low, results[b]))
        for i in range(b, size // 8):
            x, y = columns[i - b]
            change = x * first + y * second
            if i == b:
                change = jnp.where(rows > r + 1, change, 0.0)
            blocks[i] = blocks[i] - change
    return jnp.concatenate(results, axis=0)[:, size:]


def make_factor(half, rows):
    def kernel(core_ref, mine_ref, other_ref, out_ref):
        gram = by_core(
            core_ref[0] == 0,
            mine_ref[pl.ds(rows - 1, half, stride=rows), :],
            other_ref[pl.ds(rows - 1, half, stride=rows), :],
        )
        out_ref[...] = inverse_factor(gram[:, : 2 * half])

    return kernel


def copies_kernel(a, b, out_ref):
    rows = a.shape[0]
    count = out_ref.shape[0] // rows
    total = a[...] + b[...]
    for j in range(rows):
        out_ref[pl.ds(j, count, stride=rows), :] = jnp.broadcast_to(total[j : j + 1], (count, 128))


def total_kernel(in_ref, out_ref):
    rows = out_ref.shape[0]
    count = in_ref.shape[0] // rows
    for j in range(rows):
        out_ref[j : j + 1, :] = jnp.sum(in_ref[pl.ds(j, count, stride=rows), :], axis=0, keepdims=True)


def make_finish(scale):
    def kernel(core_ref, mine_ref, other_ref, stepped_ref, out_ref):
        first = core_ref[0] == 0
        corner = gather_up(jnp.where(first, mine_ref[:8, :], other_ref[:8, :]))
        triangles = gather_up(jnp.where(first, other_ref[:8, :], mine_ref[:8, :]))
        half = corner.shape[0]
        diagonal = jnp.where(first, other_ref[8:9, :half], mine_ref[8:9, :half])
        rows = lax.broadcasted_iota(jnp.int32, (half, half), 0)
        columns = lax.broadcasted_iota(jnp.int32, (half, half), 1)
        eye = jnp.where(rows == columns, 1.0, 0.0).astype(f32)

        def turned(block):
            return lax.dot_general(block, eye, (((0,), (0,)), ((), ())), precision=HIGH, preferred_element_type=f32)

        across = turned(triangles)
        upper = jnp.where(rows >= columns, triangles, across)
        lower = jnp.where(rows < columns, triangles, across)
        lower = jnp.where(rows == columns, jnp.broadcast_to(diagonal, (half, half)), lower)
        gram = jnp.concatenate(
            [
                jnp.concatenate([upper, turned(corner)], axis=1),
                jnp.concatenate([corner, lower], axis=1),
            ],
            axis=0,
        )
        out_ref[...] = scale * lax.dot_general(
            inverse_factor(gram), stepped_ref[...], NN, precision=HIGH, preferred_element_type=f32
        )

    return kernel


def shards(pool_counts, cell_picks, loadings_init):
    comps, genes = loadings_init.shape
    steps, cells = cell_picks.shape
    half = comps // 2
    local_pool = pool_counts.shape[1]
    cell_devices = lax.axis_size("cell")
    gene_devices = lax.axis_size("gene")
    chips = gene_devices // 2
    batch = cells * cell_devices
    rows = cells // 128 + 1
    width = genes + 128 - genes % 128
    first_cell = lax.axis_index("cell").astype(jnp.int32) * local_pool
    core = (lax.axis_index("gene") % 2).astype(jnp.int32).reshape(1)
    chosen = cell_picks - first_cell
    pool_by_cell = pool_counts.T
    same_core = [[2 * chip + which for chip in range(chips)] for which in range(2)]

    def tile_of(picks):
        return jnp.take(pool_by_cell, picks, axis=0, mode="clip")

    def sums_of(tile):
        return jnp.sum(tile, axis=0, dtype=f32, keepdims=True)

    def swap_cores(value):
        return lax.ppermute(value, "gene", [(i, i ^ 1) for i in range(gene_devices)])

    def round_cells(value):
        return [value] + [
            lax.ppermute(value, "cell", [(i, (i + k) % cell_devices) for i in range(cell_devices)])
            for k in range(1, cell_devices)
        ]

    def exchange(value):
        pieces = value.reshape(chips, 1, value.size // chips)
        arrived = lax.all_to_all(pieces, "gene", 0, 0, tiled=True, axis_index_groups=same_core)
        return arrived.reshape(value.shape)

    packed = jax.ShapeDtypeStruct((half * rows, 128), f32)
    square = jax.ShapeDtypeStruct((comps, comps), f32)
    local = jax.ShapeDtypeStruct((comps, genes), f32)
    row = jax.ShapeDtypeStruct((1, genes), f32)
    shared = jax.ShapeDtypeStruct((comps + 8, width), f32)

    chunk = local_pool // 8
    keep, send = vmem_call(
        first_kernel,
        (packed, packed),
        0,
        name="first",
        core=2,
        pool=3,
        scratch=[
            pltpu.VMEM((comps, genes), f32),
            pltpu.VMEM((steps, cells), jnp.int32),
            pltpu.VMEM((8, genes, chunk), bf16),
            pltpu.SemaphoreType.DMA((10,)),
        ],
    )(core, first_cell.reshape(1), loadings_init, cell_picks, pool_counts)

    def scores_of(keep, send, later):
        chip_sum = vmem_call(add_kernel, packed, 2, name="pair", core=False)(keep, swap_cores(send))
        came, later = lax.optimization_barrier((exchange(chip_sum), later))
        copies = vmem_call(make_sum(chips, rows), packed, 1, name="add_up", core=False)(came)
        mine = exchange(copies)
        return mine, swap_cores(mine), later

    def change_of(mine, other, tile, mean, next_sums, own=None):
        change = vmem_call(make_update(half, rows, own), shared, 5, name="update")(
            core, mine, other, tile, mean, next_sums
        )
        return round_cells(change)

    def factor_of(mine, other):
        return vmem_call(make_factor(half, rows), square, 2, flops=10**9, name="factor")(core, mine, other)

    def advance(parts, stepped, inverse, next_tile):
        inputs = [*parts, stepped, *inverse, next_tile]
        return vmem_call(
            make_middle(batch, bool(inverse)), (packed, packed, local, row), len(inputs), name="middle"
        )(core, *inputs)

    def one_step(state):
        step, keep, send, stepped, mean, tile = state
        following = step + 1
        picks = lax.dynamic_index_in_dim(chosen, following, keepdims=False)
        following, picks, send = lax.optimization_barrier((following, picks, send))
        mine, other, picks = scores_of(keep, send, picks)
        next_tile = tile_of(picks)
        parts = change_of(mine, other, tile, mean, sums_of(next_tile))
        inverse = (factor_of(mine, other),)
        return (following, *advance(parts, stepped, inverse, next_tile), next_tile)

    mine, other, picks = scores_of(keep, send, chosen[:2])
    tile, next_tile = jnp.split(tile_of(picks.reshape(-1)), 2)
    parts = change_of(mine, other, tile, sums_of(tile), sums_of(next_tile), cells)
    state = (*advance(parts, loadings_init, (), next_tile), next_tile)
    _, keep, send, stepped, mean, tile = lax.while_loop(
        lambda state: state[0] < steps - 1, one_step, (jnp.int32(1), *state)
    )
    mine, other, _ = scores_of(keep, send, ())
    parts = change_of(mine, other, tile, mean, mean)
    inverse = factor_of(mine, other)
    few = jax.ShapeDtypeStruct((9, 128), f32)
    many = jax.ShapeDtypeStruct((9 * chips, 128), f32)
    keep, send, stepped = vmem_call(make_last(batch), (few, few, local), len(parts) + 2, name="last")(
        core, *parts, stepped, inverse
    )
    copies = vmem_call(copies_kernel, many, 2, name="copies", core=False)(keep, swap_cores(send))
    mine = vmem_call(total_kernel, few, 1, name="total", core=False)(exchange(copies))
    scale = math.sqrt(genes * gene_devices)
    return vmem_call(make_finish(scale), local, 3, name="finish", held=False)(
        core, mine, swap_cores(mine), stepped
    )


def solution(mesh):
    placed = (P("gene", "cell"), P(None, "cell"), P(None, "gene"))
    return jax.shard_map(
        shards, mesh=mesh, in_specs=placed, out_specs=P(None, "gene"), check_vma=False
    )
```

```python
import math

import jax
import jax.numpy as jnp
from jax import lax
from jax.experimental import pallas as pl
from jax.experimental.pallas import tpu as pltpu
from jax.sharding import PartitionSpec as P

f32 = jnp.float32
bf16 = jnp.bfloat16
STEP_RATE = 1.0
HIGH = lax.Precision.HIGHEST
NT = (((1,), (1,)), ((), ()))
NN = (((1,), (0,)), ((), ()))


def vmem_call(kernel, outs, count, flops=0, name=None, core=True, pool=0, scratch=(), held=True):
    spec = pl.BlockSpec(memory_space=pltpu.VMEM)
    call = pl.pallas_call(
        kernel,
        out_shape=jax.tree.map(lambda s: pltpu.VMEM(s.shape, s.dtype), outs) if held else outs,
        in_specs=[pl.BlockSpec(memory_space=pltpu.SMEM)] * core
        + [spec] * count
        + [pl.BlockSpec(memory_space=pl.ANY)] * pool,
        out_specs=jax.tree.map(lambda _: spec, outs),
        cost_estimate=pl.CostEstimate(flops=flops, transcendentals=0, bytes_accessed=0),
        scratch_shapes=scratch,
        name=name,
    )

    def run(*args):
        last = core + count
        near = [pltpu.with_memory_space_constraint(a, pltpu.VMEM) for a in args[core:last]]
        return call(*args[:core], *near, *args[last:])

    return run


def split_pair(value):
    high = value.astype(bf16)
    low = (value - high.astype(f32)).astype(bf16)
    return jnp.concatenate([high, low], axis=0)


def gram_of(stepped):
    return lax.dot_general(stepped, stepped, NT, precision=HIGH, preferred_element_type=f32)


def by_core(first, mine, other):
    return jnp.concatenate([jnp.where(first, mine, other), jnp.where(first, other, mine)], axis=0)


def spread(scores, gram, first, keep_ref, send_ref):
    comps = scores.shape[0]
    half = comps // 2
    gram = jnp.concatenate([gram, jnp.zeros((comps, 128 - comps), f32)], axis=1)
    rows = scores.shape[1] // 128 + 1
    for j in range(rows):
        chunk = scores[:, j * 128 : (j + 1) * 128] if j + 1 < rows else gram
        top, bottom = chunk[:half], chunk[half:]
        keep_ref[pl.ds(j, half, stride=rows), :] = jnp.where(first, top, bottom)
        send_ref[pl.ds(j, half, stride=rows), :] = jnp.where(first, bottom, top)


def pack_partial(stepped, tile, shift, first, keep_ref, send_ref):
    comps = stepped.shape[0]
    both = lax.dot_general(split_pair(stepped), tile, NT, preferred_element_type=f32)
    spread(both[:comps] + both[comps:] - shift, gram_of(stepped), first, keep_ref, send_ref)


def first_kernel(core_ref, cell_ref, loadings_ref, picks_ref, pool_ref, keep_ref, send_ref, start_ref, names_ref, buffer_ref, sems):
    chunks, _, size = buffer_ref.shape
    near = [
        pltpu.make_async_copy(loadings_ref, start_ref, sems.at[chunks]),
        pltpu.make_async_copy(picks_ref, names_ref, sems.at[chunks + 1]),
    ]
    copies = [
        pltpu.make_async_copy(pool_ref.at[:, pl.ds(i * size, size)], buffer_ref.at[i], sems.at[i])
        for i in range(chunks)
    ]
    for copy in near + copies:
        copy.start()
    for copy in near:
        copy.wait()
    loadings = start_ref[...]
    comps = loadings.shape[0]
    pair = split_pair(loadings)
    picks = names_ref[0:1, :] - cell_ref[0]
    places = lax.broadcasted_iota(jnp.int32, (size, picks.shape[1]), 0)
    chosen = jnp.zeros((2 * comps, picks.shape[1]), f32)
    for i, copy in enumerate(copies):
        copy.wait()
        both = lax.dot_general(pair, buffer_ref[i], NN, preferred_element_type=f32)
        every = split_pair(both[:comps] + both[comps:])
        one_hot = jnp.where(places == picks - i * size, 1.0, 0.0).astype(bf16)
        chosen = chosen + lax.dot_general(every, one_hot, NN, preferred_element_type=f32)
    spread(chosen[:comps] + chosen[comps:], gram_of(loadings), core_ref[0] == 0, keep_ref, send_ref)


def add_kernel(a, b, out_ref):
    out_ref[...] = a[...] + b[...]


def stepped_from(parts, previous, inverse, batch, left=0.0):
    comps, genes = previous.shape
    total = sum(part[:comps, :genes] for part in parts) + left
    stepped = previous + STEP_RATE * (total * (1.0 / batch))
    if inverse is not None:
        stepped = lax.dot_general(inverse, stepped, NN, precision=HIGH, preferred_element_type=f32)
    return stepped


def row_of(part, start, genes):
    return part[start : start + 1, :genes]


def spare_row(part, genes):
    spare = part.shape[1] - genes
    return jnp.concatenate([part[i : i + 1, genes:] for i in range(genes // spare)], axis=1)


def between_groups(parts, comps, genes, batch):
    sums = [row_of(part, comps + 1, genes) for part in parts]
    mean = sum(sums) * (1.0 / batch)
    total = jnp.zeros((comps, genes), f32)
    for part, own in zip(parts, sums):
        total = total + part[:comps, genes : genes + 1] * (own * (len(parts) / batch) - mean)
    return total


def make_middle(batch, normalised):
    def kernel(core_ref, a, b, c, d, previous_ref, *refs):
        inverse = refs[0][...] if normalised else None
        tile_ref, keep_ref, send_ref, stepped_ref, mean_ref = refs[-5:]
        comps, genes = previous_ref.shape
        parts = (a, b, c, d)
        left = 0.0 if normalised else between_groups(parts, comps, genes, batch)
        stepped = stepped_from(parts, previous_ref[...], inverse, batch, left)
        stepped_ref[...] = stepped
        mean = sum(
            spare_row(part, genes) if normalised else row_of(part, comps, genes) for part in parts
        ) * (1.0 / batch)
        mean_ref[...] = mean
        shift = jnp.sum(stepped * mean, axis=1, keepdims=True)
        pack_partial(stepped, tile_ref[...], shift, core_ref[0] == 0, keep_ref, send_ref)

    return kernel


def lay_out(block):
    return jnp.concatenate([block[h : h + 8] for h in range(0, 32, 8)], axis=1)


def gather_up(rows):
    return jnp.concatenate([rows[:, w : w + 32] for w in range(0, 128, 32)], axis=0)


def make_last(batch):
    def kernel(core_ref, a, b, c, d, previous_ref, inverse_ref, keep_ref, send_ref, stepped_ref):
        stepped = stepped_from((a, b, c, d), previous_ref[...], inverse_ref[...], batch)
        stepped_ref[...] = stepped
        gram = gram_of(stepped)
        half = gram.shape[0] // 2
        rows = lax.broadcasted_iota(jnp.int32, (half, half), 0)
        columns = lax.broadcasted_iota(jnp.int32, (half, half), 1)
        upper, lower = gram[:half, :half], gram[half:, half:]
        corner = lay_out(gram[half:, :half])
        triangles = lay_out(jnp.where(rows >= columns, upper, lower))
        diagonal = jnp.sum(jnp.where(rows == columns, lower, 0.0), axis=0, keepdims=True)
        diagonal = jnp.concatenate([diagonal, jnp.zeros((1, 128 - half), f32)], axis=1)
        first = core_ref[0] == 0
        nothing = jnp.zeros((1, 128), f32)
        keep_ref[:8, :] = jnp.where(first, corner, triangles)
        keep_ref[8:9, :] = jnp.where(first, nothing, diagonal)
        send_ref[:8, :] = jnp.where(first, triangles, corner)
        send_ref[8:9, :] = jnp.where(first, diagonal, nothing)

    return kernel


def make_sum(count, rows):
    def kernel(in_ref, out_ref):
        for j in range(rows):
            total = jnp.sum(in_ref[pl.ds(j, count, stride=rows), :], axis=0, keepdims=True)
            out_ref[pl.ds(j, count, stride=rows), :] = jnp.broadcast_to(total, (count, 128))

    return kernel


def make_update(half, rows, cells=None):
    def kernel(core_ref, mine_ref, other_ref, tile_ref, mean_ref, next_ref, out_ref):
        genes = tile_ref.shape[1]
        comps = 2 * half
        width = out_ref.shape[1]
        chunks = [
            by_core(
                core_ref[0] == 0,
                mine_ref[pl.ds(j, half, stride=rows), :],
                other_ref[pl.ds(j, half, stride=rows), :],
            )
            for j in range(rows - 1)
        ]
        scores = jnp.concatenate(chunks, axis=1)
        both = lax.dot_general(split_pair(scores), tile_ref[...], NN, preferred_element_type=f32)
        totals = jnp.sum(scores, axis=1, keepdims=True)
        mean = mean_ref[...] * (1.0 / cells) if cells else mean_ref[...]
        raw = both[:comps] + both[comps:] - totals * mean
        spare = width - genes
        if cells:
            side = jnp.zeros((1, spare), f32)
            rest = out_ref.shape[0] - comps - 2
            out_ref[:comps, :] = jnp.concatenate([raw, jnp.broadcast_to(totals, (comps, spare))], axis=1)
            out_ref[comps : comps + 1, :] = jnp.concatenate([next_ref[...], side], axis=1)
            out_ref[comps + 1 : comps + 2, :] = jnp.concatenate([mean_ref[...], side], axis=1)
            out_ref[comps + 2 :, :] = jnp.zeros((rest, width), f32)
        else:
            sums = next_ref[...]
            pieces = [sums[:, i : i + spare] for i in range(0, genes, spare)]
            pieces.append(jnp.zeros((comps - len(pieces), spare), f32))
            out_ref[...] = jnp.concatenate([raw, jnp.concatenate(pieces, axis=0)], axis=1)

    return kernel


def inverse_factor(gram):
    size = gram.shape[0]
    shape = (8, 2 * size)
    rows = lax.broadcasted_iota(jnp.int32, shape, 0)
    lanes = lax.broadcasted_iota(jnp.int32, shape, 1)
    blocks = []
    for b in range(size // 8):
        eye = jnp.where(lanes == rows + (b * 8 + size), 1.0, 0.0).astype(f32)
        left = jnp.concatenate([gram[b * 8 : b * 8 + 8, :], jnp.zeros((8, size), f32)], axis=1)
        blocks.append(left + eye)
    results = list(blocks)
    for k in range(0, size, 2):
        b, r = divmod(k, 8)
        upper = blocks[b][r : r + 1, :]
        lower = blocks[b][r + 1 : r + 2, :]
        columns = [
            tuple(jnp.broadcast_to(blocks[i][:, k + h : k + h + 1], shape) for h in range(2))
            for i in range(b, size // 8)
        ]
        p = columns[0][0][r : r + 1, :]
        q = columns[0][0][r + 1 : r + 2, :]
        t = columns[0][1][r + 1 : r + 2, :]
        over = 1.0 / (p * t - q * q)
        first = (t * upper - q * lower) * over
        second = (p * lower - q * upper) * over
        inverse_p = 1.0 / p
        slope = q * inverse_p
        top = upper * lax.rsqrt(p)
        low = (lower - slope * upper) * lax.rsqrt(t - slope * q)
        results[b] = jnp.where(rows == r, top, jnp.where(rows == r + 1, low, results[b]))
        for i in range(b, size // 8):
            x, y = columns[i - b]
            change = x * first + y * second
            if i == b:
                change = jnp.where(rows > r + 1, change, 0.0)
            blocks[i] = blocks[i] - change
    return jnp.concatenate(results, axis=0)[:, size:]


def make_factor(half, rows):
    def kernel(core_ref, mine_ref, other_ref, out_ref):
        gram = by_core(
            core_ref[0] == 0,
            mine_ref[pl.ds(rows - 1, half, stride=rows), :],
            other_ref[pl.ds(rows - 1, half, stride=rows), :],
        )
        out_ref[...] = inverse_factor(gram[:, : 2 * half])

    return kernel


def copies_kernel(a, b, out_ref):
    rows = a.shape[0]
    count = out_ref.shape[0] // rows
    total = a[...] + b[...]
    for j in range(rows):
        out_ref[pl.ds(j, count, stride=rows), :] = jnp.broadcast_to(total[j : j + 1], (count, 128))


def total_kernel(in_ref, out_ref):
    rows = out_ref.shape[0]
    count = in_ref.shape[0] // rows
    for j in range(rows):
        out_ref[j : j + 1, :] = jnp.sum(in_ref[pl.ds(j, count, stride=rows), :], axis=0, keepdims=True)


def make_finish(scale):
    def kernel(core_ref, mine_ref, other_ref, stepped_ref, out_ref):
        first = core_ref[0] == 0
        corner = gather_up(jnp.where(first, mine_ref[:8, :], other_ref[:8, :]))
        triangles = gather_up(jnp.where(first, other_ref[:8, :], mine_ref[:8, :]))
        half = corner.shape[0]
        diagonal = jnp.where(first, other_ref[8:9, :half], mine_ref[8:9, :half])
        rows = lax.broadcasted_iota(jnp.int32, (half, half), 0)
        columns = lax.broadcasted_iota(jnp.int32, (half, half), 1)
        eye = jnp.where(rows == columns, 1.0, 0.0).astype(f32)

        def turned(block):
            return lax.dot_general(block, eye, (((0,), (0,)), ((), ())), precision=HIGH, preferred_element_type=f32)

        across = turned(triangles)
        upper = jnp.where(rows >= columns, triangles, across)
        lower = jnp.where(rows < columns, triangles, across)
        lower = jnp.where(rows == columns, jnp.broadcast_to(diagonal, (half, half)), lower)
        gram = jnp.concatenate(
            [
                jnp.concatenate([upper, turned(corner)], axis=1),
                jnp.concatenate([corner, lower], axis=1),
            ],
            axis=0,
        )
        out_ref[...] = scale * lax.dot_general(
            inverse_factor(gram), stepped_ref[...], NN, precision=HIGH, preferred_element_type=f32
        )

    return kernel


def shards(pool_counts, cell_picks, loadings_init):
    comps, genes = loadings_init.shape
    steps, cells = cell_picks.shape
    half = comps // 2
    local_pool = pool_counts.shape[1]
    cell_devices = lax.axis_size("cell")
    gene_devices = lax.axis_size("gene")
    chips = gene_devices // 2
    batch = cells * cell_devices
    rows = cells // 128 + 1
    width = genes + 128 - genes % 128
    first_cell = lax.axis_index("cell").astype(jnp.int32) * local_pool
    core = (lax.axis_index("gene") % 2).astype(jnp.int32).reshape(1)
    chosen = cell_picks - first_cell
    pool_by_cell = pool_counts.T
    same_core = [[2 * chip + which for chip in range(chips)] for which in range(2)]

    def tile_of(picks):
        return jnp.take(pool_by_cell, picks, axis=0, mode="clip")

    def sums_of(tile):
        return jnp.sum(tile, axis=0, dtype=f32, keepdims=True)

    def swap_cores(value):
        return lax.ppermute(value, "gene", [(i, i ^ 1) for i in range(gene_devices)])

    def round_cells(value):
        return [value] + [
            lax.ppermute(value, "cell", [(i, (i + k) % cell_devices) for i in range(cell_devices)])
            for k in range(1, cell_devices)
        ]

    def exchange(value):
        pieces = value.reshape(chips, 1, value.size // chips)
        arrived = lax.all_to_all(pieces, "gene", 0, 0, tiled=True, axis_index_groups=same_core)
        return arrived.reshape(value.shape)

    packed = jax.ShapeDtypeStruct((half * rows, 128), f32)
    square = jax.ShapeDtypeStruct((comps, comps), f32)
    local = jax.ShapeDtypeStruct((comps, genes), f32)
    row = jax.ShapeDtypeStruct((1, genes), f32)

    chunk = local_pool // 8
    keep, send = vmem_call(
        first_kernel,
        (packed, packed),
        0,
        name="first",
        core=2,
        pool=3,
        scratch=[
            pltpu.VMEM((comps, genes), f32),
            pltpu.VMEM((steps, cells), jnp.int32),
            pltpu.VMEM((8, genes, chunk), bf16),
            pltpu.SemaphoreType.DMA((10,)),
        ],
    )(core, first_cell.reshape(1), loadings_init, cell_picks, pool_counts)

    def scores_of(keep, send, later):
        chip_sum = vmem_call(add_kernel, packed, 2, name="pair", core=False)(keep, swap_cores(send))
        came, later = lax.optimization_barrier((exchange(chip_sum), later))
        copies = vmem_call(make_sum(chips, rows), packed, 1, name="add_up", core=False)(came)
        mine = exchange(copies)
        return mine, swap_cores(mine), later

    def change_of(mine, other, tile, mean, next_sums, own=None):
        shared = jax.ShapeDtypeStruct((comps + 8 if own else comps, width), f32)
        change = vmem_call(make_update(half, rows, own), shared, 5, name="update")(
            core, mine, other, tile, mean, next_sums
        )
        return round_cells(change)

    def factor_of(mine, other):
        return vmem_call(make_factor(half, rows), square, 2, flops=10**9, name="factor")(core, mine, other)

    def advance(parts, stepped, inverse, next_tile):
        inputs = [*parts, stepped, *inverse, next_tile]
        return vmem_call(
            make_middle(batch, bool(inverse)), (packed, packed, local, row), len(inputs), name="middle"
        )(core, *inputs)

    def one_step(state):
        step, keep, send, stepped, mean, tile = state
        following = step + 1
        picks = lax.dynamic_index_in_dim(chosen, following, keepdims=False)
        following, picks, send = lax.optimization_barrier((following, picks, send))
        mine, other, picks = scores_of(keep, send, picks)
        next_tile = tile_of(picks)
        parts = change_of(mine, other, tile, mean, sums_of(next_tile))
        inverse = (factor_of(mine, other),)
        return (following, *advance(parts, stepped, inverse, next_tile), next_tile)

    mine, other, picks = scores_of(keep, send, chosen[:2])
    tile, next_tile = jnp.split(tile_of(picks.reshape(-1)), 2)
    parts = change_of(mine, other, tile, sums_of(tile), sums_of(next_tile), cells)
    state = (*advance(parts, loadings_init, (), next_tile), next_tile)
    _, keep, send, stepped, mean, tile = lax.while_loop(
        lambda state: state[0] < steps - 1, one_step, (jnp.int32(1), *state)
    )
    mine, other, _ = scores_of(keep, send, ())
    parts = change_of(mine, other, tile, mean, mean)
    inverse = factor_of(mine, other)
    few = jax.ShapeDtypeStruct((9, 128), f32)
    many = jax.ShapeDtypeStruct((9 * chips, 128), f32)
    keep, send, stepped = vmem_call(make_last(batch), (few, few, local), len(parts) + 2, name="last")(
        core, *parts, stepped, inverse
    )
    copies = vmem_call(copies_kernel, many, 2, name="copies", core=False)(keep, swap_cores(send))
    mine = vmem_call(total_kernel, few, 1, name="total", core=False)(exchange(copies))
    scale = math.sqrt(genes * gene_devices)
    return vmem_call(make_finish(scale), local, 3, name="finish", held=False)(
        core, mine, swap_cores(mine), stepped
    )


def solution(mesh):
    placed = (P("gene", "cell"), P(None, "cell"), P(None, "gene"))
    return jax.shard_map(
        shards, mesh=mesh, in_specs=placed, out_specs=P(None, "gene"), check_vma=False
    )
```

```python
import math

import jax
import jax.numpy as jnp
from jax import lax
from jax.experimental import pallas as pl
from jax.experimental.pallas import tpu as pltpu
from jax.sharding import PartitionSpec as P

f32 = jnp.float32
bf16 = jnp.bfloat16
STEP_RATE = 1.0
HIGH = lax.Precision.HIGHEST
NT = (((1,), (1,)), ((), ()))
NN = (((1,), (0,)), ((), ()))


def vmem_call(kernel, outs, count, flops=0, name=None, core=True, pool=0, scratch=(), held=True):
    spec = pl.BlockSpec(memory_space=pltpu.VMEM)
    call = pl.pallas_call(
        kernel,
        out_shape=jax.tree.map(lambda s: pltpu.VMEM(s.shape, s.dtype), outs) if held else outs,
        in_specs=[pl.BlockSpec(memory_space=pltpu.SMEM)] * core
        + [spec] * count
        + [pl.BlockSpec(memory_space=pl.ANY)] * pool,
        out_specs=jax.tree.map(lambda _: spec, outs),
        cost_estimate=pl.CostEstimate(flops=flops, transcendentals=0, bytes_accessed=0),
        scratch_shapes=scratch,
        name=name,
    )

    def run(*args):
        last = core + count
        near = [pltpu.with_memory_space_constraint(a, pltpu.VMEM) for a in args[core:last]]
        return call(*args[:core], *near, *args[last:])

    return run


def split_pair(value):
    high = value.astype(bf16)
    low = (value - high.astype(f32)).astype(bf16)
    return jnp.concatenate([high, low], axis=0)


def gram_of(stepped):
    return lax.dot_general(stepped, stepped, NT, precision=HIGH, preferred_element_type=f32)


def by_core(first, mine, other):
    return jnp.concatenate([jnp.where(first, mine, other), jnp.where(first, other, mine)], axis=0)


def spread(scores, gram, first, keep_ref, send_ref):
    comps = scores.shape[0]
    half = comps // 2
    gram = jnp.concatenate([gram, jnp.zeros((comps, 128 - comps), f32)], axis=1)
    rows = scores.shape[1] // 128 + 1
    for j in range(rows):
        chunk = scores[:, j * 128 : (j + 1) * 128] if j + 1 < rows else gram
        top, bottom = chunk[:half], chunk[half:]
        keep_ref[pl.ds(j, half, stride=rows), :] = jnp.where(first, top, bottom)
        send_ref[pl.ds(j, half, stride=rows), :] = jnp.where(first, bottom, top)


def pack_partial(stepped, tile, shift, first, keep_ref, send_ref):
    comps = stepped.shape[0]
    both = lax.dot_general(split_pair(stepped), tile, NT, preferred_element_type=f32)
    spread(both[:comps] + both[comps:] - shift, gram_of(stepped), first, keep_ref, send_ref)


def first_kernel(core_ref, cell_ref, loadings_ref, picks_ref, pool_ref, keep_ref, send_ref, start_ref, names_ref, buffer_ref, sems):
    chunks, _, size = buffer_ref.shape
    near = [
        pltpu.make_async_copy(loadings_ref, start_ref, sems.at[chunks]),
        pltpu.make_async_copy(picks_ref, names_ref, sems.at[chunks + 1]),
    ]
    copies = [
        pltpu.make_async_copy(pool_ref.at[:, pl.ds(i * size, size)], buffer_ref.at[i], sems.at[i])
        for i in range(chunks)
    ]
    for copy in near + copies:
        copy.start()
    for copy in near:
        copy.wait()
    loadings = start_ref[...]
    comps = loadings.shape[0]
    pair = split_pair(loadings)
    picks = names_ref[0:1, :] - cell_ref[0]
    places = lax.broadcasted_iota(jnp.int32, (size, picks.shape[1]), 0)
    chosen = jnp.zeros((2 * comps, picks.shape[1]), f32)
    for i, copy in enumerate(copies):
        copy.wait()
        both = lax.dot_general(pair, buffer_ref[i], NN, preferred_element_type=f32)
        every = split_pair(both[:comps] + both[comps:])
        one_hot = jnp.where(places == picks - i * size, 1.0, 0.0).astype(bf16)
        chosen = chosen + lax.dot_general(every, one_hot, NN, preferred_element_type=f32)
    spread(chosen[:comps] + chosen[comps:], gram_of(loadings), core_ref[0] == 0, keep_ref, send_ref)


def add_kernel(a, b, out_ref):
    out_ref[...] = a[...] + b[...]


def stepped_from(parts, previous, inverse, batch, left=0.0):
    comps, genes = previous.shape
    total = sum(part[:comps, :genes] for part in parts) + left
    stepped = previous + STEP_RATE * (total * (1.0 / batch))
    if inverse is not None:
        stepped = lax.dot_general(inverse, stepped, NN, precision=HIGH, preferred_element_type=f32)
    return stepped


def row_of(part, start, genes):
    return part[start : start + 1, :genes]


def spare_row(part, genes):
    spare = part.shape[1] - genes
    return jnp.concatenate([part[i : i + 1, genes:] for i in range(genes // spare)], axis=1)


def between_groups(parts, comps, genes, batch):
    sums = [row_of(part, comps + 1, genes) for part in parts]
    mean = sum(sums) * (1.0 / batch)
    total = jnp.zeros((comps, genes), f32)
    for part, own in zip(parts, sums):
        total = total + part[:comps, genes : genes + 1] * (own * (len(parts) / batch) - mean)
    return total


def make_middle(batch, normalised):
    def kernel(core_ref, a, b, c, d, previous_ref, *refs):
        inverse = refs[0][...] if normalised else None
        tile_ref, keep_ref, send_ref, stepped_ref, mean_ref = refs[-5:]
        comps, genes = previous_ref.shape
        parts = (a, b, c, d)
        left = 0.0 if normalised else between_groups(parts, comps, genes, batch)
        stepped = stepped_from(parts, previous_ref[...], inverse, batch, left)
        stepped_ref[...] = stepped
        mean = sum(
            spare_row(part, genes) if normalised else row_of(part, comps, genes) for part in parts
        ) * (1.0 / batch)
        mean_ref[...] = mean
        shift = jnp.sum(stepped * mean, axis=1, keepdims=True)
        pack_partial(stepped, tile_ref[...], shift, core_ref[0] == 0, keep_ref, send_ref)

    return kernel


def lay_out(block):
    return jnp.concatenate([block[h : h + 8] for h in range(0, 32, 8)], axis=1)


def gather_up(rows):
    return jnp.concatenate([rows[:, w : w + 32] for w in range(0, 128, 32)], axis=0)


def make_last(batch):
    def kernel(core_ref, a, b, c, d, previous_ref, inverse_ref, keep_ref, send_ref, stepped_ref):
        stepped = stepped_from((a, b, c, d), previous_ref[...], inverse_ref[...], batch)
        stepped_ref[...] = stepped
        gram = gram_of(stepped)
        half = gram.shape[0] // 2
        rows = lax.broadcasted_iota(jnp.int32, (half, half), 0)
        columns = lax.broadcasted_iota(jnp.int32, (half, half), 1)
        upper, lower = gram[:half, :half], gram[half:, half:]
        corner = lay_out(gram[half:, :half])
        triangles = lay_out(jnp.where(rows >= columns, upper, lower))
        diagonal = jnp.sum(jnp.where(rows == columns, lower, 0.0), axis=0, keepdims=True)
        diagonal = jnp.concatenate([diagonal, jnp.zeros((1, 128 - half), f32)], axis=1)
        first = core_ref[0] == 0
        nothing = jnp.zeros((1, 128), f32)
        keep_ref[:8, :] = jnp.where(first, corner, triangles)
        keep_ref[8:9, :] = jnp.where(first, nothing, diagonal)
        send_ref[:8, :] = jnp.where(first, triangles, corner)
        send_ref[8:9, :] = jnp.where(first, diagonal, nothing)

    return kernel


def make_sum(count, rows):
    def kernel(in_ref, out_ref):
        for j in range(rows):
            total = jnp.sum(in_ref[pl.ds(j, count, stride=rows), :], axis=0, keepdims=True)
            out_ref[pl.ds(j, count, stride=rows), :] = jnp.broadcast_to(total, (count, 128))

    return kernel


def make_update(half, rows, cells=None):
    def kernel(core_ref, mine_ref, other_ref, tile_ref, mean_ref, next_ref, out_ref):
        genes = tile_ref.shape[1]
        comps = 2 * half
        width = out_ref.shape[1]
        chunks = [
            by_core(
                core_ref[0] == 0,
                mine_ref[pl.ds(j, half, stride=rows), :],
                other_ref[pl.ds(j, half, stride=rows), :],
            )
            for j in range(rows - 1)
        ]
        scores = jnp.concatenate(chunks, axis=1)
        both = lax.dot_general(split_pair(scores), tile_ref[...], NN, preferred_element_type=f32)
        totals = jnp.sum(scores, axis=1, keepdims=True)
        mean = mean_ref[...] * (1.0 / cells) if cells else mean_ref[...]
        raw = both[:comps] + both[comps:] - totals * mean
        spare = width - genes
        if cells:
            side = jnp.zeros((1, spare), f32)
            rest = out_ref.shape[0] - comps - 2
            out_ref[:comps, :] = jnp.concatenate([raw, jnp.broadcast_to(totals, (comps, spare))], axis=1)
            out_ref[comps : comps + 1, :] = jnp.concatenate([next_ref[...], side], axis=1)
            out_ref[comps + 1 : comps + 2, :] = jnp.concatenate([mean_ref[...], side], axis=1)
            out_ref[comps + 2 :, :] = jnp.zeros((rest, width), f32)
        else:
            sums = next_ref[...]
            pieces = [sums[:, i : i + spare] for i in range(0, genes, spare)]
            pieces.append(jnp.zeros((comps - len(pieces), spare), f32))
            out_ref[...] = jnp.concatenate([raw, jnp.concatenate(pieces, axis=0)], axis=1)

    return kernel


def inverse_factor(gram):
    size = gram.shape[0]
    shape = (8, 2 * size)
    rows = lax.broadcasted_iota(jnp.int32, shape, 0)
    lanes = lax.broadcasted_iota(jnp.int32, shape, 1)
    blocks = []
    for b in range(size // 8):
        eye = jnp.where(lanes == rows + (b * 8 + size), 1.0, 0.0).astype(f32)
        left = jnp.concatenate([gram[b * 8 : b * 8 + 8, :], jnp.zeros((8, size), f32)], axis=1)
        blocks.append(left + eye)
    results = list(blocks)
    for k in range(0, size, 2):
        b, r = divmod(k, 8)
        upper = blocks[b][r : r + 1, :]
        lower = blocks[b][r + 1 : r + 2, :]
        columns = [
            tuple(jnp.broadcast_to(blocks[i][:, k + h : k + h + 1], shape) for h in range(2))
            for i in range(b, size // 8)
        ]
        p = columns[0][0][r : r + 1, :]
        q = columns[0][0][r + 1 : r + 2, :]
        t = columns[0][1][r + 1 : r + 2, :]
        over = 1.0 / (p * t - q * q)
        first = (t * upper - q * lower) * over
        second = (p * lower - q * upper) * over
        inverse_p = 1.0 / p
        slope = q * inverse_p
        top = upper * lax.rsqrt(p)
        low = (lower - slope * upper) * lax.rsqrt(t - slope * q)
        results[b] = jnp.where(rows == r, top, jnp.where(rows == r + 1, low, results[b]))
        for i in range(b, size // 8):
            x, y = columns[i - b]
            change = x * first + y * second
            if i == b:
                change = jnp.where(rows > r + 1, change, 0.0)
            blocks[i] = blocks[i] - change
    return jnp.concatenate(results, axis=0)[:, size:]


def make_factor(half, rows):
    def kernel(core_ref, mine_ref, other_ref, out_ref):
        gram = by_core(
            core_ref[0] == 0,
            mine_ref[pl.ds(rows - 1, half, stride=rows), :],
            other_ref[pl.ds(rows - 1, half, stride=rows), :],
        )
        out_ref[...] = inverse_factor(gram[:, : 2 * half])

    return kernel


def copies_kernel(a, b, out_ref):
    rows = a.shape[0]
    count = out_ref.shape[0] // rows
    total = a[...] + b[...]
    for j in range(rows):
        out_ref[pl.ds(j, count, stride=rows), :] = jnp.broadcast_to(total[j : j + 1], (count, 128))


def total_kernel(in_ref, out_ref):
    rows = out_ref.shape[0]
    count = in_ref.shape[0] // rows
    for j in range(rows):
        out_ref[j : j + 1, :] = jnp.sum(in_ref[pl.ds(j, count, stride=rows), :], axis=0, keepdims=True)


def make_finish(scale):
    def kernel(core_ref, mine_ref, other_ref, stepped_ref, out_ref):
        first = core_ref[0] == 0
        corner = gather_up(jnp.where(first, mine_ref[:8, :], other_ref[:8, :]))
        triangles = gather_up(jnp.where(first, other_ref[:8, :], mine_ref[:8, :]))
        half = corner.shape[0]
        diagonal = jnp.where(first, other_ref[8:9, :half], mine_ref[8:9, :half])
        rows = lax.broadcasted_iota(jnp.int32, (half, half), 0)
        columns = lax.broadcasted_iota(jnp.int32, (half, half), 1)
        eye = jnp.where(rows == columns, 1.0, 0.0).astype(f32)

        def turned(block):
            return lax.dot_general(block, eye, (((0,), (0,)), ((), ())), precision=HIGH, preferred_element_type=f32)

        across = turned(triangles)
        upper = jnp.where(rows >= columns, triangles, across)
        lower = jnp.where(rows < columns, triangles, across)
        lower = jnp.where(rows == columns, jnp.broadcast_to(diagonal, (half, half)), lower)
        gram = jnp.concatenate(
            [
                jnp.concatenate([upper, turned(corner)], axis=1),
                jnp.concatenate([corner, lower], axis=1),
            ],
            axis=0,
        )
        out_ref[...] = scale * lax.dot_general(
            inverse_factor(gram), stepped_ref[...], NN, precision=HIGH, preferred_element_type=f32
        )

    return kernel


def shards(pool_counts, cell_picks, loadings_init):
    comps, genes = loadings_init.shape
    steps, cells = cell_picks.shape
    half = comps // 2
    local_pool = pool_counts.shape[1]
    cell_devices = lax.axis_size("cell")
    gene_devices = lax.axis_size("gene")
    chips = gene_devices // 2
    batch = cells * cell_devices
    rows = cells // 128 + 1
    width = genes + 128 - genes % 128
    first_cell = lax.axis_index("cell").astype(jnp.int32) * local_pool
    core = (lax.axis_index("gene") % 2).astype(jnp.int32).reshape(1)
    chosen = cell_picks - first_cell
    pool_by_cell = pool_counts.T
    same_core = [[2 * chip + which for chip in range(chips)] for which in range(2)]

    def tile_of(picks):
        return jnp.take(pool_by_cell, picks, axis=0, mode="clip")

    def sums_of(tile):
        return jnp.sum(tile, axis=0, dtype=f32, keepdims=True)

    def swap_cores(value):
        return lax.ppermute(value, "gene", [(i, i ^ 1) for i in range(gene_devices)])

    def round_cells(value):
        return [value] + [
            lax.ppermute(value, "cell", [(i, (i + k) % cell_devices) for i in range(cell_devices)])
            for k in range(cell_devices - 1, 0, -1)
        ]

    def exchange(value):
        pieces = value.reshape(chips, 1, value.size // chips)
        arrived = lax.all_to_all(pieces, "gene", 0, 0, tiled=True, axis_index_groups=same_core)
        return arrived.reshape(value.shape)

    packed = jax.ShapeDtypeStruct((half * rows, 128), f32)
    square = jax.ShapeDtypeStruct((comps, comps), f32)
    local = jax.ShapeDtypeStruct((comps, genes), f32)
    row = jax.ShapeDtypeStruct((1, genes), f32)

    chunk = local_pool // 8
    keep, send = vmem_call(
        first_kernel,
        (packed, packed),
        0,
        name="first",
        core=2,
        pool=3,
        scratch=[
            pltpu.VMEM((comps, genes), f32),
            pltpu.VMEM((steps, cells), jnp.int32),
            pltpu.VMEM((8, genes, chunk), bf16),
            pltpu.SemaphoreType.DMA((10,)),
        ],
    )(core, first_cell.reshape(1), loadings_init, cell_picks, pool_counts)

    def scores_of(keep, send, later):
        chip_sum = vmem_call(add_kernel, packed, 2, name="pair", core=False)(keep, swap_cores(send))
        came, later = lax.optimization_barrier((exchange(chip_sum), later))
        copies = vmem_call(make_sum(chips, rows), packed, 1, name="add_up", core=False)(came)
        mine = exchange(copies)
        return mine, swap_cores(mine), later

    def change_of(mine, other, tile, mean, next_sums, own=None):
        shared = jax.ShapeDtypeStruct((comps + 8 if own else comps, width), f32)
        change = vmem_call(make_update(half, rows, own), shared, 5, name="update")(
            core, mine, other, tile, mean, next_sums
        )
        return round_cells(change)

    def factor_of(mine, other):
        return vmem_call(make_factor(half, rows), square, 2, flops=10**9, name="factor")(core, mine, other)

    def advance(parts, stepped, inverse, next_tile):
        inputs = [*parts, stepped, *inverse, next_tile]
        return vmem_call(
            make_middle(batch, bool(inverse)), (packed, packed, local, row), len(inputs), name="middle"
        )(core, *inputs)

    def one_step(state):
        step, keep, send, stepped, mean, tile = state
        following = step + 1
        picks = lax.dynamic_index_in_dim(chosen, following, keepdims=False)
        following, picks, send = lax.optimization_barrier((following, picks, send))
        mine, other, picks = scores_of(keep, send, picks)
        next_tile = tile_of(picks)
        parts = change_of(mine, other, tile, mean, sums_of(next_tile))
        inverse = (factor_of(mine, other),)
        return (following, *advance(parts, stepped, inverse, next_tile), next_tile)

    mine, other, picks = scores_of(keep, send, chosen[:2])
    tile, next_tile = jnp.split(tile_of(picks.reshape(-1)), 2)
    parts = change_of(mine, other, tile, sums_of(tile), sums_of(next_tile), cells)
    state = (*advance(parts, loadings_init, (), next_tile), next_tile)
    _, keep, send, stepped, mean, tile = lax.while_loop(
        lambda state: state[0] < steps - 1, one_step, (jnp.int32(1), *state)
    )
    mine, other, _ = scores_of(keep, send, ())
    parts = change_of(mine, other, tile, mean, mean)
    inverse = factor_of(mine, other)
    few = jax.ShapeDtypeStruct((9, 128), f32)
    many = jax.ShapeDtypeStruct((9 * chips, 128), f32)
    keep, send, stepped = vmem_call(make_last(batch), (few, few, local), len(parts) + 2, name="last")(
        core, *parts, stepped, inverse
    )
    copies = vmem_call(copies_kernel, many, 2, name="copies", core=False)(keep, swap_cores(send))
    mine = vmem_call(total_kernel, few, 1, name="total", core=False)(exchange(copies))
    scale = math.sqrt(genes * gene_devices)
    return vmem_call(make_finish(scale), local, 3, name="finish", held=False)(
        core, mine, swap_cores(mine), stepped
    )


def solution(mesh):
    placed = (P("gene", "cell"), P(None, "cell"), P(None, "gene"))
    return jax.shard_map(
        shards, mesh=mesh, in_specs=placed, out_specs=P(None, "gene"), check_vma=False
    )
```
